128 devices in a mesh: dp: 1, fsdp: 128 (over z, y, x, core).
Axes of the slice: x: 4, y: 4, z: 4, core: 2. Of those that a mesh axis runs over, the one named last changes fastest.
Arguments:
- prompts: bfloat16 [128, 512, 2304], P(('dp', 'fsdp'))
- ln1_gain: bfloat16 [2304], P('fsdp')
- ln1_bias: bfloat16 [2304], P('fsdp')
- w_qkv: bfloat16 [2304, 3, 24, 96], P('fsdp')
- b_qkv: bfloat16 [6912], P('fsdp')
- w_out: bfloat16 [2304, 2304], P('fsdp')
- b_out: bfloat16 [2304], P('fsdp')
- ln2_gain: bfloat16 [2304], P('fsdp')
- ln2_bias: bfloat16 [2304], P('fsdp')
- w_up: bfloat16 [2304, 9216], P('fsdp')
- b_up: bfloat16 [9216], P('fsdp')
- w_down: bfloat16 [9216, 2304], P('fsdp')
- b_down: bfloat16 [2304], P('fsdp')
Outputs:
- output 1: bfloat16 [128, 512, 2304], P(('dp', 'fsdp'))
- output 2: bfloat16 [128, 512, 24, 96], P(('dp', 'fsdp'))
- output 3: bfloat16 [128, 512, 24, 96], P(('dp', 'fsdp'))
All inputs are finite; a program needn't handle non-finite values.
Results may differ from the reference program's by a relative error of at most 0.00838182.
Values are sent between devices in bfloat16 or wider.
A program may use at most 1 GiB of HBM per device.

```python
import jax
import jax.numpy as jnp
from jax import lax

D = 2304
HEADS = 24
HEAD = 96
SEQ = 512
BATCH = 128
FFN = 4 * D
QBLOCK = min(SEQ, 256)
LN_EPS = 1e-5


def draw_normal(key, shape, scale, offset=0.0):
    return (offset + scale * jax.random.normal(key, shape, jnp.float32)).astype(jnp.bfloat16)


def setup_inputs(seed: int = 0, part: int = 0) -> dict:
    keys = jax.random.split(jax.random.key(seed), 13)
    return {
        'prompts': draw_normal(jax.random.fold_in(keys[0], part), (BATCH, SEQ, D), 1.0),
        'ln1_gain': draw_normal(keys[1], (D,), 0.3, 1.0),
        'ln1_bias': draw_normal(keys[2], (D,), 0.3),
        'w_qkv': draw_normal(keys[3], (D, 3, HEADS, HEAD), D ** -0.5),
        'b_qkv': draw_normal(keys[4], (3 * HEADS * HEAD,), 0.5),
        'w_out': draw_normal(keys[5], (HEADS * HEAD, D), (HEADS * HEAD) ** -0.5),
        'b_out': draw_normal(keys[6], (D,), 0.5),
        'ln2_gain': draw_normal(keys[7], (D,), 0.3, 1.0),
        'ln2_bias': draw_normal(keys[8], (D,), 0.3),
        'w_up': draw_normal(keys[9], (D, FFN), D ** -0.5),
        'b_up': draw_normal(keys[10], (FFN,), 0.5),
        'w_down': draw_normal(keys[11], (FFN, D), 1.5 * FFN ** -0.5),
        'b_down': draw_normal(keys[12], (D,), 0.5),
    }


def layer_norm(act, gain, shift):
    act_f32 = act.astype(jnp.float32)
    mean_val = jnp.mean(act_f32, axis=-1, keepdims=True)
    centered = act_f32 - mean_val
    var_val = jnp.mean(centered * centered, axis=-1, keepdims=True)
    normed = centered * lax.rsqrt(var_val + LN_EPS)
    return (normed * gain.astype(jnp.float32) + shift.astype(jnp.float32)).astype(jnp.bfloat16)


def reference(prompts, ln1_gain, ln1_bias, w_qkv, b_qkv, w_out, b_out, ln2_gain, ln2_bias, w_up, b_up, w_down, b_down):
    w_qkv_flat = w_qkv.reshape(D, 3 * HEADS * HEAD)
    key_pos = jnp.arange(SEQ)

    def one_prompt(prompt):
        normed1 = layer_norm(prompt, ln1_gain, ln1_bias)
        proj_qkv = jnp.dot(normed1, w_qkv_flat, preferred_element_type=jnp.float32)
        proj_qkv = (proj_qkv + b_qkv.astype(jnp.float32)).astype(jnp.bfloat16).reshape(SEQ, 3, HEADS, HEAD)
        keys_f32 = proj_qkv[:, 1].astype(jnp.float32)
        values_f32 = proj_qkv[:, 2].astype(jnp.float32)
        query_blocks = proj_qkv[:, 0].astype(jnp.float32).reshape(SEQ // QBLOCK, QBLOCK, HEADS, HEAD)

        def one_block(block_in):
            q_blk, blk_idx = block_in
            scores = jnp.einsum('qhe,khe->hqk', q_blk, keys_f32) * (HEAD ** -0.5)
            query_pos = blk_idx * QBLOCK + jnp.arange(QBLOCK)
            allowed = key_pos[None, :] <= query_pos[:, None]
            scores = jnp.where(allowed[None], scores, -jnp.inf)
            probs = jax.nn.softmax(scores, axis=-1).astype(jnp.bfloat16)
            context = jnp.einsum('hqk,khe->qhe', probs.astype(jnp.float32), values_f32)
            return context.astype(jnp.bfloat16)

        context = lax.map(one_block, (query_blocks, jnp.arange(SEQ // QBLOCK))).reshape(SEQ, HEADS * HEAD)
        attn_out = jnp.dot(context, w_out, preferred_element_type=jnp.float32)
        resid = (prompt.astype(jnp.float32) + attn_out + b_out.astype(jnp.float32)).astype(jnp.bfloat16)
        normed2 = layer_norm(resid, ln2_gain, ln2_bias)
        hidden = jnp.dot(normed2, w_up, preferred_element_type=jnp.float32) + b_up.astype(jnp.float32)
        hidden = jax.nn.gelu(hidden, approximate=True).astype(jnp.bfloat16)
        mlp_out = jnp.dot(hidden, w_down, preferred_element_type=jnp.float32)
        out_one = (resid.astype(jnp.float32) + mlp_out + b_down.astype(jnp.float32)).astype(jnp.bfloat16)
        return out_one, proj_qkv[:, 1], proj_qkv[:, 2]

    layer_out, k_cache, v_cache = lax.map(one_prompt, prompts)
    return layer_out, k_cache, v_cache
```

```python
import functools

import jax
import jax.numpy as jnp
from jax import lax
from jax.experimental import pallas as pl
from jax.experimental.pallas import tpu as pltpu
from jax.sharding import PartitionSpec as P

LN_EPS = 1e-5
MESH = pl.DeviceIdType.MESH
BF = jnp.bfloat16
F32 = jnp.float32
CHUNKS = 9
SLOTS = 3


def layer_kernel(dims, x_ref, own, ln1g, ln1b, bqkv, bout, ln2g, ln2b, bup, bdown,
                 y_ref, kt_out, vt_out, G,
                 h, qkvt, ctxt, ctx, x1, a, wbuf, acc, R, S, LS, KS):
    seq, d, heads, hd, rows, lane = dims
    pair = 2 * lane
    me = lax.axis_index("fsdp")
    core = lax.rem(me, 2)
    cx = lax.rem(me // 2, 4)
    cy = lax.rem(me // 8, 4)
    cz = me // 32
    sib = me + 1 - 2 * core

    def pick(c, v0, v1, v2):
        return jnp.where(c == 0, v0, jnp.where(c == 1, v1, v2))

    def place(c):
        i0 = pick(c, cx, cy, cz)
        i1 = pick(c, cy, cz, cx)
        i2 = pick(c, cz, cx, cy)
        return i0, i1, i2

    def strides(c):
        return pick(c, 2, 8, 32), pick(c, 8, 32, 2), pick(c, 32, 2, 8)

    def near(i, stride):
        up = lax.rem(i + 1, 4)
        down = lax.rem(i + 3, 4)
        return me + (up - i) * stride, me + (down - i) * stride, up, down

    def send(src, dst, s, r, dev):
        pltpu.make_async_remote_copy(
            src_ref=src, dst_ref=dst, send_sem=s, recv_sem=r,
            device_id={"fsdp": dev}, device_id_type=MESH).start()

    def take(ref, sem):
        pltpu.make_async_copy(ref, ref, sem).wait()

    def colours(body):
        def step(c, carry):
            body(c)
            return carry
        lax.fori_loop(0, 3, step, 0)

    def slab(k, c):
        return (k * 2 + core) * 3 + c

    def p0_send(k):
        def body(c):
            i0, i1, i2 = place(c)
            right, left, _, _ = near(i0, strides(c)[0])
            dst = G.at[slab(k, c), i2, i1, i0]
            src = own.at[k * 3 + c]
            send(src, dst, S.at[k, 0], R.at[k * 3 + c, 0], right)
            send(src, dst, S.at[k, 0], R.at[k * 3 + c, 0], left)
        colours(body)

    def p0_forward(k):
        def body(c):
            i0, i1, i2 = place(c)
            right, left, up, down = near(i0, strides(c)[0])
            g = slab(k, c)
            take(G.at[g, 0, 0, pl.ds(0, 2)], R.at[k * 3 + c, 0])
            if k % 2 == 0:
                blk = G.at[g, i2, i1, down]
                send(blk, blk, S.at[k, 0], R.at[k * 3 + c, 1], right)
            else:
                blk = G.at[g, i2, i1, up]
                send(blk, blk, S.at[k, 0], R.at[k * 3 + c, 1], left)
        colours(body)

    def p0_done(k):
        colours(lambda c: take(G.at[slab(k, c), 0, 0, 0], R.at[k * 3 + c, 1]))

    def p1_send(k):
        def body(c):
            i0, i1, i2 = place(c)
            right, left, _, _ = near(i1, strides(c)[1])
            lo = G.at[slab(k, c), i2, i1, pl.ds(0, 2)]
            hi = G.at[slab(k, c), i2, i1, pl.ds(2, 2)]
            q = k * 3 + c
            send(lo, lo, S.at[k, 1], R.at[q, 2], right)
            send(hi, hi, S.at[k, 1], R.at[q, 2], left)
            send(hi, hi, S.at[k, 1], R.at[q, 3], right)
            send(lo, lo, S.at[k, 1], R.at[q, 3], left)
        colours(body)

    def p1_forward(k):
        def body(c):
            i0, i1, i2 = place(c)
            right, left, up, down = near(i1, strides(c)[1])
            g = slab(k, c)
            q = k * 3 + c
            take(G.at[g, 0, 0], R.at[q, 2])
            lo = G.at[g, i2, down, pl.ds(0, 2)]
            hi = G.at[g, i2, up, pl.ds(2, 2)]
            send(lo, lo, S.at[k, 1], R.at[q, 3], right)
            send(hi, hi, S.at[k, 1], R.at[q, 3], left)
        colours(body)

    def p1_done(k):
        colours(lambda c: take(G.at[slab(k, c), 0, pl.ds(0, 2)], R.at[k * 3 + c, 3]))

    def p2_first(k):
        def body(c):
            i0, i1, i2 = place(c)
            right, left, _, _ = near(i2, strides(c)[2])
            g = slab(k, c)
            lo = G.at[g, i2, pl.ds(0, 2)]
            hi = G.at[g, i2, pl.ds(2, 2)]
            send(lo, lo, S.at[k, 2], R.at[k * 3 + c, 4], right)
            send(hi, hi, S.at[k, 2], R.at[k * 3 + c, 4], left)
            send(G.at[g, i2], G.at[g, i2], S.at[k, 3], R.at[k * 3 + c, 6], sib)
        colours(body)

    def p2_second(k):
        def body(c):
            i0, i1, i2 = place(c)
            right, left, _, _ = near(i2, strides(c)[2])
            g = slab(k, c)
            lo = G.at[g, i2, pl.ds(0, 2)]
            hi = G.at[g, i2, pl.ds(2, 2)]
            send(hi, hi, S.at[k, 2], R.at[k * 3 + c, 5], right)
            send(lo, lo, S.at[k, 2], R.at[k * 3 + c, 5], left)
        colours(body)

    def p2_forward(k):
        def body(c):
            i0, i1, i2 = place(c)
            right, left, up, down = near(i2, strides(c)[2])
            g = slab(k, c)
            q = k * 3 + c
            take(G.at[g, 0], R.at[q, 4])
            lo = G.at[g, down, pl.ds(0, 2)]
            hi = G.at[g, up, pl.ds(2, 2)]
            send(lo, lo, S.at[k, 2], R.at[q, 5], right)
            send(hi, hi, S.at[k, 2], R.at[q, 5], left)
        colours(body)

    def p2_done(k):
        def body(c):
            i0, i1, i2 = place(c)
            g = slab(k, c)
            take(G.at[g, pl.ds(0, 2)], R.at[k * 3 + c, 5])
            for o in range(1, 4):
                part = G.at[g, lax.rem(i2 + o, 4)]
                send(part, part, S.at[k, 3], R.at[k * 3 + c, 6], sib)
        colours(body)

    def sibling_done(k):
        colours(lambda c: take(G.at[slab(k, c)], R.at[k * 3 + c, 6]))

    def issue(t):
        if t + 2 < CHUNKS:
            p0_send(t + 2)
        if t + 1 < CHUNKS:
            p1_send(t + 1)
        if t < CHUNKS:
            p2_first(t)

    def visit1(t):
        if t >= 1:
            p2_done(t - 1)
        if t + 2 < CHUNKS:
            p0_forward(t + 2)
        if t + 1 < CHUNKS:
            p1_forward(t + 1)
        p2_second(t)

    def visit2(t):
        p2_forward(t)
        if t + 2 < CHUNKS:
            p0_done(t + 2)
        if t + 1 < CHUNKS:
            p1_done(t + 1)
        issue(t + 1)
        if t >= 1:
            sibling_done(t - 1)

    def load_cols(k, u, slot):
        x = u // 3
        c = lax.rem(u, 3)
        for s in range(2):
            g = (k * 2 + s) * 3 + c
            dst = wbuf.at[slot, :, :, :, pl.ds(s * lane, lane)]

            @pl.when(c == 0)
            def _():
                pltpu.make_async_copy(G.at[g, :, :, x], dst, LS.at[slot]).start()

            @pl.when(c == 1)
            def _():
                pltpu.make_async_copy(G.at[g, x], dst, LS.at[slot]).start()

            @pl.when(c == 2)
            def _():
                for y in range(4):
                    pltpu.make_async_copy(
                        G.at[g, y, x], wbuf.at[slot, :, y, :, pl.ds(s * lane, lane)], LS.at[slot]).start()

    def load_rows(k, u, slot):
        c = u // 4
        z = lax.rem(u, 4)
        for s in range(2):
            g = (k * 2 + s) * 3 + c
            dst = wbuf.at[slot, :, :, :, pl.ds(s * lane, lane)]

            @pl.when(c == 0)
            def _():
                pltpu.make_async_copy(G.at[g, z], dst, LS.at[slot]).start()

            @pl.when(c == 1)
            def _():
                for x in range(4):
                    pltpu.make_async_copy(
                        G.at[g, x, z], wbuf.at[slot, :, x, :, pl.ds(s * lane, lane)], LS.at[slot]).start()

            @pl.when(c == 2)
            def _():
                pltpu.make_async_copy(G.at[g, :, :, z], dst, LS.at[slot]).start()

    def run_units(load, k, lo, hi, body):
        load(k, lo, lo % SLOTS)
        load(k, lo + 1, (lo + 1) % SLOTS)

        def step(u, carry):
            slot = lax.rem(u, SLOTS)
            take(wbuf.at[slot], LS.at[slot])

            @pl.when(u + 2 < hi)
            def _():
                load(k, u + 2, lax.rem(u + 2, SLOTS))
            body(u, slot)
            return carry
        lax.fori_loop(lo, hi, step, 0)

    def weight(slot):
        return wbuf[slot].reshape(d, pair)

    def qkv_unit(k):
        def body(u, slot):
            p = 12 * k + u
            r = jnp.dot(h[...], weight(slot), preferred_element_type=F32) + bqkv[p]
            qkvt[pl.ds(pl.multiple_of(p * pair, pair), pair), :] = r.astype(BF).T
        return body

    def out_unit(u, slot):
        p = u - 3
        cols = pl.ds(pl.multiple_of(p * pair, pair), pair)
        r = jnp.dot(ctx[...], weight(slot), preferred_element_type=F32)
        x1[:, cols] = (x_ref[:, cols].astype(F32) + r + bout[p]).astype(BF)

    def up_unit(k):
        def body(u, slot):
            p = 12 * (k - 3) + u
            cols = pl.ds(pl.multiple_of(p * pair, pair), pair)
            r = jnp.dot(h[...], weight(slot), preferred_element_type=F32) + bup[p]
            a[:, cols] = jax.nn.gelu(r, approximate=True).astype(BF)
        return body

    def down_unit(k):
        def body(u, slot):
            c = u // 4
            z = lax.rem(u, 4)
            p = 3 * (k - 6) + c
            cols = pl.ds(pl.multiple_of(p * pair, pair), pair)
            r = jnp.dot(a[:, pl.ds(pl.multiple_of(z * d, lane), d)], weight(slot), preferred_element_type=F32)

            @pl.when(z == 0)
            def _():
                acc[...] = r

            @pl.when(z > 0)
            def _():
                acc[...] += r

            @pl.when(z == 3)
            def _():
                y_ref[:, cols] = (x1[:, cols].astype(F32) + acc[...] + bdown[p]).astype(BF)
        return body

    def norm(src, gain, shift):
        n = seq // 8

        def step(b, carry):
            at = pl.ds(pl.multiple_of(b * n, n), n)
            v = src[at, :].astype(F32)
            v = v - jnp.mean(v, axis=-1, keepdims=True)
            var = jnp.mean(v * v, axis=-1, keepdims=True)
            h[at, :] = (v * lax.rsqrt(var + LN_EPS) * gain[...] + shift[...]).astype(BF)
            return carry
        lax.fori_loop(0, 8, step, 0)

    def attend(lo, hi):
        qb = seq // 2
        scale = hd ** -0.5

        def step(i, carry):
            q_rows = pl.ds(pl.multiple_of(i * hd, hd), hd)
            k_rows = pl.ds(pl.multiple_of(i * hd + d, hd), hd)
            v_rows = pl.ds(pl.multiple_of(i * hd + 2 * d, hd), hd)
            for b in range(2):
                n = (b + 1) * qb
                q = qkvt[q_rows, b * qb:n]
                s = lax.dot_general(q, qkvt[k_rows, :n], (((0,), (0,)), ((), ())),
                                    preferred_element_type=F32) * scale
                row = lax.broadcasted_iota(jnp.int32, (qb, n), 0) + b * qb
                col = lax.broadcasted_iota(jnp.int32, (qb, n), 1)
                s = jnp.where(col <= row, s, -jnp.inf)
                e = jnp.exp(s - jnp.max(s, axis=-1, keepdims=True))
                w = (e / jnp.sum(e, axis=-1, keepdims=True)).astype(BF)
                o = lax.dot_general(qkvt[v_rows, :n], w, (((1,), (1,)), ((), ())),
                                    preferred_element_type=F32)
                ctxt[q_rows, b * qb:n] = o.astype(BF)
            return carry
        lax.fori_loop(lo, hi, step, 0)

    def flip():
        def step(i, carry):
            at = pl.ds(pl.multiple_of(i * pair, pair), pair)
            ctx[:, at] = ctxt[at, :].T
            return carry
        lax.fori_loop(0, d // pair, step, 0)

    def cache_copy(which):
        out = kt_out if which == 0 else vt_out
        return pltpu.make_async_copy(qkvt.at[pl.ds((which + 1) * d, d)], out, KS.at[which])

    p0_send(0)
    p0_send(1)

    def put(q, carry):
        c = lax.rem(q, 3)
        i0, i1, i2 = place(c)
        pltpu.make_async_copy(own.at[q], G.at[slab(q // 3, c), i2, i1, i0], KS.at[2]).start()
        return carry
    lax.fori_loop(0, 27, put, 0)
    take(G.at[pl.ds(0, 27), 0, 0, 0], KS.at[2])
    p0_forward(0)
    p0_forward(1)
    p0_done(0)
    p1_send(0)
    p1_forward(0)
    p0_done(1)
    p1_done(0)
    issue(0)
    norm(x_ref, ln1g, ln1b)
    visit1(0)
    visit2(0)

    visit1(1)
    visit2(1)
    run_units(load_cols, 0, 0, 12, qkv_unit(0))
    visit1(2)
    visit2(2)
    run_units(load_cols, 1, 0, 12, qkv_unit(1))
    visit1(3)
    visit2(3)
    run_units(load_cols, 2, 0, 3, qkv_unit(2))
    a1 = heads * 5 // 12
    a2 = heads * 9 // 12
    attend(0, a1)
    visit1(4)
    attend(a1, a2)
    visit2(4)
    attend(a2, heads)
    cache_copy(0).start()
    cache_copy(1).start()
    flip()
    run_units(load_cols, 2, 3, 12, out_unit)
    visit1(5)
    norm(x1, ln2g, ln2b)
    run_units(load_cols, 3, 0, 12, up_unit(3))
    visit2(5)
    run_units(load_cols, 4, 0, 12, up_unit(4))
    visit1(6)
    visit2(6)
    run_units(load_cols, 5, 0, 12, up_unit(5))
    visit1(7)
    visit2(7)
    run_units(load_rows, 6, 0, 12, down_unit(6))
    visit1(8)
    visit2(8)
    run_units(load_rows, 7, 0, 12, down_unit(7))
    p2_done(8)
    sibling_done(8)
    run_units(load_rows, 8, 0, 12, down_unit(8))

    cache_copy(0).wait()
    cache_copy(1).wait()
    for k in range(CHUNKS):
        take(G.at[pl.ds(0, 3), 0, 0, pl.ds(0, 3)], S.at[k, 0])
        take(G.at[pl.ds(0, 3), 0, pl.ds(0, 3)], S.at[k, 1])
        take(G.at[pl.ds(0, 3), pl.ds(0, 3)], S.at[k, 2])
        take(G.at[pl.ds(0, 3)], S.at[k, 3])


def solution(mesh):
    batch_axes = ('dp', 'fsdp')
    n_dev = mesh.shape['fsdp']

    def exchange(blocks, size):
        groups = [list(range(i, i + size)) for i in range(0, n_dev, size)]
        return lax.all_to_all(blocks, 'fsdp', 0, 0, axis_index_groups=groups, tiled=True)

    def local_layer(prompts, ln1_gain, ln1_bias, w_qkv, b_qkv, w_out, b_out, ln2_gain, ln2_bias, w_up, b_up, w_down, b_down):
        _, seq, d = prompts.shape
        heads, hd = w_qkv.shape[2], w_qkv.shape[3]
        lane = d // 18
        rows = d // 16
        pair = 2 * lane
        r = w_up.shape[0]

        parts = [ln1_gain, ln1_bias, b_out, ln2_gain, ln2_bias, b_down, b_qkv, b_up]
        packed = jnp.concatenate(parts)
        total = packed.shape[0]
        packed = jnp.pad(packed, (0, -total % 128))
        packed = lax.all_gather(packed, 'fsdp', axis=0)
        vecs, at = [], 0
        for part in parts:
            vecs.append(packed[:, at:at + part.shape[0]].reshape(-1).astype(F32))
            at += part.shape[0]
        g1, s1, bo, g2, s2, bd, bq, bu = vecs

        w1 = jnp.concatenate([w_qkv.reshape(r, -1), w_out], axis=1)
        w12 = jnp.stack([w1, w_up]).reshape(2, r, 3, 4, 3, 2, lane)
        w12 = w12.transpose(3, 5, 0, 2, 4, 1, 6).reshape(8, 18 * r, lane)
        w12 = exchange(w12, 8).reshape(8, 18, r, lane).transpose(1, 0, 2, 3).reshape(18, rows, lane)
        w3 = w_down.reshape(-1, 9, 2, lane).transpose(2, 1, 0, 3).reshape(2, -1, lane)
        w3 = exchange(w3, 2).reshape(2, 9, -1, lane).transpose(1, 0, 2, 3).reshape(9, rows, lane)
        own = jnp.concatenate([w12, w3], axis=0)

        dims = (seq, d, heads, hd, rows, lane)
        vm = pl.BlockSpec(memory_space=pltpu.VMEM)
        hbm = pl.BlockSpec(memory_space=pl.ANY)
        y, kt, vt, _ = pl.pallas_call(
            functools.partial(layer_kernel, dims),
            out_shape=(
                jax.ShapeDtypeStruct((seq, d), BF),
                jax.ShapeDtypeStruct((d, seq), BF),
                jax.ShapeDtypeStruct((d, seq), BF),
                jax.ShapeDtypeStruct((6 * CHUNKS, 4, 4, 4, rows, lane), BF),
            ),
            in_specs=[vm] * 10,
            out_specs=(vm, hbm, hbm, hbm),
            scratch_shapes=[
                pltpu.VMEM((seq, d), BF),
                pltpu.VMEM((3 * d, seq), BF),
                pltpu.VMEM((d, seq), BF),
                pltpu.VMEM((seq, d), BF),
                pltpu.VMEM((seq, d), BF),
                pltpu.VMEM((seq, 4 * d), BF),
                pltpu.VMEM((SLOTS, 4, 4, rows, pair), BF),
                pltpu.VMEM((seq, pair), F32),
                pltpu.SemaphoreType.DMA((3 * CHUNKS, 7)),
                pltpu.SemaphoreType.DMA((CHUNKS, 4)),
                pltpu.SemaphoreType.DMA((SLOTS,)),
                pltpu.SemaphoreType.DMA((3,)),
            ],
            compiler_params=pltpu.CompilerParams(
                has_side_effects=True, vmem_limit_bytes=62 * 1024 * 1024),
            name="layer",
        )(prompts[0], own, g1[None], s1[None], bq.reshape(-1, 1, pair), bo.reshape(-1, 1, pair),
          g2[None], s2[None], bu.reshape(-1, 1, pair), bd.reshape(-1, 1, pair))
        kc = kt.reshape(heads, hd, seq).transpose(2, 0, 1)[None]
        vc = vt.reshape(heads, hd, seq).transpose(2, 0, 1)[None]
        return y[None], kc, vc

    weight_spec = P('fsdp')
    return jax.shard_map(local_layer, mesh=mesh, in_specs=(P(batch_axes),) + (weight_spec,) * 12, out_specs=(P(batch_axes), P(batch_axes), P(batch_axes)), check_vma=False)
```

```python
import functools

import jax
import jax.numpy as jnp
import numpy as np
from jax import lax
from jax.experimental import pallas as pl
from jax.experimental.pallas import tpu as pltpu
from jax.sharding import PartitionSpec as P

LN_EPS = 1e-5
MESH = pl.DeviceIdType.MESH
BF = jnp.bfloat16
F32 = jnp.float32
CHUNKS = 9
SLOTS = 3
LO, HI, ALL3 = pl.ds(0, 2), pl.ds(2, 2), pl.ds(0, 3)
FIRST, SECOND, ACROSS, SIBLING = range(4)
ZEROS = (0, 0, 0)
THREE = range(3)
UNITS = 12
LANES = 128
LATE = (3, 4, 5)


def loop(hi, body, lo=0):
    def step(i, carry):
        body(i)
        return carry
    lax.fori_loop(lo, hi, step, None)


def wrap(i):
    return lax.rem(i, 4)


def layer_kernel(dims, x_ref, w1, w2, w3, vec, tab,
                 y_ref, kv_ref, G12, G3,
                 h, qt, ctxt, ctx, x1, a, wbuf, wbuf3, acc, own12, own3, stage12, stage3, V, lnv, bqkv, bout, bup, bdown, vrow,
                 R, S, LS, OS, X, XS, VR, VS):
    seq, d, heads, hd, rows, lane = dims
    pair = 2 * lane
    me = lax.axis_index("fsdp")
    core = lax.rem(me, 2)
    cx = wrap(me // 2)
    cy = wrap(me // 8)
    cz = me // 32
    sib = me + 1 - 2 * core
    spot = lax.rem(me, 8)

    class Block:
        def __init__(self, k):
            self.ref = G12 if k < 6 else G3
            self.base = k if k < 6 else k - 6

        def slab(self, c):
            return (self.base * 2 + core) * 3 + c

        def own(self, c):
            return (own12 if self.ref is G12 else own3).at[self.base * 3 + c]

    def pick(c, v):
        return jnp.where(c == 0, v[0], jnp.where(c == 1, v[1], v[2]))

    def place(c):
        v = (cx, cy, cz)
        return tuple(pick(c, v[p:] + v[:p]) for p in THREE)

    def near(c, p):
        v = (2, 8, 32)
        stride = pick(c, v[p:] + v[:p])
        i = place(c)[p]
        up, down = wrap(i + 1), wrap(i + 3)
        return me + (up - i) * stride, me + (down - i) * stride, up, down

    def send(src, dst, s, r, dev):
        pltpu.make_async_remote_copy(
            src_ref=src, dst_ref=dst, send_sem=s, recv_sem=r,
            device_id={"fsdp": dev}, device_id_type=MESH).start()

    def take(ref, sem):
        pltpu.make_async_copy(ref, ref, sem).wait()

    def colours(body):
        loop(3, body)

    def await_group(k, p, role, n=None):
        B = Block(k)

        def body(c):
            at = (B.slab(c),) + ZEROS[:3 - p]
            if n is not None:
                at = at[:-1] + (n,)
            take(B.ref.at[at], R.at[k * 3 + c, p, role])
        colours(body)

    def await_siblings(k, *roles):
        for role in roles:
            B = Block(k)
            part = LO if role == SECOND else 0
            colours(lambda c: take(B.ref.at[B.slab(c), part], R.at[k * 3 + c, SIBLING, role]))

    def p0_send(k):
        B = Block(k)

        def body(c):
            i0, i1, i2 = place(c)
            right, left, _, _ = near(c, 0)
            dst = B.ref.at[B.slab(c), i2, i1, i0]
            for dev in (right, left):
                send(B.own(c), dst, S.at[k, 0], R.at[k * 3 + c, 0, FIRST], dev)
            pltpu.make_async_copy(B.own(c), dst, OS.at[k]).start()
        colours(body)

    def p0_forward(k):
        B = Block(k)
        take(B.ref.at[0, 0, 0, ALL3], OS.at[k])
        await_group(k, 0, FIRST, LO)

        def body(c):
            i0, i1, i2 = place(c)
            right, left, up, down = near(c, 0)
            from_, to = (down, right) if k % 2 == 0 else (up, left)
            blk = B.ref.at[B.slab(c), i2, i1, from_]
            send(blk, blk, S.at[k, 0], R.at[k * 3 + c, 0, ACROSS], to)
        colours(body)

    def halves(k, c, p, i):
        B = Block(k)
        at = (B.slab(c), place(c)[2], i) if p == 1 else (B.slab(c), i)
        return B.ref.at[at + (LO,)], B.ref.at[at + (HI,)]

    def to_sibling(k, c, ahead, role):
        B = Block(k)
        part = B.ref.at[B.slab(c), wrap(place(c)[2] + ahead)]
        send(part, part, S.at[k, SIBLING], R.at[k * 3 + c, SIBLING, role], sib)

    def axis_first(k, p):
        def body(c):
            right, left, _, _ = near(c, p)
            lo, hi = halves(k, c, p, place(c)[p])
            send(lo, lo, S.at[k, p], R.at[k * 3 + c, p, FIRST], right)
            send(hi, hi, S.at[k, p], R.at[k * 3 + c, p, FIRST], left)
            if p == 2:
                to_sibling(k, c, 0, FIRST)
        colours(body)

    def axis_second(k, p):
        def body(c):
            right, left, _, _ = near(c, p)
            lo, hi = halves(k, c, p, place(c)[p])
            send(hi, hi, S.at[k, p], R.at[k * 3 + c, p, SECOND], right)
            send(lo, lo, S.at[k, p], R.at[k * 3 + c, p, SECOND], left)
        colours(body)

    def axis_forward(k, p):
        await_group(k, p, FIRST)

        def body(c):
            right, left, up, down = near(c, p)
            lo, hi = halves(k, c, p, down)[0], halves(k, c, p, up)[1]
            send(lo, lo, S.at[k, p], R.at[k * 3 + c, p, ACROSS], right)
            send(hi, hi, S.at[k, p], R.at[k * 3 + c, p, ACROSS], left)
        colours(body)

    def sides_in(k):
        await_group(k, 2, SECOND)

        def body(c):
            to_sibling(k, c, 1, SECOND)
            to_sibling(k, c, 3, SECOND)
        colours(body)

    def across_in(k):
        await_group(k, 2, ACROSS)
        colours(lambda c: to_sibling(k, c, 2, ACROSS))

    def x_send(k):
        src = w1 if k < 3 else w2
        j = k % 3

        def part(i, c):
            tile = 24 * j + 6 * (i // 2) + 2 * c + lax.rem(i, 2)
            return src.at[:, pl.ds(pl.multiple_of(tile * lane, lane), lane)]

        def body(o):
            i = lax.rem(spot + o, 8)
            for c in THREE:
                send(part(i, c), stage12.at[spot, 3 * k + c], XS.at[k], X.at[k], me - spot + i)
        loop(8, body, 1)
        for c in THREE:
            pltpu.make_async_copy(part(spot, c), stage12.at[spot, 3 * k + c], X.at[k]).start()

    def x_blocks(k):
        take(stage12.at[:, pl.ds(3 * k, 3)], X.at[k])
        for c in THREE:
            q = 3 * k + c
            own12[q] = jnp.concatenate([stage12[i, q].astype(F32) for i in range(8)], axis=0).astype(BF)

    def x3_send():
        for j in THREE:
            part = lambda s: w3.at[:, pl.ds(pl.multiple_of((2 * j + s) * 3 * lane, lane), 3 * lane)]
            send(part(1 - core), stage3.at[core, j], XS.at[6], X.at[6], sib)
            pltpu.make_async_copy(part(core), stage3.at[core, j], X.at[6]).start()

    def x3_blocks():
        take(stage3, X.at[6])
        n = rows // 3
        for j in THREE:
            both = jnp.concatenate([stage3[0, j].astype(F32), stage3[1, j].astype(F32)], axis=0)
            for c in THREE:
                own3[3 * j + c] = both[c * n:(c + 1) * n].astype(BF)

    def v_send(axis):
        if axis == 0:
            for o in range(1, 8):
                send(vec, V.at[cz, cy, spot], VS.at[0], VR.at[0], me - spot + lax.rem(spot + o, 8))
            pltpu.make_async_copy(vec, V.at[cz, cy, spot], VR.at[0]).start()
        elif axis == 1:
            take(V.at[0, 0], VR.at[0])
            for o in range(1, 4):
                send(V.at[cz, cy], V.at[cz, cy], VS.at[1], VR.at[1], me + (wrap(cy + o) - cy) * 8)
        else:
            take(V.at[0, pl.ds(0, 3)], VR.at[1])
            for o in range(1, 4):
                send(V.at[cz], V.at[cz], VS.at[2], VR.at[2], me + (wrap(cz + o) - cz) * 32)

    def spread(vals, at):
        n = at.size
        select = (lax.broadcasted_iota(jnp.int32, (LANES, n), 0) == tab[1:2, at]).astype(BF)
        return jnp.dot(vals, select, preferred_element_type=F32)

    def v_rows():
        take(V.at[ALL3], VR.at[2])
        nd = d // pair

        def body(t):
            at = pl.ds(pl.multiple_of(t * pair, pair), pair)
            m = spread(V[...].reshape(-1, LANES), at).reshape(LANES, 8, pair)
            dev = lax.broadcasted_iota(jnp.int32, m.shape, 0)
            v = jnp.sum(jnp.where(dev == tab[0:1, at][None], m, 0.0), axis=0)
            for i, src in enumerate((0, 1, 3, 4)):
                lnv[i, :, at] = v[src:src + 1]
            bout[t] = v[2:3]
            bdown[:, at] = v[5:6]
        loop(nd, body)
        dev = lax.broadcasted_iota(jnp.int32, (LANES, 8 * LANES), 0)
        slot = lax.broadcasted_iota(jnp.int32, (LANES, 8 * LANES), 1)
        for i in range(2):
            take_row = (slot == dev * 8 + 6 + i).astype(BF)
            vrow[i] = jnp.dot(take_row, V[...].reshape(-1, LANES), preferred_element_type=F32).astype(BF)

    def v_long(i, out, first, count):
        wide = 3 * pair

        def body(t):
            at = pl.ds(pl.multiple_of(first + t * wide, pair), wide)
            m = spread(vrow[i], at)
            dev = lax.broadcasted_iota(jnp.int32, m.shape, 0)
            v = jnp.sum(jnp.where(dev == tab[0:1, at], m, 0.0), axis=0, keepdims=True)
            for o in THREE:
                out[3 * t + o] = v[:, o * pair:(o + 1) * pair]
        loop(count, body)

    def issue(t):
        if t + 1 < CHUNKS:
            axis_first(t + 1, 1)
            axis_second(t + 1, 1)
        axis_first(t, 2)

    def visit1(t):
        if t >= 1:
            sides_in(t - 1)
            across_in(t - 1)
        if t + 2 < CHUNKS:
            p0_forward(t + 2)
        if t + 1 < CHUNKS:
            axis_forward(t + 1, 1)
        axis_second(t, 2)

    def visit2(t):
        axis_forward(t, 2)
        if t + 2 < CHUNKS:
            await_group(t + 2, 0, ACROSS)
        if t + 1 < CHUNKS:
            await_group(t + 1, 1, SECOND)
            await_group(t + 1, 1, ACROSS)
            if t + 3 in LATE:
                p0_send(t + 3)
            issue(t + 1)
        if t >= 1:
            await_siblings(t - 1, FIRST, SECOND, ACROSS)

    def load_cols(k, u, slot):
        x = u // 3
        c = lax.rem(u, 3)
        for s in range(2):
            g = (k * 2 + s) * 3 + c
            dst = wbuf.at[slot, :, :, :, pl.ds(s * lane, lane)]

            @pl.when(c == 0)
            def _():
                pltpu.make_async_copy(G12.at[g, :, :, x], dst, LS.at[slot]).start()

            @pl.when(c == 1)
            def _():
                pltpu.make_async_copy(G12.at[g, x], dst, LS.at[slot]).start()

            @pl.when(c > 1)
            def _():
                for y in range(4):
                    pltpu.make_async_copy(
                        G12.at[g, y, x], wbuf.at[slot, :, y, :, pl.ds(s * lane, lane)], LS.at[slot]).start()

    def load_rows(k, c, z, slot):
        for s in range(2):
            g = ((k - 6) * 2 + s) * 3 + c
            pltpu.make_async_copy(
                G3.at[g, z], wbuf3.at[slot, :, :, :, pl.ds(s * 3 * lane, 3 * lane)], LS.at[slot]).start()

    def run_units(load, k, body, lo=0, hi=UNITS):
        load(k, lo, lo % SLOTS)
        load(k, lo + 1, (lo + 1) % SLOTS)

        def step(u):
            slot = lax.rem(u, SLOTS)
            take(wbuf.at[slot], LS.at[slot])

            @pl.when(u + 2 < hi)
            def _():
                load(k, u + 2, lax.rem(u + 2, SLOTS))
            body(u, slot)
        loop(hi, step, lo)

    def weight(slot):
        return wbuf[slot].reshape(d, pair)

    def qkv_unit(k):
        def body(u, slot):
            p = 12 * k + u
            r = jnp.dot(h[...], weight(slot), preferred_element_type=F32) + bqkv[p]
            t = r.astype(BF).T
            row = pl.multiple_of(p * pair, pair)

            @pl.when(p < 9)
            def _():
                qt[pl.ds(row, pair), :] = t

            @pl.when(p >= 9)
            def _():
                kv_ref[pl.ds(pl.multiple_of(row - d, pair), pair), :] = t
        return body

    def out_unit(u, slot):
        p = u - 3
        cols = pl.ds(pl.multiple_of(p * pair, pair), pair)
        r = jnp.dot(ctx[...], weight(slot), preferred_element_type=F32)
        x1[:, cols] = (x_ref[:, cols].astype(F32) + r + bout[p]).astype(BF)

    def up_unit(k):
        def body(u, slot):
            p = 12 * (k - 3) + u
            cols = pl.ds(pl.multiple_of(p * pair, pair), pair)
            r = jnp.dot(h[...], weight(slot), preferred_element_type=F32) + bup[p]
            a[:, cols] = jax.nn.gelu(r, approximate=True).astype(BF)
        return body

    def run_down(k, lo=0, hi=UNITS):
        order = lambda o: jnp.where(o == 2, 3, jnp.where(o == 3, 2, o))
        n = 16 * (rows // 3)

        def split(u):
            c = lax.rem(u, 3)
            _, _, i2 = place(c)
            return c, wrap(i2 + order(u // 3))

        def load(u):
            c, z = split(u)
            load_rows(k, c, z, lax.rem(u, SLOTS))
        load(lo)
        load(lo + 1)

        def step(u):
            slot = lax.rem(u, SLOTS)
            take(wbuf3.at[slot], LS.at[slot])

            @pl.when(u + 2 < hi)
            def _():
                load(u + 2)
            c, z = split(u)
            at = pl.ds(pl.multiple_of((c * 4 + z) * n, lane), n)
            r = jnp.dot(a[:, at], wbuf3[slot].reshape(n, 6 * lane), preferred_element_type=F32)

            @pl.when(u == 0)
            def _():
                acc[...] = r

            @pl.when(u > 0)
            def _():
                acc[...] += r
        loop(hi, step, lo)
        if hi == UNITS:
            cols = slice((k - 6) * 6 * lane, (k - 5) * 6 * lane)
            y_ref[:, cols] = (x1[:, cols].astype(F32) + acc[...] + bdown[:, cols]).astype(BF)

    def norm(src, which):
        n = seq // 8

        def step(b):
            at = pl.ds(pl.multiple_of(b * n, n), n)
            v = src[at, :].astype(F32)
            v = v - jnp.mean(v, axis=-1, keepdims=True)
            var = jnp.mean(v * v, axis=-1, keepdims=True)
            h[at, :] = (v * lax.rsqrt(var + LN_EPS) * lnv[which] + lnv[which + 1]).astype(BF)
        loop(8, step)

    def attend(lo, hi):
        qb = seq // 2
        scale = hd ** -0.5

        def step(i):
            q_rows = pl.ds(pl.multiple_of(i * hd, hd), hd)
            k_rows = q_rows
            v_rows = pl.ds(pl.multiple_of(i * hd + d, hd), hd)
            for b in range(2):
                n = (b + 1) * qb
                q = qt[q_rows, b * qb:n]
                s = lax.dot_general(q, kv_ref[k_rows, :n], (((0,), (0,)), ((), ())),
                                    preferred_element_type=F32) * scale
                row = lax.broadcasted_iota(jnp.int32, (qb, n), 0) + b * qb
                col = lax.broadcasted_iota(jnp.int32, (qb, n), 1)
                s = jnp.where(col <= row, s, -jnp.inf)
                e = jnp.exp(s - jnp.max(s, axis=-1, keepdims=True))
                w = (e / jnp.sum(e, axis=-1, keepdims=True)).astype(BF)
                o = lax.dot_general(kv_ref[v_rows, :n], w, (((1,), (1,)), ((), ())),
                                    preferred_element_type=F32)
                ctxt[q_rows, b * qb:n] = o.astype(BF)
        loop(hi, step, lo)

    def flip():
        def step(i):
            at = pl.ds(pl.multiple_of(i * pair, pair), pair)
            ctx[:, at] = ctxt[at, :].T
        loop(d // pair, step)

    for k in THREE:
        x_send(k)
    v_send(0)
    x3_send()
    x_blocks(0)
    p0_send(0)
    for k in (1, 2):
        x_blocks(k)
        p0_send(k)
    p0_forward(0)
    x3_blocks()
    await_group(0, 0, ACROSS)
    axis_first(0, 1)
    axis_second(0, 1)
    p0_forward(1)
    p0_send(6)
    axis_forward(0, 1)
    p0_send(7)
    p0_send(8)
    await_group(1, 0, ACROSS)
    await_group(0, 1, SECOND)
    await_group(0, 1, ACROSS)
    issue(0)
    for k in LATE:
        x_send(k)
    v_send(1)
    visit1(0)
    v_send(2)
    for k in LATE:
        x_blocks(k)
    visit2(0)
    v_rows()
    norm(x_ref, 0)
    visit1(1)
    v_long(0, bqkv, d, 9)
    visit2(1)
    run_units(load_cols, 0, qkv_unit(0))
    visit1(2)
    v_long(1, bup, 4 * d, 12)
    visit2(2)
    run_units(load_cols, 1, qkv_unit(1))
    visit1(3)
    visit2(3)
    run_units(load_cols, 2, qkv_unit(2), hi=3)
    a1 = heads * 5 // 12
    a2 = heads * 9 // 12
    attend(0, a1)
    visit1(4)
    attend(a1, a2)
    visit2(4)
    attend(a2, heads)
    flip()
    run_units(load_cols, 2, out_unit, 3)
    visit1(5)
    norm(x1, 2)
    run_units(load_cols, 3, up_unit(3))
    visit2(5)
    run_units(load_cols, 4, up_unit(4))
    visit1(6)
    visit2(6)
    run_units(load_cols, 5, up_unit(5))
    visit1(7)
    visit2(7)
    run_down(6)
    visit1(8)
    visit2(8)
    run_down(7)
    await_siblings(8, FIRST)
    run_down(8, 0, 3)
    sides_in(8)
    await_siblings(8, SECOND)
    run_down(8, 3, 9)
    across_in(8)
    await_siblings(8, ACROSS)
    run_down(8, 9)

    for k in range(CHUNKS):
        ref = Block(k).ref
        for p in THREE:
            take(ref.at[(ALL3,) + ZEROS[:2 - p] + (ALL3,)], S.at[k, p])
        take(ref.at[ALL3], S.at[k, SIBLING])
    for k in range(6):
        take(stage12.at[pl.ds(0, 7), pl.ds(3 * k, 3)], XS.at[k])
    take(stage3.at[0], XS.at[6])
    take(V.at[0, 0, pl.ds(0, 7)], VS.at[0])
    take(V.at[0, ALL3], VS.at[1])
    take(V.at[ALL3], VS.at[2])


def solution(mesh):
    batch_axes = ('dp', 'fsdp')

    def local_layer(prompts, ln1_gain, ln1_bias, w_qkv, b_qkv, w_out, b_out, ln2_gain, ln2_bias, w_up, b_up, w_down, b_down):
        _, seq, d = prompts.shape
        heads, hd = w_qkv.shape[2], w_qkv.shape[3]
        lane = d // 18
        rows = d // 16
        pair = 2 * lane
        third = rows // 3
        r = w_up.shape[0]

        parts = [ln1_gain, ln1_bias, b_out, ln2_gain, ln2_bias, b_down, b_qkv, b_up]
        vec = jnp.stack([jnp.pad(p, (0, 128 - p.shape[0])) for p in parts]).astype(BF)

        orders = ((0, 1, 2), (2, 0, 1), (1, 2, 0))

        def reorder(m):
            m = m.reshape(-1, 4, 4, 4, 3, third)
            return [m[:, :, :, :, c].transpose((0,) + tuple(1 + o for o in orders[c]) + (4,)).reshape(m.shape[0], -1)
                    for c in THREE]

        w1 = jnp.concatenate([w_qkv.reshape(r, -1), w_out], axis=1)
        w2 = jnp.concatenate(reorder(w_up), axis=1)

        hidden = np.arange(4 * d).reshape(4, 4, 4, 3, third)
        hidden = np.concatenate([hidden[:, :, :, c].transpose(orders[c] + (3,)).reshape(-1) for c in THREE])
        index = [(np.arange(d), d // 128), (np.arange(3 * d), 3 * d // 128), (hidden, 4 * d // 128)]
        tab = np.stack([np.concatenate([i // n for i, n in index]), np.concatenate([i % n for i, n in index])])

        dims = (seq, d, heads, hd, rows, lane)
        vm = pl.BlockSpec(memory_space=pltpu.VMEM)
        hbm = pl.BlockSpec(memory_space=pl.ANY)
        dma = pltpu.SemaphoreType.DMA
        act, act_t = pltpu.VMEM((seq, d), BF), pltpu.VMEM((d, seq), BF)
        y, kv, _, _ = pl.pallas_call(
            functools.partial(layer_kernel, dims),
            out_shape=(
                pltpu.VMEM((seq, d), BF),
                pltpu.VMEM((2 * d, seq), BF),
                jax.ShapeDtypeStruct((36, 4, 4, 4, rows, lane), BF),
                jax.ShapeDtypeStruct((18, 4, 4, 4, third, 3 * lane), BF),
            ),
            in_specs=[vm] * 6,
            out_specs=(vm, vm, hbm, hbm),
            scratch_shapes=[
                act, act_t, act_t, act, act,
                pltpu.VMEM((seq, 4 * d), BF),
                pltpu.VMEM((SLOTS, 4, 4, rows, pair), BF),
                pltpu.VMEM((SLOTS, 4, 4, third, 6 * lane), BF),
                pltpu.VMEM((seq, 6 * lane), F32),
                pltpu.VMEM((18, rows, lane), BF),
                pltpu.VMEM((9, third, 3 * lane), BF),
                pltpu.VMEM((8, 18, r, lane), BF),
                pltpu.VMEM((2, 3, w_down.shape[0], 3 * lane), BF),
                pltpu.VMEM((4, 4, 8, 8, 128), BF),
                pltpu.VMEM((4, 1, d), F32),
                pltpu.VMEM((27, 1, pair), F32),
                pltpu.VMEM((9, 1, pair), F32),
                pltpu.VMEM((36, 1, pair), F32),
                pltpu.VMEM((1, d), F32),
                pltpu.VMEM((2, 128, 128), BF),
                dma((3 * CHUNKS, 4, 3)),
                dma((CHUNKS, 4)),
                dma((SLOTS,)),
                dma((CHUNKS,)),
                dma((7,)),
                dma((7,)),
                dma((3,)),
                dma((3,)),
            ],
            compiler_params=pltpu.CompilerParams(
                has_side_effects=True, vmem_limit_bytes=50 << 20),
            name="layer",
        )(prompts[0], w1, w2, w_down, vec, jnp.asarray(tab, jnp.int32))
        kc, vc = (m.reshape(heads, hd, seq).transpose(2, 0, 1)[None] for m in (kv[:d], kv[d:]))
        return y[None], kc, vc

    weight_spec = P('fsdp')
    return jax.shard_map(local_layer, mesh=mesh, in_specs=(P(batch_axes),) + (weight_spec,) * 12, out_specs=(P(batch_axes), P(batch_axes), P(batch_axes)), check_vma=False)
```

```python
import functools

import jax
import jax.numpy as jnp
import numpy as np
from jax import lax
from jax.experimental import pallas as pl
from jax.experimental.pallas import tpu as pltpu
from jax.sharding import PartitionSpec as P

LN_EPS = 1e-5
MESH = pl.DeviceIdType.MESH
BF = jnp.bfloat16
F32 = jnp.float32
CHUNKS = 9
SLOTS = 3
LO, HI, ALL3 = pl.ds(0, 2), pl.ds(2, 2), pl.ds(0, 3)
FIRST, SECOND, ACROSS, SIBLING = range(4)
ZEROS = (0, 0, 0)
THREE = range(3)
UNITS = 12
QKV = 9
LINE = 8
LANES = 128
LATE = (3, 4, 5)


def loop(hi, body, lo=0):
    def step(i, carry):
        body(i)
        return carry
    lax.fori_loop(lo, hi, step, None)


def wrap(i):
    return lax.rem(i, 4)


def layer_kernel(dims, x_hbm, wq, wo, w2, w3, tab, *refs):
    vecs, (y_ref, kv_ref, G12, G3), refs = refs[:8], refs[8:12], refs[12:]
    (x_ref, h, qt, ctxt, ctx, x1, a, wbuf, wbuf3, acc, own12, own3, w2p, stage12, stage3, vec32, vec, V, lnv, bqkv, bout,
     bup, bdown, vrow, R, S, LS, OS, X, XS, VR, VS) = refs
    seq, d, heads, hd, rows, lane = dims
    pair = 2 * lane
    me = lax.axis_index("fsdp")
    core = lax.rem(me, 2)
    cx = wrap(me // 2)
    cy = wrap(me // 8)
    cz = me // 32
    sib = me + 1 - 2 * core
    spot = lax.rem(me, LINE)
    line = [me - spot + lax.rem(spot + o, LINE) for o in range(1, LINE)]
    column = [me + (wrap(cy + o) - cy) * 8 for o in range(1, 4)]
    pillar = [me + (wrap(cz + o) - cz) * 32 for o in range(1, 4)]

    barrier = pltpu.get_barrier_semaphore()
    partners = line + column + pillar
    for dev in partners:
        pl.semaphore_signal(barrier, inc=1, device_id={"fsdp": dev}, device_id_type=MESH)

    class Block:
        def __init__(self, k):
            self.ref = G12 if k < 6 else G3
            self.base = k if k < 6 else k - 6

        def slab(self, c):
            return (self.base * 2 + core) * 3 + c

        def own(self, c):
            return (own12 if self.ref is G12 else own3).at[self.base * 3 + c]

    def pick(c, v):
        return jnp.where(c == 0, v[0], jnp.where(c == 1, v[1], v[2]))

    def place(c):
        v = (cx, cy, cz)
        return tuple(pick(c, v[p:] + v[:p]) for p in THREE)

    def near(c, p):
        v = (2, 8, 32)
        stride = pick(c, v[p:] + v[:p])
        i = place(c)[p]
        up, down = wrap(i + 1), wrap(i + 3)
        return me + (up - i) * stride, me + (down - i) * stride, up, down

    def send(src, dst, s, r, dev):
        pltpu.make_async_remote_copy(
            src_ref=src, dst_ref=dst, send_sem=s, recv_sem=r,
            device_id={"fsdp": dev}, device_id_type=MESH).start()

    def take(ref, sem):
        pltpu.make_async_copy(ref, ref, sem).wait()

    def colours(body):
        loop(3, body)

    def await_group(k, p, role, n=None):
        B = Block(k)

        def body(c):
            at = (B.slab(c),) + ZEROS[:3 - p]
            if n is not None:
                at = at[:-1] + (n,)
            take(B.ref.at[at], R.at[k * 3 + c, p, role])
        colours(body)

    def await_siblings(k, *roles):
        for role in roles:
            B = Block(k)
            part = LO if role == SECOND else 0
            colours(lambda c: take(B.ref.at[B.slab(c), part], R.at[k * 3 + c, SIBLING, role]))

    def p0_send(k):
        B = Block(k)

        def body(c):
            i0, i1, i2 = place(c)
            right, left, _, _ = near(c, 0)
            dst = B.ref.at[B.slab(c), i2, i1, i0]
            for dev in (right, left):
                send(B.own(c), dst, S.at[k, 0], R.at[k * 3 + c, 0, FIRST], dev)
            pltpu.make_async_copy(B.own(c), dst, OS.at[k]).start()
        colours(body)

    def p0_forward(k):
        B = Block(k)
        take(B.ref.at[0, 0, 0, ALL3], OS.at[k])
        await_group(k, 0, FIRST, LO)

        def body(c):
            i0, i1, i2 = place(c)
            right, left, up, down = near(c, 0)
            from_, to = (down, right) if k % 2 == 0 else (up, left)
            blk = B.ref.at[B.slab(c), i2, i1, from_]
            send(blk, blk, S.at[k, 0], R.at[k * 3 + c, 0, ACROSS], to)
        colours(body)

    def halves(k, c, p, i):
        B = Block(k)
        at = (B.slab(c), place(c)[2], i) if p == 1 else (B.slab(c), i)
        return B.ref.at[at + (LO,)], B.ref.at[at + (HI,)]

    def to_sibling(k, c, ahead, role):
        B = Block(k)
        part = B.ref.at[B.slab(c), wrap(place(c)[2] + ahead)]
        send(part, part, S.at[k, SIBLING], R.at[k * 3 + c, SIBLING, role], sib)

    def axis_first(k, p):
        def body(c):
            right, left, _, _ = near(c, p)
            lo, hi = halves(k, c, p, place(c)[p])
            send(lo, lo, S.at[k, p], R.at[k * 3 + c, p, FIRST], right)
            send(hi, hi, S.at[k, p], R.at[k * 3 + c, p, FIRST], left)
            if p == 2:
                to_sibling(k, c, 0, FIRST)
        colours(body)

    def axis_second(k, p):
        def body(c):
            right, left, _, _ = near(c, p)
            lo, hi = halves(k, c, p, place(c)[p])
            send(hi, hi, S.at[k, p], R.at[k * 3 + c, p, SECOND], right)
            send(lo, lo, S.at[k, p], R.at[k * 3 + c, p, SECOND], left)
        colours(body)

    def axis_forward(k, p):
        await_group(k, p, FIRST)

        def body(c):
            right, left, up, down = near(c, p)
            lo, hi = halves(k, c, p, down)[0], halves(k, c, p, up)[1]
            send(lo, lo, S.at[k, p], R.at[k * 3 + c, p, ACROSS], right)
            send(hi, hi, S.at[k, p], R.at[k * 3 + c, p, ACROSS], left)
        colours(body)

    def sides_in(k):
        await_group(k, 2, SECOND)

        def body(c):
            to_sibling(k, c, 1, SECOND)
            to_sibling(k, c, 3, SECOND)
        colours(body)

    def across_in(k):
        await_group(k, 2, ACROSS)
        colours(lambda c: to_sibling(k, c, 2, ACROSS))

    share = QKV * lane

    def x_send(m, lo, n):
        at = stage12.at[m, spot, :, pl.ds(lo, n)]

        def give(src, i, dev):
            part = src.at[:, pl.ds(pl.multiple_of(i * share + lo, lane), n)]
            sem = 2 * m + (lo > 0)
            if dev is None:
                pltpu.make_async_copy(part, at, X.at[sem]).start()
            else:
                send(part, at, XS.at[sem], X.at[sem], dev)

        def route(i, dev):
            if m:
                give(w2p, i, dev)
                return

            @pl.when(i < 6)
            def _():
                give(wq, i, dev)

            @pl.when(i >= 6)
            def _():
                give(wo, i - 6, dev)
        for dev in line:
            route(lax.rem(dev, LINE), dev)
        route(spot, None)

    def x_wait(m, lo, n):
        take(stage12.at[m, :, :, pl.ds(lo, n)], X.at[2 * m + (lo > 0)])

    def x_blocks(k):
        for c in THREE:
            lanes = pl.ds((3 * (k % 3) + c) * lane, lane)
            own12[3 * k + c] = jnp.concatenate(
                [stage12[k // 3, i, :, lanes].astype(F32) for i in range(LINE)], axis=0).astype(BF)

    def x3_send():
        part = lambda s: w3.at[:, pl.ds(pl.multiple_of(s * share, lane), share)]
        send(part(1 - core), stage3.at[core], XS.at[4], X.at[4], sib)
        pltpu.make_async_copy(part(core), stage3.at[core], X.at[4]).start()

    def x3_blocks():
        take(stage3, X.at[4])
        n = rows // 3
        for j in THREE:
            lanes = slice(3 * j * lane, 3 * (j + 1) * lane)
            both = jnp.concatenate([stage3[s, :, lanes].astype(F32) for s in range(2)], axis=0)
            for c in THREE:
                own3[3 * j + c] = both[c * n:(c + 1) * n].astype(BF)

    def permute_up():
        n = rows // 3
        for c in THREE:
            v = (1, 4, 16)
            s0, s1, s2 = v[c:] + v[:c]
            for i in range(4):
                chips = [i * s2 + j * s1 + k * s0 for j in range(4) for k in range(4)]
                groups = [w2[:, q * rows + c * n:q * rows + (c + 1) * n].astype(F32) for q in chips]
                w2p[:, (4 * c + i) * 16 * n:(4 * c + i + 1) * 16 * n] = jnp.concatenate(groups, axis=1).astype(BF)

    def v_pack():
        vec32[...] = jnp.zeros_like(vec32)
        for i, ref in enumerate(vecs):
            vec32[i:i + 1, 0:ref.shape[1]] = ref[...].astype(F32)
        vec[...] = vec32[...].astype(BF)

    def v_send(axis):
        if axis == 0:
            part = V.at[cz, cy, spot]
            for dev in line:
                send(vec, part, VS.at[0], VR.at[0], dev)
            pltpu.make_async_copy(vec, part, VR.at[0]).start()
        elif axis == 1:
            take(V.at[0, 0], VR.at[0])
            for dev in column:
                send(V.at[cz, cy], V.at[cz, cy], VS.at[1], VR.at[1], dev)
        else:
            take(V.at[0, ALL3], VR.at[1])
            for dev in pillar:
                send(V.at[cz], V.at[cz], VS.at[2], VR.at[2], dev)

    def spread(vals, at):
        n = at.size
        select = (lax.broadcasted_iota(jnp.int32, (LANES, n), 0) == tab[1:2, at]).astype(BF)
        return jnp.dot(vals, select, preferred_element_type=F32)

    def v_rows():
        take(V.at[ALL3], VR.at[2])
        nd = d // pair

        def body(t):
            at = pl.ds(pl.multiple_of(t * pair, pair), pair)
            m = spread(V[...].reshape(-1, LANES), at).reshape(LANES, LINE, pair)
            dev = lax.broadcasted_iota(jnp.int32, m.shape, 0)
            v = jnp.sum(jnp.where(dev == tab[0:1, at][None], m, 0.0), axis=0)
            for i, src in enumerate((0, 1, 3, 4)):
                lnv[i, :, at] = v[src:src + 1]
            for o in range(2):
                bout[2 * t + o] = v[2:3, o * lane:(o + 1) * lane]
            bdown[:, at] = v[5:6]
        loop(nd, body)
        dev = lax.broadcasted_iota(jnp.int32, (LANES, LINE * LANES), 0)
        slot = lax.broadcasted_iota(jnp.int32, (LANES, LINE * LANES), 1)
        for i in range(2):
            take_row = (slot == dev * LINE + 6 + i).astype(BF)
            vrow[i] = jnp.dot(take_row, V[...].reshape(-1, LANES), preferred_element_type=F32).astype(BF)

    def v_long(i, out, first, count):
        wide = 3 * pair

        def body(t):
            at = pl.ds(pl.multiple_of(first + t * wide, pair), wide)
            m = spread(vrow[i], at)
            dev = lax.broadcasted_iota(jnp.int32, m.shape, 0)
            v = jnp.sum(jnp.where(dev == tab[0:1, at], m, 0.0), axis=0, keepdims=True)
            for o in range(6):
                out[6 * t + o] = v[:, o * lane:(o + 1) * lane]
        loop(count, body)

    def issue(t):
        if t + 1 < CHUNKS:
            axis_first(t + 1, 1)
            axis_second(t + 1, 1)
        axis_first(t, 2)

    def visit1(t):
        last, ahead, far = t - 1, t + 1, t + 2
        if t:
            sides_in(last)
            across_in(last)
        if far < CHUNKS:
            p0_forward(far)
        if ahead < CHUNKS:
            axis_forward(ahead, 1)
        axis_second(t, 2)

    def visit2(t):
        last, ahead, far, farther = t - 1, t + 1, t + 2, t + 3
        axis_forward(t, 2)
        if far < CHUNKS:
            await_group(far, 0, ACROSS)
        if ahead < CHUNKS:
            for role in (SECOND, ACROSS):
                await_group(ahead, 1, role)
            if farther in LATE:
                p0_send(farther)
            issue(ahead)
        if t:
            await_siblings(last, FIRST, SECOND, ACROSS)

    def load_cols(k, u, slot):
        x = u // 3
        c = lax.rem(u, 3)
        for s in range(2):
            g = (k * 2 + s) * 3 + c
            dst = wbuf.at[slot, :, :, :, pl.ds(s * lane, lane)]

            @pl.when(c == 0)
            def _():
                pltpu.make_async_copy(G12.at[g, :, :, x], dst, LS.at[slot]).start()

            @pl.when(c == 1)
            def _():
                pltpu.make_async_copy(G12.at[g, x], dst, LS.at[slot]).start()

            @pl.when(c > 1)
            def _():
                for y in range(4):
                    pltpu.make_async_copy(
                        G12.at[g, y, x], wbuf.at[slot, :, y, :, pl.ds(s * lane, lane)], LS.at[slot]).start()

    def load_rows(k, c, z, slot):
        for s in range(2):
            g = ((k - 6) * 2 + s) * 3 + c
            pltpu.make_async_copy(
                G3.at[g, z], wbuf3.at[slot, :, :, :, pl.ds(s * 3 * lane, 3 * lane)], LS.at[slot]).start()

    def run_units(load, k, body, lo=0, hi=UNITS):
        load(k, lo, lo % SLOTS)
        load(k, lo + 1, (lo + 1) % SLOTS)

        def step(u):
            slot = lax.rem(u, SLOTS)
            take(wbuf.at[slot], LS.at[slot])

            @pl.when(u + 2 < hi)
            def _():
                load(k, u + 2, lax.rem(u + 2, SLOTS))
            body(u, slot)
        loop(hi, step, lo)

    def weight(slot):
        return wbuf[slot].reshape(d, pair)

    def tiles(k, u):
        first = 18 * (u // 3) + 3 * (k % 3) + lax.rem(u, 3)
        return first, first + QKV

    def span(t):
        return pl.ds(pl.multiple_of(t * lane, lane), lane)

    def both(r):
        return r[:, :lane], r[:, lane:]

    def qkv_unit(k):
        def body(u, slot):
            r = jnp.dot(h[...], weight(slot), preferred_element_type=F32)
            for t, v in zip(tiles(k, u), both(r)):
                v = (v + bqkv[t]).astype(BF).T

                @pl.when(t < 18)
                def _():
                    qt[span(t), :] = v

                @pl.when(t >= 18)
                def _():
                    kv_ref[span(t - 18), :] = v
        return body

    def out_unit(k):
        def body(u, slot):
            r = jnp.dot(ctx[...], weight(slot), preferred_element_type=F32)
            for t, v in zip(tiles(k, u - QKV), both(r)):
                x1[:, span(t)] = (x_ref[:, span(t)].astype(F32) + v + bout[t]).astype(BF)
        return body

    def up_unit(k):
        def body(u, slot):
            r = jnp.dot(h[...], weight(slot), preferred_element_type=F32)
            for t, v in zip(tiles(k, u), both(r)):
                a[:, span(t)] = jax.nn.gelu(v + bup[t], approximate=True).astype(BF)
        return body

    def run_down(k, lo=0, hi=UNITS):
        order = lambda o: jnp.where(o == 2, 3, jnp.where(o == 3, 2, o))
        n = 16 * (rows // 3)

        def split(u):
            c = lax.rem(u, 3)
            _, _, i2 = place(c)
            return c, wrap(i2 + order(u // 3))

        def load(u):
            c, z = split(u)
            load_rows(k, c, z, lax.rem(u, SLOTS))
        load(lo)
        load(lo + 1)

        def step(u):
            slot = lax.rem(u, SLOTS)
            take(wbuf3.at[slot], LS.at[slot])

            @pl.when(u + 2 < hi)
            def _():
                load(u + 2)
            c, z = split(u)
            at = pl.ds(pl.multiple_of((c * 4 + z) * n, lane), n)
            r = jnp.dot(a[:, at], wbuf3[slot].reshape(n, 6 * lane), preferred_element_type=F32)

            @pl.when(u == 0)
            def _():
                acc[...] = r

            @pl.when(u > 0)
            def _():
                acc[...] += r
        loop(hi, step, lo)
        if hi == UNITS:
            n = 3 * lane
            for s in range(2):
                cols = pl.ds(s * share + (k - 6) * n, n)
                y_ref[:, cols] = (x1[:, cols].astype(F32) + acc[:, s * n:(s + 1) * n] + bdown[:, cols]).astype(BF)

    def norm(src, which):
        n = seq // 8

        def step(b):
            at = pl.ds(pl.multiple_of(b * n, n), n)
            v = src[at, :].astype(F32)
            v = v - jnp.mean(v, axis=-1, keepdims=True)
            var = jnp.mean(v * v, axis=-1, keepdims=True)
            h[at, :] = (v * lax.rsqrt(var + LN_EPS) * lnv[which] + lnv[which + 1]).astype(BF)
        loop(8, step)

    def attend(lo, hi):
        qb = seq // 2
        scale = hd ** -0.5

        def step(i):
            q_rows = pl.ds(pl.multiple_of(i * hd, hd), hd)
            k_rows = q_rows
            v_rows = pl.ds(pl.multiple_of(i * hd + d, hd), hd)
            for b in range(2):
                n = (b + 1) * qb
                q = qt[q_rows, b * qb:n]
                s = lax.dot_general(q, kv_ref[k_rows, :n], (((0,), (0,)), ((), ())),
                                    preferred_element_type=F32) * scale
                row = lax.broadcasted_iota(jnp.int32, (qb, n), 0) + b * qb
                col = lax.broadcasted_iota(jnp.int32, (qb, n), 1)
                s = jnp.where(col <= row, s, -jnp.inf)
                e = jnp.exp(s - jnp.max(s, axis=-1, keepdims=True))
                w = (e / jnp.sum(e, axis=-1, keepdims=True)).astype(BF)
                o = lax.dot_general(kv_ref[v_rows, :n], w, (((1,), (1,)), ((), ())),
                                    preferred_element_type=F32)
                ctxt[q_rows, b * qb:n] = o.astype(BF)
        loop(hi, step, lo)

    def flip():
        def step(i):
            at = pl.ds(pl.multiple_of(i * pair, pair), pair)
            ctx[:, at] = ctxt[at, :].T
        loop(d // pair, step)

    x_copy = pltpu.make_async_copy(x_hbm, x_ref, OS.at[CHUNKS])
    x_copy.start()
    v_pack()
    pl.semaphore_wait(barrier, len(partners))
    early, rest, whole = (0, 3 * lane), (3 * lane, 6 * lane), (0, share)
    x_send(0, *early)
    x_send(0, *rest)
    x3_send()
    v_send(0)
    x_wait(0, *early)
    x_blocks(0)
    p0_send(0)
    x_wait(0, *rest)
    for k in (1, 2):
        x_blocks(k)
        p0_send(k)
    p0_forward(0)
    x3_blocks()
    await_group(0, 0, ACROSS)
    axis_first(0, 1)
    axis_second(0, 1)
    p0_forward(1)
    p0_send(6)
    axis_forward(0, 1)
    p0_send(7)
    p0_send(8)
    await_group(1, 0, ACROSS)
    await_group(0, 1, SECOND)
    await_group(0, 1, ACROSS)
    issue(0)
    permute_up()
    v_send(1)
    visit1(0)
    x_send(1, *whole)
    v_send(2)
    x_copy.wait()
    x_wait(1, *whole)
    for k in LATE:
        x_blocks(k)
    visit2(0)
    v_rows()
    norm(x_ref, 0)
    visit1(1)
    v_long(0, bqkv, d, 9)
    visit2(1)
    run_units(load_cols, 0, qkv_unit(0), hi=QKV)
    visit1(2)
    v_long(1, bup, 4 * d, 12)
    visit2(2)
    run_units(load_cols, 1, qkv_unit(1), hi=QKV)
    visit1(3)
    visit2(3)
    run_units(load_cols, 2, qkv_unit(2), hi=QKV)
    a1 = heads * 5 // UNITS
    a2 = heads * QKV // UNITS
    attend(0, a1)
    visit1(4)
    attend(a1, a2)
    visit2(4)
    attend(a2, heads)
    flip()
    for k in THREE:
        run_units(load_cols, k, out_unit(k), QKV)
    visit1(5)
    norm(x1, 2)
    run_units(load_cols, 3, up_unit(3))
    visit2(5)
    run_units(load_cols, 4, up_unit(4))
    visit1(6)
    visit2(6)
    run_units(load_cols, 5, up_unit(5))
    visit1(7)
    visit2(7)
    run_down(6)
    visit1(8)
    visit2(8)
    run_down(7)
    await_siblings(8, FIRST)
    run_down(8, 0, 3)
    sides_in(8)
    await_siblings(8, SECOND)
    run_down(8, 3, 9)
    across_in(8)
    await_siblings(8, ACROSS)
    run_down(8, 9)

    for k in range(CHUNKS):
        ref = Block(k).ref
        for p in THREE:
            take(ref.at[(ALL3,) + ZEROS[:2 - p] + (ALL3,)], S.at[k, p])
        take(ref.at[ALL3], S.at[k, SIBLING])
    for m, lo, n in ((0,) + early, (0,) + rest, (1,) + whole):
        take(stage12.at[m, pl.ds(0, 7), :, pl.ds(lo, n)], XS.at[2 * m + (lo > 0)])
    take(stage3.at[0], XS.at[4])
    take(V.at[0, 0, pl.ds(0, 7)], VS.at[0])
    take(V.at[0, ALL3], VS.at[1])
    take(V.at[ALL3], VS.at[2])


def solution(mesh):
    batch_axes = ('dp', 'fsdp')

    def local_layer(prompts, ln1_gain, ln1_bias, w_qkv, b_qkv, w_out, b_out, ln2_gain, ln2_bias, w_up, b_up, w_down, b_down):
        _, seq, d = prompts.shape
        heads, hd = w_qkv.shape[2], w_qkv.shape[3]
        lane = d // 18
        rows = d // 16
        pair = 2 * lane
        third = rows // 3
        r = w_up.shape[0]

        parts = [ln1_gain, ln1_bias, b_out, ln2_gain, ln2_bias, b_down, b_qkv, b_up]
        orders = ((0, 1, 2), (2, 0, 1), (1, 2, 0))

        hidden = np.arange(4 * d).reshape(4, 4, 4, 3, third)
        hidden = np.concatenate([hidden[:, :, :, c].transpose(orders[c] + (3,)).reshape(-1) for c in THREE])
        index = [(np.arange(d), d // 128), (np.arange(3 * d), 3 * d // 128), (hidden, 4 * d // 128)]
        tab = np.stack([np.concatenate([i // n for i, n in index]), np.concatenate([i % n for i, n in index])])

        dims = (seq, d, heads, hd, rows, lane)
        vm = pl.BlockSpec(memory_space=pltpu.VMEM)
        hbm = pl.BlockSpec(memory_space=pl.ANY)
        dma = pltpu.SemaphoreType.DMA
        act, act_t = pltpu.VMEM((seq, d), BF), pltpu.VMEM((d, seq), BF)
        y, kv, _, _ = pl.pallas_call(
            functools.partial(layer_kernel, dims),
            out_shape=(
                pltpu.VMEM((seq, d), BF),
                pltpu.VMEM((2 * d, seq), BF),
                jax.ShapeDtypeStruct((36, 4, 4, 4, rows, lane), BF),
                jax.ShapeDtypeStruct((18, 4, 4, 4, third, 3 * lane), BF),
            ),
            in_specs=[hbm] + [vm] * 13,
            out_specs=(vm, vm, hbm, hbm),
            scratch_shapes=[
                act, act, act_t, act_t, act, act,
                pltpu.VMEM((seq, 4 * d), BF),
                pltpu.VMEM((SLOTS, 4, 4, rows, pair), BF),
                pltpu.VMEM((SLOTS, 4, 4, third, 6 * lane), BF),
                pltpu.VMEM((seq, 6 * lane), F32),
                pltpu.VMEM((18, rows, lane), BF),
                pltpu.VMEM((9, third, 3 * lane), BF),
                pltpu.VMEM((r, 4 * d), BF),
                pltpu.VMEM((2, LINE, r, QKV * lane), BF),
                pltpu.VMEM((2, w_down.shape[0], QKV * lane), BF),
                pltpu.VMEM((LINE, LANES), F32),
                pltpu.VMEM((LINE, LANES), BF),
                pltpu.VMEM((4, 4, LINE, LINE, LANES), BF),
                pltpu.VMEM((4, 1, d), F32),
                pltpu.VMEM((54, 1, lane), F32),
                pltpu.VMEM((18, 1, lane), F32),
                pltpu.VMEM((72, 1, lane), F32),
                pltpu.VMEM((1, d), F32),
                pltpu.VMEM((2, LANES, LANES), BF),
                dma((3 * CHUNKS, 4, 3)),
                dma((CHUNKS, 4)),
                dma((SLOTS,)),
                dma((CHUNKS + 1,)),
                dma((5,)),
                dma((5,)),
                dma((3,)),
                dma((3,)),
            ],
            compiler_params=pltpu.CompilerParams(
                has_side_effects=True, collective_id=0, vmem_limit_bytes=50 << 20),
            name="layer",
        )(prompts[0], w_qkv.reshape(r, -1), w_out, w_up, w_down, jnp.asarray(tab, jnp.int32), *(p[None] for p in parts))
        kc, vc = (m.reshape(heads, hd, seq).transpose(2, 0, 1)[None] for m in (kv[:d], kv[d:]))
        return y[None], kc, vc

    weight_spec = P('fsdp')
    return jax.shard_map(local_layer, mesh=mesh, in_specs=(P(batch_axes),) + (weight_spec,) * 12, out_specs=(P(batch_axes), P(batch_axes), P(batch_axes)), check_vma=False)
```

```python
import functools

import jax
import jax.numpy as jnp
import numpy as np
from jax import lax
from jax.experimental import pallas as pl
from jax.experimental.pallas import tpu as pltpu
from jax.sharding import PartitionSpec as P

LN_EPS = 1e-5
MESH = pl.DeviceIdType.MESH
BF = jnp.bfloat16
F32 = jnp.float32
CHUNKS = 9
SLOTS = 3
LO, HI, ALL3 = pl.ds(0, 2), pl.ds(2, 2), pl.ds(0, 3)
FIRST, SECOND, ACROSS, SIBLING = range(4)
ZEROS = (0, 0, 0)
THREE = range(3)
UNITS = 12
QKV = 9
LINE = 8
LANES = 128
LATE = (3, 4, 5)


def loop(hi, body, lo=0):
    def step(i, carry):
        body(i)
        return carry
    lax.fori_loop(lo, hi, step, None)


def wrap(i):
    return lax.rem(i, 4)


def layer_kernel(dims, x_hbm, wq, wo, w2, w3, tab, *refs):
    vecs, (y_ref, kv_ref, G12, G3), refs = refs[:8], refs[8:12], refs[12:]
    (x_ref, h, qt, ctxt, ctx, x1, a, wbuf, wbuf3, acc, own12, own3, w2p, stage12, stage3, vec32, vec, V, lnv, bqkv, bout,
     bup, bdown, vrow, R, S, LS, OS, X, XS, VR, VS) = refs
    seq, d, heads, hd, rows, lane = dims
    pair = 2 * lane
    me = lax.axis_index("fsdp")
    core = lax.rem(me, 2)
    cx = wrap(me // 2)
    cy = wrap(me // 8)
    cz = me // 32
    sib = me + 1 - 2 * core
    spot = lax.rem(me, LINE)
    line = [me - spot + lax.rem(spot + o, LINE) for o in range(1, LINE)]
    column = [me + (wrap(cy + o) - cy) * 8 for o in range(1, 4)]
    pillar = [me + (wrap(cz + o) - cz) * 32 for o in range(1, 4)]

    barrier = pltpu.get_barrier_semaphore()
    partners = line + column + pillar
    for dev in partners:
        pl.semaphore_signal(barrier, inc=1, device_id={"fsdp": dev}, device_id_type=MESH)

    class Block:
        def __init__(self, k):
            self.ref = G12 if k < 6 else G3
            self.base = k if k < 6 else k - 6

        def slab(self, c):
            return (self.base * 2 + core) * 3 + c

        def own(self, c):
            return (own12 if self.ref is G12 else own3).at[self.base * 3 + c]

    def pick(c, v):
        return jnp.where(c == 0, v[0], jnp.where(c == 1, v[1], v[2]))

    def place(c):
        v = (cx, cy, cz)
        return tuple(pick(c, v[p:] + v[:p]) for p in THREE)

    def near(c, p):
        v = (2, 8, 32)
        stride = pick(c, v[p:] + v[:p])
        i = place(c)[p]
        up, down = wrap(i + 1), wrap(i + 3)
        return me + (up - i) * stride, me + (down - i) * stride, up, down

    def send(src, dst, s, r, dev):
        pltpu.make_async_remote_copy(
            src_ref=src, dst_ref=dst, send_sem=s, recv_sem=r,
            device_id={"fsdp": dev}, device_id_type=MESH).start()

    def take(ref, sem):
        pltpu.make_async_copy(ref, ref, sem).wait()

    def colours(body):
        loop(3, body)

    def await_group(k, p, role, n=None):
        B = Block(k)

        def body(c):
            at = (B.slab(c),) + ZEROS[:3 - p]
            if n is not None:
                at = at[:-1] + (n,)
            take(B.ref.at[at], R.at[k * 3 + c, p, role])
        colours(body)

    def await_siblings(k, *roles):
        for role in roles:
            B = Block(k)
            part = LO if role == SECOND else 0
            colours(lambda c: take(B.ref.at[B.slab(c), part], R.at[k * 3 + c, SIBLING, role]))

    def p0_send(k):
        B = Block(k)

        def body(c):
            i0, i1, i2 = place(c)
            right, left, _, _ = near(c, 0)
            dst = B.ref.at[B.slab(c), i2, i1, i0]
            for dev in (right, left):
                send(B.own(c), dst, S.at[k, 0], R.at[k * 3 + c, 0, FIRST], dev)
            pltpu.make_async_copy(B.own(c), dst, OS.at[k]).start()
        colours(body)

    def p0_forward(k):
        B = Block(k)
        take(B.ref.at[0, 0, 0, ALL3], OS.at[k])
        await_group(k, 0, FIRST, LO)

        def body(c):
            i0, i1, i2 = place(c)
            right, left, up, down = near(c, 0)
            from_, to = (down, right) if k % 2 == 0 else (up, left)
            blk = B.ref.at[B.slab(c), i2, i1, from_]
            send(blk, blk, S.at[k, 0], R.at[k * 3 + c, 0, ACROSS], to)
        colours(body)

    def halves(k, c, p, i):
        B = Block(k)
        at = (B.slab(c), place(c)[2], i) if p == 1 else (B.slab(c), i)
        return B.ref.at[at + (LO,)], B.ref.at[at + (HI,)]

    def to_sibling(k, c, ahead, role):
        B = Block(k)
        part = B.ref.at[B.slab(c), wrap(place(c)[2] + ahead)]
        send(part, part, S.at[k, SIBLING], R.at[k * 3 + c, SIBLING, role], sib)

    def axis_first(k, p):
        def body(c):
            right, left, _, _ = near(c, p)
            lo, hi = halves(k, c, p, place(c)[p])
            send(lo, lo, S.at[k, p], R.at[k * 3 + c, p, FIRST], right)
            send(hi, hi, S.at[k, p], R.at[k * 3 + c, p, FIRST], left)
            if p == 2:
                to_sibling(k, c, 0, FIRST)
        colours(body)

    def axis_second(k, p):
        def body(c):
            right, left, _, _ = near(c, p)
            lo, hi = halves(k, c, p, place(c)[p])
            send(hi, hi, S.at[k, p], R.at[k * 3 + c, p, SECOND], right)
            send(lo, lo, S.at[k, p], R.at[k * 3 + c, p, SECOND], left)
        colours(body)

    def axis_forward(k, p):
        await_group(k, p, FIRST)

        def body(c):
            right, left, up, down = near(c, p)
            lo, hi = halves(k, c, p, down)[0], halves(k, c, p, up)[1]
            send(lo, lo, S.at[k, p], R.at[k * 3 + c, p, ACROSS], right)
            send(hi, hi, S.at[k, p], R.at[k * 3 + c, p, ACROSS], left)
        colours(body)

    def sides_in(k):
        await_group(k, 2, SECOND)

        def body(c):
            to_sibling(k, c, 1, SECOND)
            to_sibling(k, c, 3, SECOND)
        colours(body)

    def across_in(k):
        await_group(k, 2, ACROSS)
        colours(lambda c: to_sibling(k, c, 2, ACROSS))

    share = QKV * lane

    def x_send(m, lo, n):
        at = stage12.at[m, spot, :, pl.ds(lo, n)]

        def give(src, i, dev):
            part = src.at[:, pl.ds(pl.multiple_of(i * share + lo, lane), n)]
            sem = 2 * m + (lo > 0)
            if dev is None:
                pltpu.make_async_copy(part, at, X.at[sem]).start()
            else:
                send(part, at, XS.at[sem], X.at[sem], dev)

        def route(i, dev):
            if m:
                give(w2p, i, dev)
                return

            @pl.when(i < 6)
            def _():
                give(wq, i, dev)

            @pl.when(i >= 6)
            def _():
                give(wo, i - 6, dev)
        for dev in line:
            route(lax.rem(dev, LINE), dev)
        route(spot, None)

    def x_wait(m, lo, n):
        take(stage12.at[m, :, :, pl.ds(lo, n)], X.at[2 * m + (lo > 0)])

    def x_blocks(k):
        for c in THREE:
            lanes = pl.ds((3 * (k % 3) + c) * lane, lane)
            own12[3 * k + c] = jnp.concatenate(
                [stage12[k // 3, i, :, lanes].astype(F32) for i in range(LINE)], axis=0).astype(BF)

    def x3_send():
        part = lambda s: w3.at[:, pl.ds(pl.multiple_of(s * share, lane), share)]
        send(part(1 - core), stage3.at[core], XS.at[4], X.at[4], sib)
        pltpu.make_async_copy(part(core), stage3.at[core], X.at[4]).start()

    def x3_blocks():
        take(stage3, X.at[4])
        n = rows // 3
        for j in THREE:
            lanes = slice(3 * j * lane, 3 * (j + 1) * lane)
            both = jnp.concatenate([stage3[s, :, lanes].astype(F32) for s in range(2)], axis=0)
            for c in THREE:
                own3[3 * j + c] = both[c * n:(c + 1) * n].astype(BF)

    def permute_up():
        n = rows // 3
        for c in THREE:
            v = (1, 4, 16)
            s0, s1, s2 = v[c:] + v[:c]
            for i in range(4):
                chips = [i * s2 + j * s1 + k * s0 for j in range(4) for k in range(4)]
                groups = [w2[:, q * rows + c * n:q * rows + (c + 1) * n].astype(F32) for q in chips]
                w2p[:, (4 * c + i) * 16 * n:(4 * c + i + 1) * 16 * n] = jnp.concatenate(groups, axis=1).astype(BF)

    def v_pack():
        vec32[...] = jnp.zeros_like(vec32)
        for i, ref in enumerate(vecs):
            vec32[i:i + 1, 0:ref.shape[1]] = ref[...].astype(F32)
        vec[...] = vec32[...].astype(BF)

    def v_send(axis):
        if axis == 0:
            part = V.at[cz, cy, spot]
            for dev in line:
                send(vec, part, VS.at[0], VR.at[0], dev)
            pltpu.make_async_copy(vec, part, VR.at[0]).start()
        elif axis == 1:
            take(V.at[0, 0], VR.at[0])
            for dev in column:
                send(V.at[cz, cy], V.at[cz, cy], VS.at[1], VR.at[1], dev)
        else:
            take(V.at[0, ALL3], VR.at[1])
            for dev in pillar:
                send(V.at[cz], V.at[cz], VS.at[2], VR.at[2], dev)

    def spread(vals, at):
        n = at.size
        select = (lax.broadcasted_iota(jnp.int32, (LANES, n), 0) == tab[1:2, at]).astype(BF)
        return jnp.dot(vals, select, preferred_element_type=F32)

    def v_rows():
        take(V.at[ALL3], VR.at[2])
        nd = d // pair

        def body(t):
            at = pl.ds(pl.multiple_of(t * pair, pair), pair)
            m = spread(V[...].reshape(-1, LANES), at).reshape(LANES, LINE, pair)
            dev = lax.broadcasted_iota(jnp.int32, m.shape, 0)
            v = jnp.sum(jnp.where(dev == tab[0:1, at][None], m, 0.0), axis=0)
            for i, src in enumerate((0, 1, 3, 4)):
                lnv[i, :, at] = v[src:src + 1]
            for o in range(2):
                bout[2 * t + o] = v[2:3, o * lane:(o + 1) * lane]
            bdown[:, at] = v[5:6]
        loop(nd, body)
        dev = lax.broadcasted_iota(jnp.int32, (LANES, LINE * LANES), 0)
        slot = lax.broadcasted_iota(jnp.int32, (LANES, LINE * LANES), 1)
        for i in range(2):
            take_row = (slot == dev * LINE + 6 + i).astype(BF)
            vrow[i] = jnp.dot(take_row, V[...].reshape(-1, LANES), preferred_element_type=F32).astype(BF)

    def v_long(i, out, first, count):
        wide = 3 * pair

        def body(t):
            at = pl.ds(pl.multiple_of(first + t * wide, pair), wide)
            m = spread(vrow[i], at)
            dev = lax.broadcasted_iota(jnp.int32, m.shape, 0)
            v = jnp.sum(jnp.where(dev == tab[0:1, at], m, 0.0), axis=0, keepdims=True)
            for o in range(6):
                out[6 * t + o] = v[:, o * lane:(o + 1) * lane]
        loop(count, body)

    def issue(t):
        if t + 1 < CHUNKS:
            axis_first(t + 1, 1)
            axis_second(t + 1, 1)
        axis_first(t, 2)

    def visit1(t):
        last, ahead, far = t - 1, t + 1, t + 2
        if t:
            sides_in(last)
            across_in(last)
        if far < CHUNKS:
            p0_forward(far)
        if ahead < CHUNKS:
            axis_forward(ahead, 1)
        axis_second(t, 2)

    def visit2(t):
        last, ahead, far, farther = t - 1, t + 1, t + 2, t + 3
        axis_forward(t, 2)
        if far < CHUNKS:
            await_group(far, 0, ACROSS)
        if ahead < CHUNKS:
            for role in (SECOND, ACROSS):
                await_group(ahead, 1, role)
            if farther in LATE:
                p0_send(farther)
            issue(ahead)
        if t:
            await_siblings(last, FIRST, SECOND, ACROSS)

    def load_cols(k, u, slot):
        x = u // 3
        c = lax.rem(u, 3)
        for s in range(2):
            g = (k * 2 + s) * 3 + c
            dst = wbuf.at[slot, :, :, :, pl.ds(s * lane, lane)]

            @pl.when(c == 0)
            def _():
                pltpu.make_async_copy(G12.at[g, :, :, x], dst, LS.at[slot]).start()

            @pl.when(c == 1)
            def _():
                pltpu.make_async_copy(G12.at[g, x], dst, LS.at[slot]).start()

            @pl.when(c > 1)
            def _():
                for y in range(4):
                    pltpu.make_async_copy(
                        G12.at[g, y, x], wbuf.at[slot, :, y, :, pl.ds(s * lane, lane)], LS.at[slot]).start()

    def load_rows(k, c, z, slot):
        for s in range(2):
            g = ((k - 6) * 2 + s) * 3 + c
            pltpu.make_async_copy(
                G3.at[g, z], wbuf3.at[slot, :, :, :, pl.ds(s * 3 * lane, 3 * lane)], LS.at[slot]).start()

    def run_units(load, k, body, lo=0, hi=UNITS):
        load(k, lo, lo % SLOTS)
        load(k, lo + 1, (lo + 1) % SLOTS)

        def step(u):
            slot = lax.rem(u, SLOTS)
            take(wbuf.at[slot], LS.at[slot])

            @pl.when(u + 2 < hi)
            def _():
                load(k, u + 2, lax.rem(u + 2, SLOTS))
            body(u, slot)
        loop(hi, step, lo)

    def weight(slot):
        return wbuf[slot].reshape(d, pair)

    def tiles(k, u):
        first = 18 * (u // 3) + 3 * (k % 3) + lax.rem(u, 3)
        return first, first + QKV

    def span(t):
        return pl.ds(pl.multiple_of(t * lane, lane), lane)

    def both(r):
        return r[:, :lane], r[:, lane:]

    def qkv_unit(k):
        def body(u, slot):
            r = jnp.dot(h[...], weight(slot), preferred_element_type=F32)
            for t, v in zip(tiles(k, u), both(r)):
                v = (v + bqkv[t]).astype(BF).T

                @pl.when(t < 18)
                def _():
                    qt[span(t), :] = v

                @pl.when(t >= 18)
                def _():
                    kv_ref[span(t - 18), :] = v
        return body

    def out_unit(k):
        def body(u, slot):
            r = jnp.dot(ctx[...], weight(slot), preferred_element_type=F32)
            for t, v in zip(tiles(k, u - QKV), both(r)):
                x1[:, span(t)] = (x_ref[:, span(t)].astype(F32) + v + bout[t]).astype(BF)
        return body

    def up_unit(k):
        def body(u, slot):
            r = jnp.dot(h[...], weight(slot), preferred_element_type=F32)
            for t, v in zip(tiles(k, u), both(r)):
                a[:, span(t)] = jax.nn.gelu(v + bup[t], approximate=True).astype(BF)
        return body

    def run_down(k, lo=0, hi=UNITS):
        order = lambda o: jnp.where(o == 2, 3, jnp.where(o == 3, 2, o))
        n = 16 * (rows // 3)

        def split(u):
            c = lax.rem(u, 3)
            _, _, i2 = place(c)
            return c, wrap(i2 + order(u // 3))

        def load(u):
            c, z = split(u)
            load_rows(k, c, z, lax.rem(u, SLOTS))
        load(lo)
        load(lo + 1)

        def step(u):
            slot = lax.rem(u, SLOTS)
            take(wbuf3.at[slot], LS.at[slot])

            @pl.when(u + 2 < hi)
            def _():
                load(u + 2)
            c, z = split(u)
            at = pl.ds(pl.multiple_of((c * 4 + z) * n, lane), n)
            r = jnp.dot(a[:, at], wbuf3[slot].reshape(n, 6 * lane), preferred_element_type=F32)

            @pl.when(u == 0)
            def _():
                acc[...] = r

            @pl.when(u > 0)
            def _():
                acc[...] += r
        loop(hi, step, lo)
        if hi == UNITS:
            n = 3 * lane
            for s in range(2):
                cols = pl.ds(s * share + (k - 6) * n, n)
                y_ref[:, cols] = (x1[:, cols].astype(F32) + acc[:, s * n:(s + 1) * n] + bdown[:, cols]).astype(BF)

    def norm(src, which):
        n = seq // 8

        def step(b):
            at = pl.ds(pl.multiple_of(b * n, n), n)
            v = src[at, :].astype(F32)
            v = v - jnp.mean(v, axis=-1, keepdims=True)
            var = jnp.mean(v * v, axis=-1, keepdims=True)
            h[at, :] = (v * lax.rsqrt(var + LN_EPS) * lnv[which] + lnv[which + 1]).astype(BF)
        loop(8, step)

    def attend(lo, hi):
        qb = seq // 2
        scale = hd ** -0.5

        def step(i):
            q_rows = pl.ds(pl.multiple_of(i * hd, hd), hd)
            k_rows = q_rows
            v_rows = pl.ds(pl.multiple_of(i * hd + d, hd), hd)
            for b in range(2):
                n = (b + 1) * qb
                q = qt[q_rows, b * qb:n]
                s = lax.dot_general(q, kv_ref[k_rows, :n], (((0,), (0,)), ((), ())),
                                    preferred_element_type=F32) * scale
                row = lax.broadcasted_iota(jnp.int32, (qb, n), 0) + b * qb
                col = lax.broadcasted_iota(jnp.int32, (qb, n), 1)
                s = jnp.where(col <= row, s, -jnp.inf)
                e = jnp.exp(s - jnp.max(s, axis=-1, keepdims=True))
                w = (e / jnp.sum(e, axis=-1, keepdims=True)).astype(BF)
                o = lax.dot_general(kv_ref[v_rows, :n], w, (((1,), (1,)), ((), ())),
                                    preferred_element_type=F32)
                ctxt[q_rows, b * qb:n] = o.astype(BF)
        loop(hi, step, lo)

    def flip():
        def step(i):
            at = pl.ds(pl.multiple_of(i * pair, pair), pair)
            ctx[:, at] = ctxt[at, :].T
        loop(d // pair, step)

    x_copy = pltpu.make_async_copy(x_hbm, x_ref, OS.at[CHUNKS])
    x_copy.start()
    v_pack()
    permute_up()
    pl.semaphore_wait(barrier, len(partners))
    early, rest, whole = (0, 3 * lane), (3 * lane, 6 * lane), (0, share)
    x_send(0, *early)
    x_send(0, *rest)
    x3_send()
    v_send(0)
    x_wait(0, *early)
    x_blocks(0)
    p0_send(0)
    x_wait(0, *rest)
    for k in (1, 2):
        x_blocks(k)
        p0_send(k)
    p0_forward(0)
    x3_blocks()
    await_group(0, 0, ACROSS)
    axis_first(0, 1)
    axis_second(0, 1)
    p0_forward(1)
    p0_send(6)
    axis_forward(0, 1)
    await_group(1, 0, ACROSS)
    axis_first(1, 1)
    axis_second(1, 1)
    x_send(1, *whole)
    v_send(1)
    p0_send(7)
    p0_send(8)
    await_group(0, 1, SECOND)
    await_group(0, 1, ACROSS)
    axis_first(0, 2)
    v_send(2)
    visit1(0)
    x_copy.wait()
    x_wait(1, *whole)
    for k in LATE:
        x_blocks(k)
    visit2(0)
    v_rows()
    norm(x_ref, 0)
    visit1(1)
    v_long(0, bqkv, d, 9)
    visit2(1)
    run_units(load_cols, 0, qkv_unit(0), hi=QKV)
    visit1(2)
    v_long(1, bup, 4 * d, 12)
    visit2(2)
    run_units(load_cols, 1, qkv_unit(1), hi=QKV)
    visit1(3)
    visit2(3)
    run_units(load_cols, 2, qkv_unit(2), hi=QKV)
    a1 = heads * 5 // UNITS
    a2 = heads * QKV // UNITS
    attend(0, a1)
    visit1(4)
    attend(a1, a2)
    visit2(4)
    attend(a2, heads)
    flip()
    for k in THREE:
        run_units(load_cols, k, out_unit(k), QKV)
    visit1(5)
    norm(x1, 2)
    run_units(load_cols, 3, up_unit(3))
    visit2(5)
    run_units(load_cols, 4, up_unit(4))
    visit1(6)
    visit2(6)
    run_units(load_cols, 5, up_unit(5))
    visit1(7)
    visit2(7)
    run_down(6)
    visit1(8)
    visit2(8)
    run_down(7)
    await_siblings(8, FIRST)
    run_down(8, 0, 3)
    sides_in(8)
    await_siblings(8, SECOND)
    run_down(8, 3, 9)
    across_in(8)
    await_siblings(8, ACROSS)
    run_down(8, 9)

    for k in range(CHUNKS):
        ref = Block(k).ref
        for p in THREE:
            take(ref.at[(ALL3,) + ZEROS[:2 - p] + (ALL3,)], S.at[k, p])
        take(ref.at[ALL3], S.at[k, SIBLING])
    for m, lo, n in ((0,) + early, (0,) + rest, (1,) + whole):
        take(stage12.at[m, pl.ds(0, 7), :, pl.ds(lo, n)], XS.at[2 * m + (lo > 0)])
    take(stage3.at[0], XS.at[4])
    take(V.at[0, 0, pl.ds(0, 7)], VS.at[0])
    take(V.at[0, ALL3], VS.at[1])
    take(V.at[ALL3], VS.at[2])


def solution(mesh):
    batch_axes = ('dp', 'fsdp')

    def local_layer(prompts, ln1_gain, ln1_bias, w_qkv, b_qkv, w_out, b_out, ln2_gain, ln2_bias, w_up, b_up, w_down, b_down):
        _, seq, d = prompts.shape
        heads, hd = w_qkv.shape[2], w_qkv.shape[3]
        lane = d // 18
        rows = d // 16
        pair = 2 * lane
        third = rows // 3
        r = w_up.shape[0]

        parts = [ln1_gain, ln1_bias, b_out, ln2_gain, ln2_bias, b_down, b_qkv, b_up]
        orders = ((0, 1, 2), (2, 0, 1), (1, 2, 0))

        hidden = np.arange(4 * d).reshape(4, 4, 4, 3, third)
        hidden = np.concatenate([hidden[:, :, :, c].transpose(orders[c] + (3,)).reshape(-1) for c in THREE])
        index = [(np.arange(d), d // 128), (np.arange(3 * d), 3 * d // 128), (hidden, 4 * d // 128)]
        tab = np.stack([np.concatenate([i // n for i, n in index]), np.concatenate([i % n for i, n in index])])

        dims = (seq, d, heads, hd, rows, lane)
        vm = pl.BlockSpec(memory_space=pltpu.VMEM)
        hbm = pl.BlockSpec(memory_space=pl.ANY)
        dma = pltpu.SemaphoreType.DMA
        act, act_t = pltpu.VMEM((seq, d), BF), pltpu.VMEM((d, seq), BF)
        y, kv, _, _ = pl.pallas_call(
            functools.partial(layer_kernel, dims),
            out_shape=(
                pltpu.VMEM((seq, d), BF),
                pltpu.VMEM((2 * d, seq), BF),
                jax.ShapeDtypeStruct((36, 4, 4, 4, rows, lane), BF),
                jax.ShapeDtypeStruct((18, 4, 4, 4, third, 3 * lane), BF),
            ),
            in_specs=[hbm] + [vm] * 13,
            out_specs=(vm, vm, hbm, hbm),
            scratch_shapes=[
                act, act, act_t, act_t, act, act,
                pltpu.VMEM((seq, 4 * d), BF),
                pltpu.VMEM((SLOTS, 4, 4, rows, pair), BF),
                pltpu.VMEM((SLOTS, 4, 4, third, 6 * lane), BF),
                pltpu.VMEM((seq, 6 * lane), F32),
                pltpu.VMEM((18, rows, lane), BF),
                pltpu.VMEM((9, third, 3 * lane), BF),
                pltpu.VMEM((r, 4 * d), BF),
                pltpu.VMEM((2, LINE, r, QKV * lane), BF),
                pltpu.VMEM((2, w_down.shape[0], QKV * lane), BF),
                pltpu.VMEM((LINE, LANES), F32),
                pltpu.VMEM((LINE, LANES), BF),
                pltpu.VMEM((4, 4, LINE, LINE, LANES), BF),
                pltpu.VMEM((4, 1, d), F32),
                pltpu.VMEM((54, 1, lane), F32),
                pltpu.VMEM((18, 1, lane), F32),
                pltpu.VMEM((72, 1, lane), F32),
                pltpu.VMEM((1, d), F32),
                pltpu.VMEM((2, LANES, LANES), BF),
                dma((3 * CHUNKS, 4, 3)),
                dma((CHUNKS, 4)),
                dma((SLOTS,)),
                dma((CHUNKS + 1,)),
                dma((5,)),
                dma((5,)),
                dma((3,)),
                dma((3,)),
            ],
            compiler_params=pltpu.CompilerParams(
                has_side_effects=True, collective_id=0, vmem_limit_bytes=50 << 20),
            name="layer",
        )(prompts[0], w_qkv.reshape(r, -1), w_out, w_up, w_down, jnp.asarray(tab, jnp.int32), *(p[None] for p in parts))
        kc, vc = (m.reshape(heads, hd, seq).transpose(2, 0, 1)[None] for m in (kv[:d], kv[d:]))
        return y[None], kc, vc

    weight_spec = P('fsdp')
    return jax.shard_map(local_layer, mesh=mesh, in_specs=(P(batch_axes),) + (weight_spec,) * 12, out_specs=(P(batch_axes), P(batch_axes), P(batch_axes)), check_vma=False)
```

```python
import functools

import jax
import jax.numpy as jnp
import numpy as np
from jax import lax
from jax.experimental import pallas as pl
from jax.experimental.pallas import tpu as pltpu
from jax.sharding import PartitionSpec as P

LN_EPS = 1e-5
MESH = pl.DeviceIdType.MESH
BF = jnp.bfloat16
F32 = jnp.float32
CHUNKS = 9
SLOTS = 3
LO, HI, ALL3 = pl.ds(0, 2), pl.ds(2, 2), pl.ds(0, 3)
FIRST, SECOND, ACROSS, SIBLING = range(4)
ZEROS = (0, 0, 0)
THREE = range(3)
UNITS = 12
QKV = 9
LINE = 8
SIDES = (1, 3)
QUARTERS = (0, *SIDES, ACROSS)
LAST = CHUNKS - 1
LANES = 128
LATE = (3, 4, 5)


def loop(hi, body, lo=0):
    def step(i, carry):
        body(i)
        return carry
    lax.fori_loop(lo, hi, step, None)


def wrap(i):
    return lax.rem(i, 4)


def layer_kernel(dims, x_hbm, wq, wo, w2, w3, tab, *refs):
    vecs, (y_ref, kv_ref, G12, G3), refs = refs[:8], refs[8:12], refs[12:]
    (x_ref, h, qt, ctxt, ctx, x1, a, wbuf, wbuf3, acc, own12, own3, w2p, stage12, stage3, vec32, vec, V, lnv, bqkv, bout,
     bup, bdown, vrow, R, S, LS, OS, X, XS, VR, VS) = refs
    seq, d, heads, hd, rows, lane = dims
    pair = 2 * lane
    me = lax.axis_index("fsdp")
    core = lax.rem(me, 2)
    cx = wrap(me // 2)
    cy = wrap(me // 8)
    cz = me // 32
    sib = me + 1 - 2 * core
    spot = lax.rem(me, LINE)
    line = [me - spot + lax.rem(spot + o, LINE) for o in range(1, LINE)]
    column = [me + (wrap(cy + o) - cy) * 8 for o in range(1, 4)]
    pillar = [me + (wrap(cz + o) - cz) * 32 for o in range(1, 4)]

    barrier = pltpu.get_barrier_semaphore()
    partners = line + column + pillar
    for dev in partners:
        pl.semaphore_signal(barrier, inc=1, device_id={"fsdp": dev}, device_id_type=MESH)

    class Block:
        def __init__(self, k):
            self.ref = G12 if k < 6 else G3
            self.base = k if k < 6 else k - 6

        def slab(self, c):
            return (self.base * 2 + core) * 3 + c

        def own(self, c):
            return (own12 if self.ref is G12 else own3).at[self.base * 3 + c]

    def pick(c, v):
        return jnp.where(c == 0, v[0], jnp.where(c == 1, v[1], v[2]))

    def place(c):
        v = (cx, cy, cz)
        return tuple(pick(c, v[p:] + v[:p]) for p in THREE)

    def near(c, p):
        v = (2, 8, 32)
        stride = pick(c, v[p:] + v[:p])
        i = place(c)[p]
        up, down = wrap(i + 1), wrap(i + 3)
        return me + (up - i) * stride, me + (down - i) * stride, up, down

    def send(src, dst, s, r, dev):
        pltpu.make_async_remote_copy(
            src_ref=src, dst_ref=dst, send_sem=s, recv_sem=r,
            device_id={"fsdp": dev}, device_id_type=MESH).start()

    def take(ref, sem):
        pltpu.make_async_copy(ref, ref, sem).wait()

    def colours(body):
        loop(3, body)

    def await_group(k, p, role, n=None):
        B = Block(k)

        def body(c):
            at = (B.slab(c),) + ZEROS[:3 - p]
            if n is not None:
                at = at[:-1] + (n,)
            take(B.ref.at[at], R.at[k * 3 + c, p, role])
        colours(body)

    def await_siblings(k, *quarters):
        B = Block(k)
        for ahead in quarters:
            colours(lambda c: take(B.ref.at[B.slab(c), 0], R.at[k * 3 + c, SIBLING, ahead]))

    def p0_send(k):
        B = Block(k)

        def body(c):
            i0, i1, i2 = place(c)
            right, left, _, _ = near(c, 0)
            dst = B.ref.at[B.slab(c), i2, i1, i0]
            for dev in (right, left):
                send(B.own(c), dst, S.at[k, 0], R.at[k * 3 + c, 0, FIRST], dev)
            pltpu.make_async_copy(B.own(c), dst, OS.at[k]).start()
        colours(body)

    def p0_forward(k):
        B = Block(k)
        take(B.ref.at[0, 0, 0, ALL3], OS.at[k])
        await_group(k, 0, FIRST, LO)

        def body(c):
            i0, i1, i2 = place(c)
            right, left, up, down = near(c, 0)
            from_, to = (down, right) if k % 2 == 0 else (up, left)
            blk = B.ref.at[B.slab(c), i2, i1, from_]
            send(blk, blk, S.at[k, 0], R.at[k * 3 + c, 0, ACROSS], to)
        colours(body)

    def halves(k, c, p, i):
        B = Block(k)
        at = (B.slab(c), place(c)[2], i) if p == 1 else (B.slab(c), i)
        return B.ref.at[at + (LO,)], B.ref.at[at + (HI,)]

    def to_sibling(k, c, ahead):
        B = Block(k)
        part = B.ref.at[B.slab(c), wrap(place(c)[2] + ahead)]
        send(part, part, S.at[k, SIBLING], R.at[k * 3 + c, SIBLING, ahead], sib)

    def axis_first(k, p):
        def body(c):
            right, left, _, _ = near(c, p)
            lo, hi = halves(k, c, p, place(c)[p])
            send(lo, lo, S.at[k, p], R.at[k * 3 + c, p, FIRST], right)
            send(hi, hi, S.at[k, p], R.at[k * 3 + c, p, FIRST], left)
            if p == 2:
                to_sibling(k, c, 0)
        colours(body)

    def axis_second(k, p):
        def body(c):
            right, left, _, _ = near(c, p)
            lo, hi = halves(k, c, p, place(c)[p])
            send(hi, hi, S.at[k, p], R.at[k * 3 + c, p, SECOND], right)
            send(lo, lo, S.at[k, p], R.at[k * 3 + c, p, SECOND], left)
        colours(body)

    def axis_forward(k, p):
        await_group(k, p, FIRST)

        def body(c):
            right, left, up, down = near(c, p)
            lo, hi = halves(k, c, p, down)[0], halves(k, c, p, up)[1]
            send(lo, lo, S.at[k, p], R.at[k * 3 + c, p, ACROSS], right)
            send(hi, hi, S.at[k, p], R.at[k * 3 + c, p, ACROSS], left)
        colours(body)

    def sides_in(k):
        await_group(k, 2, SECOND)

        for ahead in SIDES:
            colours(lambda c: to_sibling(k, c, ahead))

    def across_in(k):
        await_group(k, 2, ACROSS)
        colours(lambda c: to_sibling(k, c, ACROSS))

    share = QKV * lane

    def x_send(m, lo, n):
        at = stage12.at[m, spot, :, pl.ds(lo, n)]

        def give(src, i, dev):
            part = src.at[:, pl.ds(pl.multiple_of(i * share + lo, lane), n)]
            sem = 2 * m + (lo > 0)
            if dev is None:
                pltpu.make_async_copy(part, at, X.at[sem]).start()
            else:
                send(part, at, XS.at[sem], X.at[sem], dev)

        def route(i, dev):
            if m:
                give(w2p, i, dev)
                return

            @pl.when(i < 6)
            def _():
                give(wq, i, dev)

            @pl.when(i >= 6)
            def _():
                give(wo, i - 6, dev)
        for dev in line:
            route(lax.rem(dev, LINE), dev)
        route(spot, None)

    def x_wait(m, lo, n):
        take(stage12.at[m, :, :, pl.ds(lo, n)], X.at[2 * m + (lo > 0)])

    def x_blocks(k):
        for c in THREE:
            lanes = pl.ds((3 * (k % 3) + c) * lane, lane)
            own12[3 * k + c] = jnp.concatenate(
                [stage12[k // 3, i, :, lanes].astype(F32) for i in range(LINE)], axis=0).astype(BF)

    def x3_send():
        part = lambda s: w3.at[:, pl.ds(pl.multiple_of(s * share, lane), share)]
        send(part(1 - core), stage3.at[core], XS.at[4], X.at[4], sib)
        pltpu.make_async_copy(part(core), stage3.at[core], X.at[4]).start()

    def x3_blocks():
        take(stage3, X.at[4])
        n = rows // 3
        for j in THREE:
            lanes = slice(3 * j * lane, 3 * (j + 1) * lane)
            both = jnp.concatenate([stage3[s, :, lanes].astype(F32) for s in range(2)], axis=0)
            for c in THREE:
                own3[3 * j + c] = both[c * n:(c + 1) * n].astype(BF)

    def permute_up():
        n = rows // 3
        for c in THREE:
            v = (1, 4, 16)
            s0, s1, s2 = v[c:] + v[:c]
            for i in range(4):
                chips = [i * s2 + j * s1 + k * s0 for j in range(4) for k in range(4)]
                groups = [w2[:, q * rows + c * n:q * rows + (c + 1) * n].astype(F32) for q in chips]
                w2p[:, (4 * c + i) * 16 * n:(4 * c + i + 1) * 16 * n] = jnp.concatenate(groups, axis=1).astype(BF)

    def v_pack():
        vec32[...] = jnp.zeros_like(vec32)
        for i, ref in enumerate(vecs):
            vec32[i:i + 1, 0:ref.shape[1]] = ref[...].astype(F32)
        vec[...] = vec32[...].astype(BF)

    def v_send(axis):
        if axis == 0:
            part = V.at[cz, cy, spot]
            for dev in line:
                send(vec, part, VS.at[0], VR.at[0], dev)
            pltpu.make_async_copy(vec, part, VR.at[0]).start()
        elif axis == 1:
            take(V.at[0, 0], VR.at[0])
            for dev in column:
                send(V.at[cz, cy], V.at[cz, cy], VS.at[1], VR.at[1], dev)
        else:
            take(V.at[0, ALL3], VR.at[1])
            for dev in pillar:
                send(V.at[cz], V.at[cz], VS.at[2], VR.at[2], dev)

    def spread(vals, at):
        n = at.size
        select = (lax.broadcasted_iota(jnp.int32, (LANES, n), 0) == tab[1:2, at]).astype(BF)
        return jnp.dot(vals, select, preferred_element_type=F32)

    def v_rows():
        take(V.at[ALL3], VR.at[2])
        nd = d // pair

        def body(t):
            at = pl.ds(pl.multiple_of(t * pair, pair), pair)
            m = spread(V[...].reshape(-1, LANES), at).reshape(LANES, LINE, pair)
            dev = lax.broadcasted_iota(jnp.int32, m.shape, 0)
            v = jnp.sum(jnp.where(dev == tab[0:1, at][None], m, 0.0), axis=0)
            for i, src in enumerate((0, 1, 3, 4)):
                lnv[i, :, at] = v[src:src + 1]
            for o in range(2):
                bout[2 * t + o] = v[2:3, o * lane:(o + 1) * lane]
            bdown[:, at] = v[5:6]
        loop(nd, body)
        dev = lax.broadcasted_iota(jnp.int32, (LANES, LINE * LANES), 0)
        slot = lax.broadcasted_iota(jnp.int32, (LANES, LINE * LANES), 1)
        for i in range(2):
            take_row = (slot == dev * LINE + 6 + i).astype(BF)
            vrow[i] = jnp.dot(take_row, V[...].reshape(-1, LANES), preferred_element_type=F32).astype(BF)

    def v_long(i, out, first, count):
        wide = 3 * pair

        def body(t):
            at = pl.ds(pl.multiple_of(first + t * wide, pair), wide)
            m = spread(vrow[i], at)
            dev = lax.broadcasted_iota(jnp.int32, m.shape, 0)
            v = jnp.sum(jnp.where(dev == tab[0:1, at], m, 0.0), axis=0, keepdims=True)
            for o in range(6):
                out[6 * t + o] = v[:, o * lane:(o + 1) * lane]
        loop(count, body)

    def issue(t):
        if t + 1 < CHUNKS:
            axis_first(t + 1, 1)
            axis_second(t + 1, 1)
        axis_first(t, 2)

    def visit1(t):
        last, ahead, far = t - 1, t + 1, t + 2
        if t:
            if t < LAST:
                sides_in(last)
            across_in(last)
        if far < CHUNKS:
            p0_forward(far)
        if ahead < CHUNKS:
            axis_forward(ahead, 1)
        if t < LAST:
            axis_second(t, 2)

    def visit2(t):
        last, ahead, far, farther = t - 1, t + 1, t + 2, t + 3
        axis_forward(t, 2)
        if far < CHUNKS:
            await_group(far, 0, ACROSS)
        if ahead < CHUNKS:
            for role in (SECOND, ACROSS):
                await_group(ahead, 1, role)
            if farther in LATE:
                p0_send(farther)
            issue(ahead)
        if ahead == LAST:
            axis_second(LAST, 2)
        if t == LAST:
            await_siblings(last, ACROSS)
        elif t:
            await_siblings(last, *QUARTERS)

    def load_cols(k, u, slot):
        x = u // 3
        c = lax.rem(u, 3)
        for s in range(2):
            g = (k * 2 + s) * 3 + c
            dst = wbuf.at[slot, :, :, :, pl.ds(s * lane, lane)]

            @pl.when(c == 0)
            def _():
                pltpu.make_async_copy(G12.at[g, :, :, x], dst, LS.at[slot]).start()

            @pl.when(c == 1)
            def _():
                pltpu.make_async_copy(G12.at[g, x], dst, LS.at[slot]).start()

            @pl.when(c > 1)
            def _():
                for y in range(4):
                    pltpu.make_async_copy(
                        G12.at[g, y, x], wbuf.at[slot, :, y, :, pl.ds(s * lane, lane)], LS.at[slot]).start()

    def load_rows(k, c, z, slot):
        for s in range(2):
            g = ((k - 6) * 2 + s) * 3 + c
            pltpu.make_async_copy(
                G3.at[g, z], wbuf3.at[slot, :, :, :, pl.ds(s * 3 * lane, 3 * lane)], LS.at[slot]).start()

    def run_units(load, k, body, lo=0, hi=UNITS):
        load(k, lo, lo % SLOTS)
        load(k, lo + 1, (lo + 1) % SLOTS)

        def step(u):
            slot = lax.rem(u, SLOTS)
            take(wbuf.at[slot], LS.at[slot])

            @pl.when(u + 2 < hi)
            def _():
                load(k, u + 2, lax.rem(u + 2, SLOTS))
            body(u, slot)
        loop(hi, step, lo)

    def weight(slot):
        return wbuf[slot].reshape(d, pair)

    def tiles(k, u):
        first = 18 * (u // 3) + 3 * (k % 3) + lax.rem(u, 3)
        return first, first + QKV

    def span(t):
        return pl.ds(pl.multiple_of(t * lane, lane), lane)

    def both(r):
        return r[:, :lane], r[:, lane:]

    def qkv_unit(k):
        def body(u, slot):
            r = jnp.dot(h[...], weight(slot), preferred_element_type=F32)
            for t, v in zip(tiles(k, u), both(r)):
                v = (v + bqkv[t]).astype(BF).T

                @pl.when(t < 18)
                def _():
                    qt[span(t), :] = v

                @pl.when(t >= 18)
                def _():
                    kv_ref[span(t - 18), :] = v
        return body

    def out_unit(k):
        def body(u, slot):
            r = jnp.dot(ctx[...], weight(slot), preferred_element_type=F32)
            for t, v in zip(tiles(k, u - QKV), both(r)):
                x1[:, span(t)] = (x_ref[:, span(t)].astype(F32) + v + bout[t]).astype(BF)
        return body

    def up_unit(k):
        def body(u, slot):
            r = jnp.dot(h[...], weight(slot), preferred_element_type=F32)
            for t, v in zip(tiles(k, u), both(r)):
                a[:, span(t)] = jax.nn.gelu(v + bup[t], approximate=True).astype(BF)
        return body

    def run_down(k, lo=0, hi=UNITS, known=UNITS, primed=False):
        order = lambda o: jnp.where(o == 2, 3, jnp.where(o == 3, 2, o))
        n = 16 * (rows // 3)

        def split(u):
            c = lax.rem(u, 3)
            _, _, i2 = place(c)
            return c, wrap(i2 + order(u // 3))

        def load(u):
            c, z = split(u)
            load_rows(k, c, z, lax.rem(u, SLOTS))
        if not primed:
            load(lo)
            load(lo + 1)

        def step(u):
            slot = lax.rem(u, SLOTS)
            take(wbuf3.at[slot], LS.at[slot])

            @pl.when(u + 2 < known)
            def _():
                load(u + 2)
            c, z = split(u)
            at = pl.ds(pl.multiple_of((c * 4 + z) * n, lane), n)
            r = jnp.dot(a[:, at], wbuf3[slot].reshape(n, 6 * lane), preferred_element_type=F32)

            @pl.when(u == 0)
            def _():
                acc[...] = r

            @pl.when(u > 0)
            def _():
                acc[...] += r
        loop(hi, step, lo)
        if hi == UNITS:
            n = 3 * lane
            for s in range(2):
                cols = pl.ds(s * share + (k - 6) * n, n)
                y_ref[:, cols] = (x1[:, cols].astype(F32) + acc[:, s * n:(s + 1) * n] + bdown[:, cols]).astype(BF)

    def norm(src, which):
        n = seq // 8

        def step(b):
            at = pl.ds(pl.multiple_of(b * n, n), n)
            v = src[at, :].astype(F32)
            v = v - jnp.mean(v, axis=-1, keepdims=True)
            var = jnp.mean(v * v, axis=-1, keepdims=True)
            h[at, :] = (v * lax.rsqrt(var + LN_EPS) * lnv[which] + lnv[which + 1]).astype(BF)
        loop(8, step)

    def attend(lo, hi):
        qb = seq // 2
        scale = hd ** -0.5

        def step(i):
            q_rows = pl.ds(pl.multiple_of(i * hd, hd), hd)
            k_rows = q_rows
            v_rows = pl.ds(pl.multiple_of(i * hd + d, hd), hd)
            for b in range(2):
                n = (b + 1) * qb
                q = qt[q_rows, b * qb:n]
                s = lax.dot_general(q, kv_ref[k_rows, :n], (((0,), (0,)), ((), ())),
                                    preferred_element_type=F32) * scale
                row = lax.broadcasted_iota(jnp.int32, (qb, n), 0) + b * qb
                col = lax.broadcasted_iota(jnp.int32, (qb, n), 1)
                s = jnp.where(col <= row, s, -jnp.inf)
                e = jnp.exp(s - jnp.max(s, axis=-1, keepdims=True))
                w = (e / jnp.sum(e, axis=-1, keepdims=True)).astype(BF)
                o = lax.dot_general(kv_ref[v_rows, :n], w, (((1,), (1,)), ((), ())),
                                    preferred_element_type=F32)
                ctxt[q_rows, b * qb:n] = o.astype(BF)
        loop(hi, step, lo)

    def flip():
        def step(i):
            at = pl.ds(pl.multiple_of(i * pair, pair), pair)
            ctx[:, at] = ctxt[at, :].T
        loop(d // pair, step)

    x_copy = pltpu.make_async_copy(x_hbm, x_ref, OS.at[CHUNKS])
    x_copy.start()
    v_pack()
    permute_up()
    pl.semaphore_wait(barrier, len(partners))
    early, rest, whole = (0, 3 * lane), (3 * lane, 6 * lane), (0, share)
    x_send(0, *early)
    x_send(0, *rest)
    x3_send()
    v_send(0)
    x_wait(0, *early)
    x_blocks(0)
    p0_send(0)
    x_wait(0, *rest)
    for k in (1, 2):
        x_blocks(k)
        p0_send(k)
    p0_forward(0)
    x3_blocks()
    await_group(0, 0, ACROSS)
    axis_first(0, 1)
    axis_second(0, 1)
    p0_forward(1)
    p0_send(6)
    axis_forward(0, 1)
    await_group(1, 0, ACROSS)
    axis_first(1, 1)
    axis_second(1, 1)
    x_send(1, *whole)
    v_send(1)
    p0_send(7)
    p0_send(8)
    await_group(0, 1, SECOND)
    await_group(0, 1, ACROSS)
    axis_first(0, 2)
    v_send(2)
    visit1(0)
    x_copy.wait()
    x_wait(1, *whole)
    for k in LATE:
        x_blocks(k)
    visit2(0)
    v_rows()
    norm(x_ref, 0)
    visit1(1)
    v_long(0, bqkv, d, 9)
    visit2(1)
    run_units(load_cols, 0, qkv_unit(0), hi=QKV)
    visit1(2)
    v_long(1, bup, 4 * d, 12)
    visit2(2)
    run_units(load_cols, 1, qkv_unit(1), hi=QKV)
    visit1(3)
    visit2(3)
    run_units(load_cols, 2, qkv_unit(2), hi=QKV)
    a1 = heads * 5 // UNITS
    a2 = heads * QKV // UNITS
    attend(0, a1)
    visit1(4)
    attend(a1, a2)
    visit2(4)
    attend(a2, heads)
    flip()
    for k in THREE:
        run_units(load_cols, k, out_unit(k), QKV)
    visit1(5)
    norm(x1, 2)
    run_units(load_cols, 3, up_unit(3))
    visit2(5)
    run_units(load_cols, 4, up_unit(4))
    visit1(6)
    visit2(6)
    run_units(load_cols, 5, up_unit(5))
    visit1(7)
    visit2(7)
    q1, q2, q3 = 3, 6, QKV
    run_down(6, hi=q2)
    sides_in(7)
    run_down(6, q2, primed=True)
    await_siblings(7, 0, *SIDES)
    run_down(7, hi=q2, known=q3)
    visit1(LAST)
    run_down(7, q2, q3, q3, True)
    visit2(LAST)
    run_down(7, q3)
    await_siblings(LAST, 0)
    run_down(LAST, hi=q1, known=q1)
    sides_in(LAST)
    await_siblings(LAST, SIDES[0])
    run_down(LAST, q1, q2, q2)
    across_in(LAST)
    await_siblings(LAST, SIDES[1])
    run_down(LAST, q2, q3, q3)
    await_siblings(LAST, ACROSS)
    run_down(LAST, q3)

    for k in range(CHUNKS):
        ref = Block(k).ref
        for p in THREE:
            take(ref.at[(ALL3,) + ZEROS[:2 - p] + (ALL3,)], S.at[k, p])
        take(ref.at[ALL3], S.at[k, SIBLING])
    for m, lo, n in ((0,) + early, (0,) + rest, (1,) + whole):
        take(stage12.at[m, pl.ds(0, 7), :, pl.ds(lo, n)], XS.at[2 * m + (lo > 0)])
    take(stage3.at[0], XS.at[4])
    take(V.at[0, 0, pl.ds(0, 7)], VS.at[0])
    take(V.at[0, ALL3], VS.at[1])
    take(V.at[ALL3], VS.at[2])


def solution(mesh):
    batch_axes = ('dp', 'fsdp')

    def local_layer(prompts, ln1_gain, ln1_bias, w_qkv, b_qkv, w_out, b_out, ln2_gain, ln2_bias, w_up, b_up, w_down, b_down):
        _, seq, d = prompts.shape
        heads, hd = w_qkv.shape[2], w_qkv.shape[3]
        lane = d // 18
        rows = d // 16
        pair = 2 * lane
        third = rows // 3
        r = w_up.shape[0]

        parts = [ln1_gain, ln1_bias, b_out, ln2_gain, ln2_bias, b_down, b_qkv, b_up]
        orders = ((0, 1, 2), (2, 0, 1), (1, 2, 0))

        hidden = np.arange(4 * d).reshape(4, 4, 4, 3, third)
        hidden = np.concatenate([hidden[:, :, :, c].transpose(orders[c] + (3,)).reshape(-1) for c in THREE])
        index = [(np.arange(d), d // 128), (np.arange(3 * d), 3 * d // 128), (hidden, 4 * d // 128)]
        tab = np.stack([np.concatenate([i // n for i, n in index]), np.concatenate([i % n for i, n in index])])

        dims = (seq, d, heads, hd, rows, lane)
        vm = pl.BlockSpec(memory_space=pltpu.VMEM)
        hbm = pl.BlockSpec(memory_space=pl.ANY)
        dma = pltpu.SemaphoreType.DMA
        act, act_t = pltpu.VMEM((seq, d), BF), pltpu.VMEM((d, seq), BF)
        y, kv, _, _ = pl.pallas_call(
            functools.partial(layer_kernel, dims),
            out_shape=(
                pltpu.VMEM((seq, d), BF),
                pltpu.VMEM((2 * d, seq), BF),
                jax.ShapeDtypeStruct((36, 4, 4, 4, rows, lane), BF),
                jax.ShapeDtypeStruct((18, 4, 4, 4, third, 3 * lane), BF),
            ),
            in_specs=[hbm] + [vm] * 13,
            out_specs=(vm, vm, hbm, hbm),
            scratch_shapes=[
                act, act, act_t, act_t, act, act,
                pltpu.VMEM((seq, 4 * d), BF),
                pltpu.VMEM((SLOTS, 4, 4, rows, pair), BF),
                pltpu.VMEM((SLOTS, 4, 4, third, 6 * lane), BF),
                pltpu.VMEM((seq, 6 * lane), F32),
                pltpu.VMEM((18, rows, lane), BF),
                pltpu.VMEM((9, third, 3 * lane), BF),
                pltpu.VMEM((r, 4 * d), BF),
                pltpu.VMEM((2, LINE, r, QKV * lane), BF),
                pltpu.VMEM((2, w_down.shape[0], QKV * lane), BF),
                pltpu.VMEM((LINE, LANES), F32),
                pltpu.VMEM((LINE, LANES), BF),
                pltpu.VMEM((4, 4, LINE, LINE, LANES), BF),
                pltpu.VMEM((4, 1, d), F32),
                pltpu.VMEM((54, 1, lane), F32),
                pltpu.VMEM((18, 1, lane), F32),
                pltpu.VMEM((72, 1, lane), F32),
                pltpu.VMEM((1, d), F32),
                pltpu.VMEM((2, LANES, LANES), BF),
                dma((3 * CHUNKS, 4, 4)),
                dma((CHUNKS, 4)),
                dma((SLOTS,)),
                dma((CHUNKS + 1,)),
                dma((5,)),
                dma((5,)),
                dma((3,)),
                dma((3,)),
            ],
            compiler_params=pltpu.CompilerParams(
                has_side_effects=True, collective_id=0, vmem_limit_bytes=50 << 20),
            name="layer",
        )(prompts[0], w_qkv.reshape(r, -1), w_out, w_up, w_down, jnp.asarray(tab, jnp.int32), *(p[None] for p in parts))
        kc, vc = (m.reshape(heads, hd, seq).transpose(2, 0, 1)[None] for m in (kv[:d], kv[d:]))
        return y[None], kc, vc

    weight_spec = P('fsdp')
    return jax.shard_map(local_layer, mesh=mesh, in_specs=(P(batch_axes),) + (weight_spec,) * 12, out_specs=(P(batch_axes), P(batch_axes), P(batch_axes)), check_vma=False)
```

```python
import functools

import jax
import jax.numpy as jnp
import numpy as np
from jax import lax
from jax.experimental import pallas as pl
from jax.experimental.pallas import tpu as pltpu
from jax.sharding import PartitionSpec as P

LN_EPS = 1e-5
MESH = pl.DeviceIdType.MESH
BF = jnp.bfloat16
F32 = jnp.float32
CHUNKS = 9
SLOTS = 3
LO, HI, ALL3 = pl.ds(0, 2), pl.ds(2, 2), pl.ds(0, 3)
FIRST, SECOND, ACROSS, SIBLING = range(4)
ZEROS = (0, 0, 0)
THREE = range(3)
TWO = range(2)
OTHERS = pl.ds(0, 7)
UNITS = 12
QKV = 9
LINE = 8
SIDES = (1, 3)
QUARTERS = (0, *SIDES, ACROSS)
LAST = CHUNKS - 1
LANES = 128
LATE = (3, 4, 5)


def loop(hi, body, lo=0):
    def step(i, carry):
        body(i)
        return carry
    lax.fori_loop(lo, hi, step, None)


def wrap(i):
    return lax.rem(i, 4)


def thirds(u):
    return u // 3, lax.rem(u, 3)


def layer_kernel(dims, x_hbm, wq, wo, w2, w3, tab, *refs):
    vecs, (y_ref, kv_ref, G12, G3), refs = refs[:8], refs[8:12], refs[12:]
    (x_ref, h, qt, ctxt, ctx, x1, a, wbuf, wbuf3, acc, own12, own3, G8, w2p, stage12, stage3, vec32, vec, V, lnv, bqkv, bout,
     bup, bdown, vrow, R, S, LS, OS, X, XS, VR, VS) = refs
    seq, d, heads, hd, rows, lane = dims
    pair = 2 * lane
    me = lax.axis_index("fsdp")
    core = lax.rem(me, 2)
    cx = wrap(me // 2)
    cy = wrap(me // 8)
    cz = me // 32
    sib = me + 1 - 2 * core
    spot = lax.rem(me, LINE)
    line = [me - spot + lax.rem(spot + o, LINE) for o in range(1, LINE)]
    column = [me + (wrap(cy + o) - cy) * 8 for o in range(1, 4)]
    pillar = [me + (wrap(cz + o) - cz) * 32 for o in range(1, 4)]

    barrier = pltpu.get_barrier_semaphore()
    partners = line + column + pillar
    for dev in partners:
        pl.semaphore_signal(barrier, inc=1, device_id={"fsdp": dev}, device_id_type=MESH)

    class Block:
        def __init__(self, k):
            self.ref, self.base = (G12, k) if k < 6 else (G3, k - 6)
            self.blocks, self.first = (own12, 3 * k) if k < 6 else (own3, 3 * (k - 6))
            if k == LAST:
                self.ref, self.base = G8, 0

        def slab(self, c):
            return (self.base * 2 + core) * 3 + c

        def own(self, c):
            return self.blocks.at[self.first + c]

    def pick(c, v):
        return jnp.where(c == 0, v[0], jnp.where(c == 1, v[1], v[2]))

    def place(c):
        v = (cx, cy, cz)
        return tuple(pick(c, v[p:] + v[:p]) for p in THREE)

    def near(c, p):
        v = (2, 8, 32)
        stride = pick(c, v[p:] + v[:p])
        i = place(c)[p]
        up, down = wrap(i + 1), wrap(i + 3)
        return me + (up - i) * stride, me + (down - i) * stride, up, down

    def send(src, dst, s, r, dev):
        pltpu.make_async_remote_copy(
            src_ref=src, dst_ref=dst, send_sem=s, recv_sem=r,
            device_id={"fsdp": dev}, device_id_type=MESH).start()

    def take(ref, sem):
        pltpu.make_async_copy(ref, ref, sem).wait()

    def colours(body):
        loop(3, body)

    def await_group(k, p, role, n=None):
        B = Block(k)

        def body(c):
            at = (B.slab(c),) + ZEROS[:3 - p]
            if n is not None:
                at = at[:-1] + (n,)
            take(B.ref.at[at], R.at[k * 3 + c, p, role])
        colours(body)

    def await_siblings(k, *quarters):
        B = Block(k)
        for ahead in quarters:
            colours(lambda c: take(B.ref.at[B.slab(c), 0], R.at[k * 3 + c, SIBLING, ahead]))

    def p0_send(k):
        B = Block(k)

        def body(c):
            i0, i1, i2 = place(c)
            right, left, _, _ = near(c, 0)
            dst = B.ref.at[B.slab(c), i2, i1, i0]
            for dev in (right, left):
                send(B.own(c), dst, S.at[k, 0], R.at[k * 3 + c, 0, FIRST], dev)
            pltpu.make_async_copy(B.own(c), dst, OS.at[k]).start()
        colours(body)

    def p0_forward(k):
        B = Block(k)
        take(B.ref.at[0, 0, 0, ALL3], OS.at[k])
        await_group(k, 0, FIRST, LO)

        def body(c):
            i0, i1, i2 = place(c)
            right, left, up, down = near(c, 0)
            from_, to = (down, right) if k % 2 == 0 else (up, left)
            blk = B.ref.at[B.slab(c), i2, i1, from_]
            send(blk, blk, S.at[k, 0], R.at[k * 3 + c, 0, ACROSS], to)
        colours(body)

    def halves(k, c, p, i):
        B = Block(k)
        at = (B.slab(c), place(c)[2], i) if p == 1 else (B.slab(c), i)
        return B.ref.at[at + (LO,)], B.ref.at[at + (HI,)]

    def to_sibling(k, c, ahead):
        B = Block(k)
        part = B.ref.at[B.slab(c), wrap(place(c)[2] + ahead)]
        send(part, part, S.at[k, SIBLING], R.at[k * 3 + c, SIBLING, ahead], sib)

    def axis_first(k, p):
        def body(c):
            right, left, _, _ = near(c, p)
            lo, hi = halves(k, c, p, place(c)[p])
            send(lo, lo, S.at[k, p], R.at[k * 3 + c, p, FIRST], right)
            send(hi, hi, S.at[k, p], R.at[k * 3 + c, p, FIRST], left)
            if p == 2:
                to_sibling(k, c, 0)
        colours(body)

    def axis_second(k, p):
        def body(c):
            right, left, _, _ = near(c, p)
            lo, hi = halves(k, c, p, place(c)[p])
            send(hi, hi, S.at[k, p], R.at[k * 3 + c, p, SECOND], right)
            send(lo, lo, S.at[k, p], R.at[k * 3 + c, p, SECOND], left)
        colours(body)

    def axis_forward(k, p):
        await_group(k, p, FIRST)

        def body(c):
            right, left, up, down = near(c, p)
            lo, hi = halves(k, c, p, down)[0], halves(k, c, p, up)[1]
            send(lo, lo, S.at[k, p], R.at[k * 3 + c, p, ACROSS], right)
            send(hi, hi, S.at[k, p], R.at[k * 3 + c, p, ACROSS], left)
        colours(body)

    def sides_in(k):
        await_group(k, 2, SECOND)

        for ahead in SIDES:
            colours(lambda c: to_sibling(k, c, ahead))

    def across_in(k):
        await_group(k, 2, ACROSS)
        colours(lambda c: to_sibling(k, c, ACROSS))

    share = QKV * lane

    def x_send(m, lo, n):
        at = stage12.at[m, spot, :, pl.ds(lo, n)]

        def give(src, i, dev):
            part = src.at[:, pl.ds(pl.multiple_of(i * share + lo, lane), n)]
            sem = 2 * m + (lo > 0)
            if dev is None:
                pltpu.make_async_copy(part, at, X.at[sem]).start()
            else:
                send(part, at, XS.at[sem], X.at[sem], dev)

        def route(i, dev):
            if m:
                give(w2p, i, dev)
                return

            @pl.when(i < 6)
            def _():
                give(wq, i, dev)

            @pl.when(i >= 6)
            def _():
                give(wo, i - 6, dev)
        for dev in line:
            route(lax.rem(dev, LINE), dev)
        route(spot, None)

    def x_wait(m, lo, n):
        take(stage12.at[m, :, :, pl.ds(lo, n)], X.at[2 * m + (lo > 0)])

    def x_blocks(k):
        for c in THREE:
            lanes = pl.ds((3 * (k % 3) + c) * lane, lane)
            own12[3 * k + c] = jnp.concatenate(
                [stage12[k // 3, i, :, lanes].astype(F32) for i in range(LINE)], axis=0).astype(BF)

    def x3_send():
        part = lambda s: w3.at[:, pl.ds(pl.multiple_of(s * share, lane), share)]
        send(part(1 - core), stage3.at[core], XS.at[4], X.at[4], sib)
        pltpu.make_async_copy(part(core), stage3.at[core], X.at[4]).start()

    def x3_blocks():
        take(stage3, X.at[4])
        n = rows // 3
        for j in THREE:
            lanes = slice(3 * j * lane, 3 * (j + 1) * lane)
            both = jnp.concatenate([stage3[s, :, lanes].astype(F32) for s in TWO], axis=0)
            for c in THREE:
                own3[3 * j + c] = both[c * n:(c + 1) * n].astype(BF)

    def permute_up():
        n = rows // 3
        for c in THREE:
            v = (1, 4, 16)
            s0, s1, s2 = v[c:] + v[:c]
            for i in range(4):
                chips = [i * s2 + j * s1 + k * s0 for j in range(4) for k in range(4)]
                groups = [w2[:, q * rows + c * n:q * rows + (c + 1) * n].astype(F32) for q in chips]
                w2p[:, (4 * c + i) * 16 * n:(4 * c + i + 1) * 16 * n] = jnp.concatenate(groups, axis=1).astype(BF)

    def v_pack():
        vec32[...] = jnp.zeros_like(vec32)
        for i, ref in enumerate(vecs):
            vec32[i:i + 1, :ref.shape[1]] = ref[...].astype(F32)
        vec[...] = vec32[...].astype(BF)

    def v_send(axis):
        if axis == 0:
            part = V.at[cz, cy, spot]
            for dev in line:
                send(vec, part, VS.at[0], VR.at[0], dev)
            pltpu.make_async_copy(vec, part, VR.at[0]).start()
        elif axis == 1:
            take(V.at[0, 0], VR.at[0])
            for dev in column:
                send(V.at[cz, cy], V.at[cz, cy], VS.at[1], VR.at[1], dev)
        else:
            take(V.at[0, ALL3], VR.at[1])
            for dev in pillar:
                send(V.at[cz], V.at[cz], VS.at[2], VR.at[2], dev)

    def spread(vals, at):
        n = at.size
        select = (lax.broadcasted_iota(jnp.int32, (LANES, n), 0) == tab[1:2, at]).astype(BF)
        return jnp.dot(vals, select, preferred_element_type=F32)

    def v_rows():
        take(V.at[ALL3], VR.at[2])
        nd = d // pair

        def body(t):
            at = pl.ds(pl.multiple_of(t * pair, pair), pair)
            m = spread(V[...].reshape(-1, LANES), at).reshape(LANES, LINE, pair)
            dev = lax.broadcasted_iota(jnp.int32, m.shape, 0)
            v = jnp.sum(jnp.where(dev == tab[0:1, at][None], m, 0.0), axis=0)
            for i, src in enumerate((0, 1, 3, 4)):
                lnv[i, :, at] = v[src:src + 1]
            for o in TWO:
                bout[2 * t + o] = v[2:3, o * lane:(o + 1) * lane]
            bdown[:, at] = v[5:6]
        loop(nd, body)
        dev = lax.broadcasted_iota(jnp.int32, (LANES, LINE * LANES), 0)
        slot = lax.broadcasted_iota(jnp.int32, (LANES, LINE * LANES), 1)
        for i in TWO:
            take_row = (slot == dev * LINE + 6 + i).astype(BF)
            vrow[i] = jnp.dot(take_row, V[...].reshape(-1, LANES), preferred_element_type=F32).astype(BF)

    def v_long(i, out, first, count):
        wide = 3 * pair

        def body(t):
            at = pl.ds(pl.multiple_of(first + t * wide, pair), wide)
            m = spread(vrow[i], at)
            dev = lax.broadcasted_iota(jnp.int32, m.shape, 0)
            v = jnp.sum(jnp.where(dev == tab[0:1, at], m, 0.0), axis=0, keepdims=True)
            for o in range(6):
                out[6 * t + o] = v[:, o * lane:(o + 1) * lane]
        loop(count, body)

    def issue(t):
        if t + 1 < CHUNKS:
            axis_first(t + 1, 1)
            axis_second(t + 1, 1)
        axis_first(t, 2)

    def visit1(t):
        last, ahead, far = t - 1, t + 1, t + 2
        if t:
            if t < LAST:
                sides_in(last)
            across_in(last)
        if far < CHUNKS:
            p0_forward(far)
        if ahead < CHUNKS:
            axis_forward(ahead, 1)
        if t < LAST:
            axis_second(t, 2)

    def visit2(t):
        last, ahead, far, farther = t - 1, t + 1, t + 2, t + 3
        axis_forward(t, 2)
        if far < CHUNKS:
            await_group(far, 0, ACROSS)
        if ahead < CHUNKS:
            for role in (SECOND, ACROSS):
                await_group(ahead, 1, role)
            if farther in LATE:
                p0_send(farther)
            issue(ahead)
        if ahead == LAST:
            axis_second(LAST, 2)
        if t == LAST:
            await_siblings(last, ACROSS)
        elif t:
            await_siblings(last, *QUARTERS)

    def load_cols(k, u, slot):
        x, c = thirds(u)
        for s in TWO:
            g = (k * 2 + s) * 3 + c
            dst = wbuf.at[slot, :, :, :, pl.ds(s * lane, lane)]

            @pl.when(c == 0)
            def _():
                pltpu.make_async_copy(G12.at[g, :, :, x], dst, LS.at[slot]).start()

            @pl.when(c == 1)
            def _():
                pltpu.make_async_copy(G12.at[g, x], dst, LS.at[slot]).start()

            @pl.when(c > 1)
            def _():
                for y in range(4):
                    pltpu.make_async_copy(
                        G12.at[g, y, x], wbuf.at[slot, :, y, :, pl.ds(s * lane, lane)], LS.at[slot]).start()

    def load_rows(k, c, z, slot):
        for s in TWO:
            g = ((k - 6) * 2 + s) * 3 + c
            pltpu.make_async_copy(
                G3.at[g, z], wbuf3.at[slot, :, :, :, pl.ds(s * 3 * lane, 3 * lane)], LS.at[slot]).start()

    def run_units(k, unit, lo=0, hi=UNITS, known=None, primed=False):
        load, known, body = load_cols, known or hi, unit(k)
        if not primed:
            load(k, lo, lo % SLOTS)
            load(k, lo + 1, (lo + 1) % SLOTS)

        def step(u):
            slot = lax.rem(u, SLOTS)
            take(wbuf.at[slot], LS.at[slot])

            @pl.when(u + 2 < known)
            def _():
                load(k, u + 2, lax.rem(u + 2, SLOTS))
            body(u, slot)
        loop(hi, step, lo)

    def weight(slot):
        return wbuf[slot].reshape(d, pair)

    def tiles(k, u):
        x, c = thirds(u)
        first = 18 * x + 3 * (k % 3) + c
        return first, first + QKV

    def span(t):
        return pl.ds(pl.multiple_of(t * lane, lane), lane)

    def both(r):
        return r[:, :lane], r[:, lane:]

    def qkv_unit(k):
        def body(u, slot):
            r = jnp.dot(h[...], weight(slot), preferred_element_type=F32)
            for t, v in zip(tiles(k, u), both(r)):
                v = (v + bqkv[t]).astype(BF).T

                @pl.when(t < 18)
                def _():
                    qt[span(t), :] = v

                @pl.when(t >= 18)
                def _():
                    kv_ref[span(t - 18), :] = v
        return body

    def out_unit(k):
        def body(u, slot):
            r = jnp.dot(ctx[...], weight(slot), preferred_element_type=F32)
            for t, v in zip(tiles(k, u - QKV), both(r)):
                x1[:, span(t)] = (x_ref[:, span(t)].astype(F32) + v + bout[t]).astype(BF)
        return body

    def up_unit(k):
        def body(u, slot):
            r = jnp.dot(h[...], weight(slot), preferred_element_type=F32)
            for t, v in zip(tiles(k, u), both(r)):
                a[:, span(t)] = jax.nn.gelu(v + bup[t], approximate=True).astype(BF)
        return body

    def quarter(u):
        o, c = thirds(u)
        return c, wrap(place(c)[2] + o + o // 2 - o // 3 * 2)

    def down_lhs(c, z):
        n = 16 * (rows // 3)
        return a[:, pl.ds(pl.multiple_of((c * 4 + z) * n, lane), n)]

    def add(u, cols, r):
        @pl.when(u == 0)
        def _():
            acc[:, cols] = r

        @pl.when(u > 0)
        def _():
            acc[:, cols] += r

    def finish(k):
        n = 3 * lane
        for s in TWO:
            cols = pl.ds(s * share + (k - 6) * n, n)
            y_ref[:, cols] = (x1[:, cols].astype(F32) + acc[:, s * n:(s + 1) * n] + bdown[:, cols]).astype(BF)

    def run_down(k, lo=0, hi=UNITS, known=UNITS, primed=False):
        def load(u):
            c, z = quarter(u)
            load_rows(k, c, z, lax.rem(u, SLOTS))
        if not primed:
            load(lo)
            load(lo + 1)

        def step(u):
            slot = lax.rem(u, SLOTS)
            take(wbuf3.at[slot], LS.at[slot])

            @pl.when(u + 2 < known)
            def _():
                load(u + 2)
            w = wbuf3[slot].reshape(-1, 6 * lane)
            add(u, slice(None), jnp.dot(down_lhs(*quarter(u)), w, preferred_element_type=F32))
        loop(hi, step, lo)
        if hi == UNITS:
            finish(k)

    def run_last(lo, hi):
        n = 3 * lane

        def step(u):
            c, z = quarter(u)
            for s in TWO:
                w = G8[3 * s + c, z].reshape(-1, n)
                add(u, slice(s * n, (s + 1) * n), jnp.dot(down_lhs(c, z), w, preferred_element_type=F32))
        loop(hi, step, lo)
        if hi == UNITS:
            finish(LAST)

    def norm(src, which):
        n = seq // 8

        def step(b):
            at = pl.ds(pl.multiple_of(b * n, n), n)
            v = src[at, :].astype(F32)
            v = v - jnp.mean(v, axis=-1, keepdims=True)
            var = jnp.mean(v * v, axis=-1, keepdims=True)
            h[at, :] = (v * lax.rsqrt(var + LN_EPS) * lnv[which] + lnv[which + 1]).astype(BF)
        loop(8, step)

    def attend(lo, hi):
        qb = seq // 2
        scale = hd ** -0.5

        def step(i):
            q_rows = pl.ds(pl.multiple_of(i * hd, hd), hd)
            k_rows = q_rows
            v_rows = pl.ds(pl.multiple_of(i * hd + d, hd), hd)
            for b in TWO:
                n = (b + 1) * qb
                q = qt[q_rows, b * qb:n]
                s = lax.dot_general(q, kv_ref[k_rows, :n], (((0,), (0,)), ((), ())),
                                    preferred_element_type=F32) * scale
                row = lax.broadcasted_iota(jnp.int32, (qb, n), 0) + b * qb
                col = lax.broadcasted_iota(jnp.int32, (qb, n), 1)
                s = jnp.where(col <= row, s, -jnp.inf)
                e = jnp.exp(s - jnp.max(s, axis=-1, keepdims=True))
                w = (e / jnp.sum(e, axis=-1, keepdims=True)).astype(BF)
                o = lax.dot_general(kv_ref[v_rows, :n], w, (((1,), (1,)), ((), ())),
                                    preferred_element_type=F32)
                ctxt[q_rows, b * qb:n] = o.astype(BF)
        loop(hi, step, lo)

    def flip():
        def step(i):
            at = pl.ds(pl.multiple_of(i * pair, pair), pair)
            ctx[:, at] = ctxt[at, :].T
        loop(d // pair, step)

    x_copy = pltpu.make_async_copy(x_hbm, x_ref, OS.at[CHUNKS])
    x_copy.start()
    v_pack()
    permute_up()
    pl.semaphore_wait(barrier, len(partners))
    early, rest, whole = (0, 3 * lane), (3 * lane, 6 * lane), (0, share)
    x_send(0, *early)
    x_send(0, *rest)
    x3_send()
    v_send(0)
    x_wait(0, *early)
    x_blocks(0)
    p0_send(0)
    x_wait(0, *rest)
    for k in (1, 2):
        x_blocks(k)
        p0_send(k)
    p0_forward(0)
    x3_blocks()
    await_group(0, 0, ACROSS)
    axis_first(0, 1)
    axis_second(0, 1)
    p0_forward(1)
    p0_send(6)
    axis_forward(0, 1)
    await_group(1, 0, ACROSS)
    axis_first(1, 1)
    axis_second(1, 1)
    x_send(1, *whole)
    v_send(1)
    p0_send(7)
    p0_send(8)
    await_group(0, 1, SECOND)
    await_group(0, 1, ACROSS)
    axis_first(0, 2)
    v_send(2)
    visit1(0)
    x_copy.wait()
    x_wait(1, *whole)
    for k in LATE:
        x_blocks(k)
    visit2(0)
    v_rows()
    norm(x_ref, 0)
    visit1(1)
    v_long(0, bqkv, d, 9)
    visit2(1)
    run_units(0, qkv_unit, hi=QKV)
    visit1(2)
    v_long(1, bup, 4 * d, 12)
    visit2(2)
    run_units(1, qkv_unit, hi=QKV)
    visit1(3)
    visit2(3)
    run_units(2, qkv_unit, hi=QKV)
    q1, q2, q3 = 3, 6, QKV
    a1, a2 = heads * q3 // 24, heads * 18 // 24
    attend(0, a1)
    visit1(4)
    attend(a1, a2)
    visit2(4)
    attend(a2, heads)
    flip()
    run_units(0, out_unit, QKV)
    run_units(1, out_unit, QKV)
    visit1(5)
    run_units(2, out_unit, QKV)
    norm(x1, 2)
    run_units(3, up_unit, hi=q1, known=UNITS)
    visit2(5)
    run_units(3, up_unit, q1, primed=True)
    run_units(4, up_unit, hi=q2, known=UNITS)
    visit1(6)
    run_units(4, up_unit, q2, primed=True)
    visit2(6)
    run_units(5, up_unit, hi=q3, known=UNITS)
    visit1(7)
    run_units(5, up_unit, q3, primed=True)
    visit2(7)
    run_down(6, hi=q2)
    sides_in(7)
    run_down(6, q2, primed=True)
    await_siblings(7, 0, *SIDES)
    run_down(7, hi=q2, known=q3)
    visit1(LAST)
    run_down(7, q2, q3, q3, True)
    visit2(LAST)
    run_down(7, q3)
    await_siblings(LAST, 0)
    run_last(0, q1)
    sides_in(LAST)
    await_siblings(LAST, SIDES[0])
    run_last(q1, q2)
    across_in(LAST)
    await_siblings(LAST, SIDES[1])
    run_last(q2, q3)
    await_siblings(LAST, ACROSS)
    run_last(q3, UNITS)

    for k in range(CHUNKS):
        ref = Block(k).ref
        for p in THREE:
            take(ref.at[(ALL3,) + ZEROS[:2 - p] + (ALL3,)], S.at[k, p])
        take(ref.at[ALL3], S.at[k, SIBLING])
    for m, lo, n in ((0,) + early, (0,) + rest, (1,) + whole):
        take(stage12.at[m, OTHERS, :, pl.ds(lo, n)], XS.at[2 * m + (lo > 0)])
    take(stage3.at[0], XS.at[4])
    take(V.at[0, 0, OTHERS], VS.at[0])
    take(V.at[0, ALL3], VS.at[1])
    take(V.at[ALL3], VS.at[2])


def solution(mesh):
    batch_axes = ('dp', 'fsdp')

    def local_layer(prompts, ln1_gain, ln1_bias, w_qkv, b_qkv, w_out, b_out, ln2_gain, ln2_bias, w_up, b_up, w_down, b_down):
        _, seq, d = prompts.shape
        heads, hd = w_qkv.shape[2], w_qkv.shape[3]
        lane = d // 18
        rows = d // 16
        pair = 2 * lane
        third = rows // 3
        r = w_up.shape[0]

        parts = [ln1_gain, ln1_bias, b_out, ln2_gain, ln2_bias, b_down, b_qkv, b_up]
        orders = ((0, 1, 2), (2, 0, 1), (1, 2, 0))

        hidden = np.arange(4 * d).reshape(4, 4, 4, 3, third)
        hidden = np.concatenate([hidden[:, :, :, c].transpose(orders[c] + (3,)).reshape(-1) for c in THREE])
        index = [(np.arange(d), d // 128), (np.arange(3 * d), 3 * d // 128), (hidden, 4 * d // 128)]
        tab = np.stack([np.concatenate([i // n for i, n in index]), np.concatenate([i % n for i, n in index])])

        dims = (seq, d, heads, hd, rows, lane)
        vm = pl.BlockSpec(memory_space=pltpu.VMEM)
        hbm = pl.BlockSpec(memory_space=pl.ANY)
        dma = pltpu.SemaphoreType.DMA
        act, act_t = pltpu.VMEM((seq, d), BF), pltpu.VMEM((d, seq), BF)
        y, kv, _, _ = pl.pallas_call(
            functools.partial(layer_kernel, dims),
            out_shape=(
                pltpu.VMEM((seq, d), BF),
                pltpu.VMEM((2 * d, seq), BF),
                jax.ShapeDtypeStruct((36, 4, 4, 4, rows, lane), BF),
                jax.ShapeDtypeStruct((12, 4, 4, 4, third, 3 * lane), BF),
            ),
            in_specs=[hbm] + [vm] * 13,
            out_specs=(vm, vm, hbm, hbm),
            scratch_shapes=[
                act, act, act_t, act_t, act, act,
                pltpu.VMEM((seq, 4 * d), BF),
                pltpu.VMEM((SLOTS, 4, 4, rows, pair), BF),
                pltpu.VMEM((SLOTS, 4, 4, third, 6 * lane), BF),
                pltpu.VMEM((seq, 6 * lane), F32),
                pltpu.VMEM((18, rows, lane), BF),
                pltpu.VMEM((9, third, 3 * lane), BF),
                pltpu.VMEM((6, 4, 4, 4, third, 3 * lane), BF),
                pltpu.VMEM((r, 4 * d), BF),
                pltpu.VMEM((2, LINE, r, QKV * lane), BF),
                pltpu.VMEM((2, w_down.shape[0], QKV * lane), BF),
                pltpu.VMEM((LINE, LANES), F32),
                pltpu.VMEM((LINE, LANES), BF),
                pltpu.VMEM((4, 4, LINE, LINE, LANES), BF),
                pltpu.VMEM((4, 1, d), F32),
                pltpu.VMEM((54, 1, lane), F32),
                pltpu.VMEM((18, 1, lane), F32),
                pltpu.VMEM((72, 1, lane), F32),
                pltpu.VMEM((1, d), F32),
                pltpu.VMEM((2, LANES, LANES), BF),
                dma((3 * CHUNKS, 4, 4)),
                dma((CHUNKS, 4)),
                dma((SLOTS,)),
                dma((CHUNKS + 1,)),
                dma((5,)),
                dma((5,)),
                dma((3,)),
                dma((3,)),
            ],
            compiler_params=pltpu.CompilerParams(
                has_side_effects=True, collective_id=0, vmem_limit_bytes=54 << 20),
            name="layer",
        )(prompts[0], w_qkv.reshape(r, -1), w_out, w_up, w_down, jnp.asarray(tab, jnp.int32), *(p[None] for p in parts))
        kc, vc = (m.reshape(heads, hd, seq).transpose(2, 0, 1)[None] for m in (kv[:d], kv[d:]))
        return y[None], kc, vc

    weight_spec = P('fsdp')
    return jax.shard_map(local_layer, mesh=mesh, in_specs=(P(batch_axes),) + (weight_spec,) * 12, out_specs=(P(batch_axes), P(batch_axes), P(batch_axes)), check_vma=False)
```

```python
import functools

import jax
import jax.numpy as jnp
import numpy as np
from jax import lax
from jax.experimental import pallas as pl
from jax.experimental.pallas import tpu as pltpu
from jax.sharding import PartitionSpec as P

LN_EPS = 1e-5
MESH = pl.DeviceIdType.MESH
BF = jnp.bfloat16
F32 = jnp.float32
CHUNKS = 9
SLOTS = 3
LO, HI, ALL3 = pl.ds(0, 2), pl.ds(2, 2), pl.ds(0, 3)
FIRST, SECOND, ACROSS, SIBLING = range(4)
ZEROS = (0, 0, 0)
THREE = range(3)
TWO = range(2)
OTHERS = pl.ds(0, 7)
UNITS = 12
QKV = 9
LINE = 8
SIDES = (1, 3)
QUARTERS = (0, *SIDES, ACROSS)
LAST = CHUNKS - 1
LANES = 128
LATE = (3, 4, 5)


def loop(hi, body, lo=0):
    def step(i, carry):
        body(i)
        return carry
    lax.fori_loop(lo, hi, step, None)


def wrap(i):
    return lax.rem(i, 4)


def thirds(u):
    return u // 3, lax.rem(u, 3)


def layer_kernel(dims, x_hbm, wq, wo, w2, w3, tab, *refs):
    vecs, (y_ref, kv_ref, G12, G3), refs = refs[:8], refs[8:12], refs[12:]
    (x_ref, h, qt, ctxt, ctx, x1, a, wbuf, wbuf3, acc, own12, own3, G8, w2p, stage12, stage3, vec32, vec, V, lnv, bqkv, bout,
     bup, bdown, vrow, R, S, LS, OS, X, XS, VR, VS) = refs
    seq, d, heads, hd, rows, lane = dims
    pair = 2 * lane
    me = lax.axis_index("fsdp")
    core = lax.rem(me, 2)
    cx = wrap(me // 2)
    cy = wrap(me // 8)
    cz = me // 32
    sib = me + 1 - 2 * core
    spot = lax.rem(me, LINE)
    line = [me - spot + lax.rem(spot + o, LINE) for o in range(1, LINE)]
    column = [me + (wrap(cy + o) - cy) * 8 for o in range(1, 4)]
    pillar = [me + (wrap(cz + o) - cz) * 32 for o in range(1, 4)]

    barrier = pltpu.get_barrier_semaphore()
    partners = line + column + pillar
    for dev in partners:
        pl.semaphore_signal(barrier, inc=1, device_id={"fsdp": dev}, device_id_type=MESH)

    class Block:
        def __init__(self, k):
            self.ref, self.base = (G12, k) if k < 6 else (G3, k - 6)
            self.blocks, self.first = (own12, 3 * k) if k < 6 else (own3, 3 * (k - 6))
            if k == LAST:
                self.ref, self.base = G8, 0

        def slab(self, c):
            return (self.base * 2 + core) * 3 + c

        def own(self, c):
            return self.blocks.at[self.first + c]

    def pick(c, v):
        return jnp.where(c == 0, v[0], jnp.where(c == 1, v[1], v[2]))

    def place(c):
        v = (cx, cy, cz)
        return tuple(pick(c, v[p:] + v[:p]) for p in THREE)

    def near(c, p):
        v = (2, 8, 32)
        stride = pick(c, v[p:] + v[:p])
        i = place(c)[p]
        up, down = wrap(i + 1), wrap(i + 3)
        return me + (up - i) * stride, me + (down - i) * stride, up, down

    def send(src, dst, s, r, dev):
        pltpu.make_async_remote_copy(
            src_ref=src, dst_ref=dst, send_sem=s, recv_sem=r,
            device_id={"fsdp": dev}, device_id_type=MESH).start()

    def take(ref, sem):
        pltpu.make_async_copy(ref, ref, sem).wait()

    def colours(body):
        loop(3, body)

    def await_group(k, p, role, n=None):
        B = Block(k)

        def body(c):
            at = (B.slab(c),) + ZEROS[:3 - p]
            if n is not None:
                at = at[:-1] + (n,)
            take(B.ref.at[at], R.at[k * 3 + c, p, role])
        colours(body)

    def await_siblings(k, *quarters):
        B = Block(k)
        for ahead in quarters:
            colours(lambda c: take(B.ref.at[B.slab(c), 0], R.at[k * 3 + c, SIBLING, ahead]))

    def p0_send(k):
        B = Block(k)

        def body(c):
            i0, i1, i2 = place(c)
            right, left, _, _ = near(c, 0)
            dst = B.ref.at[B.slab(c), i2, i1, i0]
            for dev in (right, left):
                send(B.own(c), dst, S.at[k, 0], R.at[k * 3 + c, 0, FIRST], dev)
            pltpu.make_async_copy(B.own(c), dst, OS.at[k]).start()
        colours(body)

    def p0_forward(k):
        B = Block(k)
        take(B.ref.at[0, 0, 0, ALL3], OS.at[k])
        await_group(k, 0, FIRST, LO)

        def body(c):
            i0, i1, i2 = place(c)
            right, left, up, down = near(c, 0)
            from_, to = (down, right) if k % 2 == 0 else (up, left)
            blk = B.ref.at[B.slab(c), i2, i1, from_]
            send(blk, blk, S.at[k, 0], R.at[k * 3 + c, 0, ACROSS], to)
        colours(body)

    def halves(k, c, p, i):
        B = Block(k)
        at = (B.slab(c), place(c)[2], i) if p == 1 else (B.slab(c), i)
        return B.ref.at[at + (LO,)], B.ref.at[at + (HI,)]

    def to_sibling(k, c, ahead):
        B = Block(k)
        part = B.ref.at[B.slab(c), wrap(place(c)[2] + ahead)]
        send(part, part, S.at[k, SIBLING], R.at[k * 3 + c, SIBLING, ahead], sib)

    def axis_first(k, p):
        def body(c):
            right, left, _, _ = near(c, p)
            lo, hi = halves(k, c, p, place(c)[p])
            send(lo, lo, S.at[k, p], R.at[k * 3 + c, p, FIRST], right)
            send(hi, hi, S.at[k, p], R.at[k * 3 + c, p, FIRST], left)
            if p == 2:
                to_sibling(k, c, 0)
        colours(body)

    def axis_second(k, p):
        def body(c):
            right, left, _, _ = near(c, p)
            lo, hi = halves(k, c, p, place(c)[p])
            send(hi, hi, S.at[k, p], R.at[k * 3 + c, p, SECOND], right)
            send(lo, lo, S.at[k, p], R.at[k * 3 + c, p, SECOND], left)
        colours(body)

    def axis_forward(k, p):
        await_group(k, p, FIRST)

        def body(c):
            right, left, up, down = near(c, p)
            lo, hi = halves(k, c, p, down)[0], halves(k, c, p, up)[1]
            send(lo, lo, S.at[k, p], R.at[k * 3 + c, p, ACROSS], right)
            send(hi, hi, S.at[k, p], R.at[k * 3 + c, p, ACROSS], left)
        colours(body)

    def sides_in(k):
        await_group(k, 2, SECOND)

        for ahead in SIDES:
            colours(lambda c: to_sibling(k, c, ahead))

    def across_in(k):
        await_group(k, 2, ACROSS)
        colours(lambda c: to_sibling(k, c, ACROSS))

    share = QKV * lane

    def x_send(m, lo, n):
        at = stage12.at[m, spot, :, pl.ds(lo, n)]

        def give(src, i, dev):
            part = src.at[:, pl.ds(pl.multiple_of(i * share + lo, lane), n)]
            sem = 2 * m + (lo > 0)
            if dev is None:
                pltpu.make_async_copy(part, at, X.at[sem]).start()
            else:
                send(part, at, XS.at[sem], X.at[sem], dev)

        def route(i, dev):
            if m:
                give(w2p, i, dev)
                return

            @pl.when(i < 6)
            def _():
                give(wq, i, dev)

            @pl.when(i >= 6)
            def _():
                give(wo, i - 6, dev)
        for dev in line:
            route(lax.rem(dev, LINE), dev)
        route(spot, None)

    def x_wait(m, lo, n):
        take(stage12.at[m, :, :, pl.ds(lo, n)], X.at[2 * m + (lo > 0)])

    def x_blocks(k):
        for c in THREE:
            lanes = pl.ds((3 * (k % 3) + c) * lane, lane)
            own12[3 * k + c] = jnp.concatenate(
                [stage12[k // 3, i, :, lanes].astype(F32) for i in range(LINE)], axis=0).astype(BF)

    def x3_send():
        part = lambda s: w3.at[:, pl.ds(pl.multiple_of(s * share, lane), share)]
        send(part(1 - core), stage3.at[core], XS.at[4], X.at[4], sib)
        pltpu.make_async_copy(part(core), stage3.at[core], X.at[4]).start()

    def x3_blocks():
        take(stage3, X.at[4])
        n = rows // 3
        for j in THREE:
            lanes = slice(3 * j * lane, 3 * (j + 1) * lane)
            both = jnp.concatenate([stage3[s, :, lanes].astype(F32) for s in TWO], axis=0)
            for c in THREE:
                own3[3 * j + c] = both[c * n:(c + 1) * n].astype(BF)

    def permute_up():
        n = rows // 3
        for c in THREE:
            v = (1, 4, 16)
            s0, s1, s2 = v[c:] + v[:c]
            for i in range(4):
                chips = [i * s2 + j * s1 + k * s0 for j in range(4) for k in range(4)]
                groups = [w2[:, q * rows + c * n:q * rows + (c + 1) * n].astype(F32) for q in chips]
                w2p[:, (4 * c + i) * 16 * n:(4 * c + i + 1) * 16 * n] = jnp.concatenate(groups, axis=1).astype(BF)

    def v_pack():
        vec32[...] = jnp.zeros_like(vec32)
        for i, ref in enumerate(vecs):
            vec32[i:i + 1, :ref.shape[1]] = ref[...].astype(F32)
        vec[...] = vec32[...].astype(BF)

    def v_send(axis):
        if axis == 0:
            part = V.at[cz, cy, spot]
            for dev in line:
                send(vec, part, VS.at[0], VR.at[0], dev)
            pltpu.make_async_copy(vec, part, VR.at[0]).start()
        elif axis == 1:
            take(V.at[0, 0], VR.at[0])
            for dev in column:
                send(V.at[cz, cy], V.at[cz, cy], VS.at[1], VR.at[1], dev)
        else:
            take(V.at[0, ALL3], VR.at[1])
            for dev in pillar:
                send(V.at[cz], V.at[cz], VS.at[2], VR.at[2], dev)

    def spread(vals, at):
        n = at.size
        select = (lax.broadcasted_iota(jnp.int32, (LANES, n), 0) == tab[1:2, at]).astype(BF)
        return jnp.dot(vals, select, preferred_element_type=F32)

    def v_rows():
        take(V.at[ALL3], VR.at[2])
        nd = d // pair

        def body(t):
            at = pl.ds(pl.multiple_of(t * pair, pair), pair)
            m = spread(V[...].reshape(-1, LANES), at).reshape(LANES, LINE, pair)
            dev = lax.broadcasted_iota(jnp.int32, m.shape, 0)
            v = jnp.sum(jnp.where(dev == tab[0:1, at][None], m, 0.0), axis=0)
            for i, src in enumerate((0, 1, 3, 4)):
                lnv[i, :, at] = v[src:src + 1]
            for o in TWO:
                bout[2 * t + o] = v[2:3, o * lane:(o + 1) * lane]
            bdown[:, at] = v[5:6]
        loop(nd, body)
        dev = lax.broadcasted_iota(jnp.int32, (LANES, LINE * LANES), 0)
        slot = lax.broadcasted_iota(jnp.int32, (LANES, LINE * LANES), 1)
        for i in TWO:
            take_row = (slot == dev * LINE + 6 + i).astype(BF)
            vrow[i] = jnp.dot(take_row, V[...].reshape(-1, LANES), preferred_element_type=F32).astype(BF)

    def v_long(i, out, first, count):
        wide = 3 * pair

        def body(t):
            at = pl.ds(pl.multiple_of(first + t * wide, pair), wide)
            m = spread(vrow[i], at)
            dev = lax.broadcasted_iota(jnp.int32, m.shape, 0)
            v = jnp.sum(jnp.where(dev == tab[0:1, at], m, 0.0), axis=0, keepdims=True)
            for o in range(6):
                out[6 * t + o] = v[:, o * lane:(o + 1) * lane]
        loop(count, body)

    def issue(t):
        if t + 1 < CHUNKS:
            axis_first(t + 1, 1)
            axis_second(t + 1, 1)
        axis_first(t, 2)

    def visit1(t):
        last, ahead, far = t - 1, t + 1, t + 2
        if t:
            sides_in(last)
            across_in(last)
        if far < CHUNKS:
            p0_forward(far)
        if ahead < CHUNKS:
            axis_forward(ahead, 1)
        axis_second(t, 2)

    def visit2(t):
        last, ahead, far, farther = t - 1, t + 1, t + 2, t + 3
        axis_forward(t, 2)
        if far < CHUNKS:
            await_group(far, 0, ACROSS)
        if ahead < CHUNKS:
            for role in (SECOND, ACROSS):
                await_group(ahead, 1, role)
            if farther in LATE:
                p0_send(farther)
            issue(ahead)
        if ahead == LAST:
            axis_second(LAST, 2)
        if t:
            await_siblings(last, *QUARTERS)

    def load_cols(k, u, slot):
        x, c = thirds(u)
        for s in TWO:
            g = (k * 2 + s) * 3 + c
            dst = wbuf.at[slot, :, :, :, pl.ds(s * lane, lane)]

            @pl.when(c == 0)
            def _():
                pltpu.make_async_copy(G12.at[g, :, :, x], dst, LS.at[slot]).start()

            @pl.when(c == 1)
            def _():
                pltpu.make_async_copy(G12.at[g, x], dst, LS.at[slot]).start()

            @pl.when(c > 1)
            def _():
                for y in range(4):
                    pltpu.make_async_copy(
                        G12.at[g, y, x], wbuf.at[slot, :, y, :, pl.ds(s * lane, lane)], LS.at[slot]).start()

    def load_rows(k, c, z, slot):
        for s in TWO:
            g = ((k - 6) * 2 + s) * 3 + c
            pltpu.make_async_copy(
                G3.at[g, z], wbuf3.at[slot, :, :, :, pl.ds(s * 3 * lane, 3 * lane)], LS.at[slot]).start()

    def run_units(k, unit, lo=0, hi=UNITS, known=None, primed=False):
        load, known, body = load_cols, known or hi, unit(k)
        if not primed:
            load(k, lo, lo % SLOTS)
            load(k, lo + 1, (lo + 1) % SLOTS)

        def step(u):
            slot = lax.rem(u, SLOTS)
            take(wbuf.at[slot], LS.at[slot])

            @pl.when(u + 2 < known)
            def _():
                load(k, u + 2, lax.rem(u + 2, SLOTS))
            body(u, slot)
        loop(hi, step, lo)

    def weight(slot):
        return wbuf[slot].reshape(d, pair)

    def tiles(k, u):
        x, c = thirds(u)
        first = 18 * x + 3 * (k % 3) + c
        return first, first + QKV

    def span(t):
        return pl.ds(pl.multiple_of(t * lane, lane), lane)

    def both(r):
        return r[:, :lane], r[:, lane:]

    def qkv_unit(k):
        def body(u, slot):
            r = jnp.dot(h[...], weight(slot), preferred_element_type=F32)
            for t, v in zip(tiles(k, u), both(r)):
                v = (v + bqkv[t]).astype(BF).T

                @pl.when(t < 18)
                def _():
                    qt[span(t), :] = v

                @pl.when(t >= 18)
                def _():
                    kv_ref[span(t - 18), :] = v
        return body

    def out_unit(k):
        def body(u, slot):
            r = jnp.dot(ctx[...], weight(slot), preferred_element_type=F32)
            for t, v in zip(tiles(k, u - QKV), both(r)):
                x1[:, span(t)] = (x_ref[:, span(t)].astype(F32) + v + bout[t]).astype(BF)
        return body

    def up_unit(k):
        def body(u, slot):
            r = jnp.dot(h[...], weight(slot), preferred_element_type=F32)
            for t, v in zip(tiles(k, u), both(r)):
                a[:, span(t)] = jax.nn.gelu(v + bup[t], approximate=True).astype(BF)
        return body

    def quarter(u):
        o, c = thirds(u)
        return c, wrap(place(c)[2] + o + o // 2 - o // 3 * 2)

    def down_lhs(c, z):
        n = 16 * (rows // 3)
        return a[:, pl.ds(pl.multiple_of((c * 4 + z) * n, lane), n)]

    def add(u, cols, r):
        @pl.when(u == 0)
        def _():
            acc[:, cols] = r

        @pl.when(u > 0)
        def _():
            acc[:, cols] += r

    def finish(k):
        n = 3 * lane
        for s in TWO:
            cols = pl.ds(s * share + (k - 6) * n, n)
            y_ref[:, cols] = (x1[:, cols].astype(F32) + acc[:, s * n:(s + 1) * n] + bdown[:, cols]).astype(BF)

    def run_down(k, lo=0, hi=UNITS, known=UNITS, primed=False):
        def load(u):
            c, z = quarter(u)
            load_rows(k, c, z, lax.rem(u, SLOTS))
        if not primed:
            load(lo)
            load(lo + 1)

        def step(u):
            slot = lax.rem(u, SLOTS)
            take(wbuf3.at[slot], LS.at[slot])

            @pl.when(u + 2 < known)
            def _():
                load(u + 2)
            w = wbuf3[slot].reshape(-1, 6 * lane)
            add(u, slice(None), jnp.dot(down_lhs(*quarter(u)), w, preferred_element_type=F32))
        loop(hi, step, lo)
        if hi == UNITS:
            finish(k)

    def run_last(lo, hi, s, ahead=None):
        n = 3 * lane
        cols = pl.ds(pl.multiple_of(s * n, lane), n)

        def step(u):
            c, z = quarter(u)
            if ahead is not None:
                take(G8.at[c, ahead], R.at[LAST * 3 + c, SIBLING, ahead])
            add(u, cols, jnp.dot(down_lhs(c, z), G8[3 * s + c, z].reshape(-1, n), preferred_element_type=F32))
        loop(hi, step, lo)

    def norm(src, which):
        n = seq // 8

        def step(b):
            at = pl.ds(pl.multiple_of(b * n, n), n)
            v = src[at, :].astype(F32)
            v = v - jnp.mean(v, axis=-1, keepdims=True)
            var = jnp.mean(v * v, axis=-1, keepdims=True)
            h[at, :] = (v * lax.rsqrt(var + LN_EPS) * lnv[which] + lnv[which + 1]).astype(BF)
        loop(8, step)

    def attend(lo, hi):
        qb = seq // 2
        scale = hd ** -0.5

        def step(i):
            q_rows = pl.ds(pl.multiple_of(i * hd, hd), hd)
            k_rows = q_rows
            v_rows = pl.ds(pl.multiple_of(i * hd + d, hd), hd)
            for b in TWO:
                n = (b + 1) * qb
                q = qt[q_rows, b * qb:n]
                s = lax.dot_general(q, kv_ref[k_rows, :n], (((0,), (0,)), ((), ())),
                                    preferred_element_type=F32) * scale
                row = lax.broadcasted_iota(jnp.int32, (qb, n), 0) + b * qb
                col = lax.broadcasted_iota(jnp.int32, (qb, n), 1)
                s = jnp.where(col <= row, s, -jnp.inf)
                e = jnp.exp(s - jnp.max(s, axis=-1, keepdims=True))
                w = (e / jnp.sum(e, axis=-1, keepdims=True)).astype(BF)
                o = lax.dot_general(kv_ref[v_rows, :n], w, (((1,), (1,)), ((), ())),
                                    preferred_element_type=F32)
                ctxt[q_rows, b * qb:n] = o.astype(BF)
        loop(hi, step, lo)

    def flip():
        def step(i):
            at = pl.ds(pl.multiple_of(i * pair, pair), pair)
            ctx[:, at] = ctxt[at, :].T
        loop(d // pair, step)

    x_copy = pltpu.make_async_copy(x_hbm, x_ref, OS.at[CHUNKS])
    x_copy.start()
    v_pack()
    permute_up()
    pl.semaphore_wait(barrier, len(partners))
    early, rest, whole = (0, 3 * lane), (3 * lane, 6 * lane), (0, share)
    x_send(0, *early)
    x_send(0, *rest)
    x3_send()
    v_send(0)
    x_wait(0, *early)
    x_blocks(0)
    p0_send(0)
    x_wait(0, *rest)
    for k in (1, 2):
        x_blocks(k)
        p0_send(k)
    p0_forward(0)
    x3_blocks()
    await_group(0, 0, ACROSS)
    axis_first(0, 1)
    axis_second(0, 1)
    p0_forward(1)
    p0_send(6)
    axis_forward(0, 1)
    await_group(1, 0, ACROSS)
    axis_first(1, 1)
    axis_second(1, 1)
    x_send(1, *whole)
    v_send(1)
    p0_send(7)
    p0_send(8)
    await_group(0, 1, SECOND)
    await_group(0, 1, ACROSS)
    axis_first(0, 2)
    v_send(2)
    visit1(0)
    x_copy.wait()
    x_wait(1, *whole)
    for k in LATE:
        x_blocks(k)
    visit2(0)
    v_rows()
    norm(x_ref, 0)
    visit1(1)
    v_long(0, bqkv, d, 9)
    visit2(1)
    run_units(0, qkv_unit, hi=QKV)
    visit1(2)
    v_long(1, bup, 4 * d, 12)
    visit2(2)
    run_units(1, qkv_unit, hi=QKV)
    visit1(3)
    visit2(3)
    run_units(2, qkv_unit, hi=QKV)
    q1, q2, q3 = 3, 6, QKV
    a1, a2 = heads * q3 // 24, heads * 18 // 24
    attend(0, a1)
    visit1(4)
    attend(a1, a2)
    visit2(4)
    attend(a2, heads)
    flip()
    run_units(0, out_unit, QKV)
    run_units(1, out_unit, QKV)
    visit1(5)
    run_units(2, out_unit, QKV)
    norm(x1, 2)
    run_units(3, up_unit, hi=q1, known=UNITS)
    visit2(5)
    run_units(3, up_unit, q1, primed=True)
    run_units(4, up_unit, hi=q2, known=UNITS)
    visit1(6)
    run_units(4, up_unit, q2, primed=True)
    visit2(6)
    run_units(5, up_unit, hi=q3, known=UNITS)
    visit1(7)
    run_units(5, up_unit, q3, primed=True)
    visit2(7)
    run_down(6, hi=q2)
    sides_in(7)
    run_down(6, q2, primed=True)
    across_in(7)
    await_siblings(7, FIRST, *SIDES)
    run_down(7, hi=q2, known=q3)
    axis_forward(LAST, 2)
    run_down(7, q2, q3, q3, True)
    await_siblings(7, ACROSS)
    run_down(7, q3)
    other = 1 - core
    sides_in(LAST)
    run_last(FIRST, q1, core)
    run_last(FIRST, q1, other, FIRST)
    run_last(q1, q3, core)
    run_last(q1, q2, other, SIDES[0])
    across_in(LAST)
    run_last(q2, q3, other, SIDES[1])
    run_last(q3, UNITS, core)
    run_last(q3, UNITS, other, ACROSS)
    finish(LAST)

    for k in range(CHUNKS):
        ref = Block(k).ref
        for p in THREE:
            take(ref.at[(ALL3,) + ZEROS[:2 - p] + (ALL3,)], S.at[k, p])
        take(ref.at[ALL3], S.at[k, SIBLING])
    for m, lo, n in ((0,) + early, (0,) + rest, (1,) + whole):
        take(stage12.at[m, OTHERS, :, pl.ds(lo, n)], XS.at[2 * m + (lo > 0)])
    take(stage3.at[0], XS.at[4])
    take(V.at[0, 0, OTHERS], VS.at[0])
    take(V.at[0, ALL3], VS.at[1])
    take(V.at[ALL3], VS.at[2])


def solution(mesh):
    batch_axes = ('dp', 'fsdp')

    def local_layer(prompts, ln1_gain, ln1_bias, w_qkv, b_qkv, w_out, b_out, ln2_gain, ln2_bias, w_up, b_up, w_down, b_down):
        _, seq, d = prompts.shape
        heads, hd = w_qkv.shape[2], w_qkv.shape[3]
        lane = d // 18
        rows = d // 16
        pair = 2 * lane
        third = rows // 3
        r = w_up.shape[0]

        parts = [ln1_gain, ln1_bias, b_out, ln2_gain, ln2_bias, b_down, b_qkv, b_up]
        orders = ((0, 1, 2), (2, 0, 1), (1, 2, 0))

        hidden = np.arange(4 * d).reshape(4, 4, 4, 3, third)
        hidden = np.concatenate([hidden[:, :, :, c].transpose(orders[c] + (3,)).reshape(-1) for c in THREE])
        index = [(np.arange(d), d // 128), (np.arange(3 * d), 3 * d // 128), (hidden, 4 * d // 128)]
        tab = np.stack([np.concatenate([i // n for i, n in index]), np.concatenate([i % n for i, n in index])])

        dims = (seq, d, heads, hd, rows, lane)
        vm = pl.BlockSpec(memory_space=pltpu.VMEM)
        hbm = pl.BlockSpec(memory_space=pl.ANY)
        dma = pltpu.SemaphoreType.DMA
        act, act_t = pltpu.VMEM((seq, d), BF), pltpu.VMEM((d, seq), BF)
        y, kv, _, _ = pl.pallas_call(
            functools.partial(layer_kernel, dims),
            out_shape=(
                pltpu.VMEM((seq, d), BF),
                pltpu.VMEM((2 * d, seq), BF),
                jax.ShapeDtypeStruct((36, 4, 4, 4, rows, lane), BF),
                jax.ShapeDtypeStruct((12, 4, 4, 4, third, 3 * lane), BF),
            ),
            in_specs=[hbm] + [vm] * 13,
            out_specs=(vm, vm, hbm, hbm),
            scratch_shapes=[
                act, act, act_t, act_t, act, act,
                pltpu.VMEM((seq, 4 * d), BF),
                pltpu.VMEM((SLOTS, 4, 4, rows, pair), BF),
                pltpu.VMEM((SLOTS, 4, 4, third, 6 * lane), BF),
                pltpu.VMEM((seq, 6 * lane), F32),
                pltpu.VMEM((18, rows, lane), BF),
                pltpu.VMEM((9, third, 3 * lane), BF),
                pltpu.VMEM((6, 4, 4, 4, third, 3 * lane), BF),
                pltpu.VMEM((r, 4 * d), BF),
                pltpu.VMEM((2, LINE, r, QKV * lane), BF),
                pltpu.VMEM((2, w_down.shape[0], QKV * lane), BF),
                pltpu.VMEM((LINE, LANES), F32),
                pltpu.VMEM((LINE, LANES), BF),
                pltpu.VMEM((4, 4, LINE, LINE, LANES), BF),
                pltpu.VMEM((4, 1, d), F32),
                pltpu.VMEM((54, 1, lane), F32),
                pltpu.VMEM((18, 1, lane), F32),
                pltpu.VMEM((72, 1, lane), F32),
                pltpu.VMEM((1, d), F32),
                pltpu.VMEM((2, LANES, LANES), BF),
                dma((3 * CHUNKS, 4, 4)),
                dma((CHUNKS, 4)),
                dma((SLOTS,)),
                dma((CHUNKS + 1,)),
                dma((5,)),
                dma((5,)),
                dma((3,)),
                dma((3,)),
            ],
            compiler_params=pltpu.CompilerParams(
                has_side_effects=True, collective_id=0, vmem_limit_bytes=54 << 20),
            name="layer",
        )(prompts[0], w_qkv.reshape(r, -1), w_out, w_up, w_down, jnp.asarray(tab, jnp.int32), *(p[None] for p in parts))
        kc, vc = (m.reshape(heads, hd, seq).transpose(2, 0, 1)[None] for m in (kv[:d], kv[d:]))
        return y[None], kc, vc

    weight_spec = P('fsdp')
    return jax.shard_map(local_layer, mesh=mesh, in_specs=(P(batch_axes),) + (weight_spec,) * 12, out_specs=(P(batch_axes), P(batch_axes), P(batch_axes)), check_vma=False)
```

```python
import functools

import jax
import jax.numpy as jnp
import numpy as np
from jax import lax
from jax.experimental import pallas as pl
from jax.experimental.pallas import tpu as pltpu
from jax.sharding import PartitionSpec as P

LN_EPS = 1e-5
MESH = pl.DeviceIdType.MESH
BF = jnp.bfloat16
F32 = jnp.float32
CHUNKS = 9
SLOTS = 3
LO, HI, ALL3 = pl.ds(0, 2), pl.ds(2, 2), pl.ds(0, 3)
FIRST, SECOND, ACROSS, SIBLING = range(4)
ZEROS = (0, 0, 0)
THREE = range(3)
TWO = range(2)
OTHERS = pl.ds(0, 7)
UNITS = 12
QKV = 9
LINE = 8
SIDES = (1, 3)
QUARTERS = (0, *SIDES, ACROSS)
LAST = CHUNKS - 1
LANES = 128
LATE = (3, 4, 5)


def loop(hi, body, lo=0):
    def step(i, carry):
        body(i)
        return carry
    lax.fori_loop(lo, hi, step, None)


def wrap(i):
    return lax.rem(i, 4)


def thirds(u):
    return u // 3, lax.rem(u, 3)


def layer_kernel(dims, x_hbm, wq, wo, w2, w3, tab, *refs):
    vecs, (y_ref, kv_ref, G12, G3), refs = refs[:8], refs[8:12], refs[12:]
    (x_ref, h, qt, ctxt, ctx, x1, a, wbuf, wbuf3, acc, own12, own3, G8, w2p, stage12, stage3, vec32, vec, V, lnv, bqkv, bout,
     bup, bdown, vrow, R, S, LS, OS, X, XS, VR, VS) = refs
    seq, d, heads, hd, rows, lane = dims
    pair = 2 * lane
    me = lax.axis_index("fsdp")
    core = lax.rem(me, 2)
    cx = wrap(me // 2)
    cy = wrap(me // 8)
    cz = me // 32
    sib = me + 1 - 2 * core
    spot = lax.rem(me, LINE)
    line = [me - spot + lax.rem(spot + o, LINE) for o in range(1, LINE)]
    column = [me + (wrap(cy + o) - cy) * 8 for o in range(1, 4)]
    pillar = [me + (wrap(cz + o) - cz) * 32 for o in range(1, 4)]

    barrier = pltpu.get_barrier_semaphore()
    partners = line + column + pillar
    for dev in partners:
        pl.semaphore_signal(barrier, inc=1, device_id={"fsdp": dev}, device_id_type=MESH)

    class Block:
        def __init__(self, k):
            self.ref, self.base = (G12, k) if k < 6 else (G3, k - 6)
            self.blocks, self.first = (own12, 3 * k) if k < 6 else (own3, 3 * (k - 6))
            if k == LAST:
                self.ref, self.base = G8, 0

        def slab(self, c):
            return (self.base * 2 + core) * 3 + c

        def own(self, c):
            return self.blocks.at[self.first + c]

    def pick(c, v):
        return jnp.where(c == 0, v[0], jnp.where(c == 1, v[1], v[2]))

    def place(c):
        v = (cx, cy, cz)
        return tuple(pick(c, v[p:] + v[:p]) for p in THREE)

    def near(c, p):
        v = (2, 8, 32)
        stride = pick(c, v[p:] + v[:p])
        i = place(c)[p]
        up, down = wrap(i + 1), wrap(i + 3)
        return me + (up - i) * stride, me + (down - i) * stride, up, down

    def send(src, dst, s, r, dev):
        pltpu.make_async_remote_copy(
            src_ref=src, dst_ref=dst, send_sem=s, recv_sem=r,
            device_id={"fsdp": dev}, device_id_type=MESH).start()

    def take(ref, sem):
        pltpu.make_async_copy(ref, ref, sem).wait()

    def colours(body):
        loop(3, body)

    def await_group(k, p, role, n=None):
        B = Block(k)

        def body(c):
            at = (B.slab(c),) + ZEROS[:3 - p]
            if n is not None:
                at = at[:-1] + (n,)
            take(B.ref.at[at], R.at[k * 3 + c, p, role])
        colours(body)

    def await_siblings(k, *quarters):
        B = Block(k)
        for ahead in quarters:
            colours(lambda c: take(B.ref.at[B.slab(c), 0], R.at[k * 3 + c, SIBLING, ahead]))

    def p0_send(k):
        B = Block(k)

        def body(c):
            i0, i1, i2 = place(c)
            right, left, _, _ = near(c, 0)
            dst = B.ref.at[B.slab(c), i2, i1, i0]
            for dev in (right, left):
                send(B.own(c), dst, S.at[k, 0], R.at[k * 3 + c, 0, FIRST], dev)
            pltpu.make_async_copy(B.own(c), dst, OS.at[k]).start()
        colours(body)

    def p0_forward(k):
        B = Block(k)
        take(B.ref.at[0, 0, 0, ALL3], OS.at[k])
        await_group(k, 0, FIRST, LO)

        def body(c):
            i0, i1, i2 = place(c)
            right, left, up, down = near(c, 0)
            from_, to = (down, right) if k % 2 == 0 else (up, left)
            blk = B.ref.at[B.slab(c), i2, i1, from_]
            send(blk, blk, S.at[k, 0], R.at[k * 3 + c, 0, ACROSS], to)
        colours(body)

    def halves(k, c, p, i):
        B = Block(k)
        at = (B.slab(c), place(c)[2], i) if p == 1 else (B.slab(c), i)
        return B.ref.at[at + (LO,)], B.ref.at[at + (HI,)]

    def to_sibling(k, c, ahead):
        B = Block(k)
        part = B.ref.at[B.slab(c), wrap(place(c)[2] + ahead)]
        send(part, part, S.at[k, SIBLING], R.at[k * 3 + c, SIBLING, ahead], sib)

    def axis_first(k, p):
        def body(c):
            right, left, _, _ = near(c, p)
            lo, hi = halves(k, c, p, place(c)[p])
            send(lo, lo, S.at[k, p], R.at[k * 3 + c, p, FIRST], right)
            send(hi, hi, S.at[k, p], R.at[k * 3 + c, p, FIRST], left)
            if p == 2:
                to_sibling(k, c, 0)
        colours(body)

    def axis_second(k, p):
        def body(c):
            right, left, _, _ = near(c, p)
            lo, hi = halves(k, c, p, place(c)[p])
            send(hi, hi, S.at[k, p], R.at[k * 3 + c, p, SECOND], right)
            send(lo, lo, S.at[k, p], R.at[k * 3 + c, p, SECOND], left)
        colours(body)

    def axis_forward(k, p):
        await_group(k, p, FIRST)

        def body(c):
            right, left, up, down = near(c, p)
            lo, hi = halves(k, c, p, down)[0], halves(k, c, p, up)[1]
            send(lo, lo, S.at[k, p], R.at[k * 3 + c, p, ACROSS], right)
            send(hi, hi, S.at[k, p], R.at[k * 3 + c, p, ACROSS], left)
        colours(body)

    def sides_in(k):
        await_group(k, 2, SECOND)

        for ahead in SIDES:
            colours(lambda c: to_sibling(k, c, ahead))

    def across_in(k):
        await_group(k, 2, ACROSS)
        colours(lambda c: to_sibling(k, c, ACROSS))

    share = QKV * lane

    def x_send(m, lo, n):
        at = stage12.at[m, spot, :, pl.ds(lo, n)]

        def give(src, i, dev):
            part = src.at[:, pl.ds(pl.multiple_of(i * share + lo, lane), n)]
            sem = 2 * m + (lo > 0)
            if dev is None:
                pltpu.make_async_copy(part, at, X.at[sem]).start()
            else:
                send(part, at, XS.at[sem], X.at[sem], dev)

        def route(i, dev):
            if m:
                give(w2p, i, dev)
                return

            @pl.when(i < 6)
            def _():
                give(wq, i, dev)

            @pl.when(i >= 6)
            def _():
                give(wo, i - 6, dev)
        for dev in line:
            route(lax.rem(dev, LINE), dev)
        route(spot, None)

    def x_wait(m, lo, n):
        take(stage12.at[m, :, :, pl.ds(lo, n)], X.at[2 * m + (lo > 0)])

    def x_blocks(k):
        for c in THREE:
            lanes = pl.ds((3 * (k % 3) + c) * lane, lane)
            own12[3 * k + c] = jnp.concatenate(
                [stage12[k // 3, i, :, lanes].astype(F32) for i in range(LINE)], axis=0).astype(BF)

    def x3_send():
        part = lambda s: w3.at[:, pl.ds(pl.multiple_of(s * share, lane), share)]
        send(part(1 - core), stage3.at[core], XS.at[4], X.at[4], sib)
        pltpu.make_async_copy(part(core), stage3.at[core], X.at[4]).start()

    def x3_blocks():
        take(stage3, X.at[4])
        n = rows // 3
        for j in THREE:
            lanes = slice(3 * j * lane, 3 * (j + 1) * lane)
            both = jnp.concatenate([stage3[s, :, lanes].astype(F32) for s in TWO], axis=0)
            for c in THREE:
                own3[3 * j + c] = both[c * n:(c + 1) * n].astype(BF)

    def permute_up():
        n = rows // 3
        for c in THREE:
            v = (1, 4, 16)
            s0, s1, s2 = v[c:] + v[:c]
            for i in range(4):
                chips = [i * s2 + j * s1 + k * s0 for j in range(4) for k in range(4)]
                groups = [w2[:, q * rows + c * n:q * rows + (c + 1) * n].astype(F32) for q in chips]
                w2p[:, (4 * c + i) * 16 * n:(4 * c + i + 1) * 16 * n] = jnp.concatenate(groups, axis=1).astype(BF)

    def v_pack():
        vec32[...] = jnp.zeros_like(vec32)
        for i, ref in enumerate(vecs):
            vec32[i:i + 1, :ref.shape[1]] = ref[...].astype(F32)
        vec[...] = vec32[...].astype(BF)

    def v_send(axis):
        if axis == 0:
            part = V.at[cz, cy, spot]
            for dev in line:
                send(vec, part, VS.at[0], VR.at[0], dev)
            pltpu.make_async_copy(vec, part, VR.at[0]).start()
        elif axis == 1:
            take(V.at[0, 0], VR.at[0])
            for dev in column:
                send(V.at[cz, cy], V.at[cz, cy], VS.at[1], VR.at[1], dev)
        else:
            take(V.at[0, ALL3], VR.at[1])
            for dev in pillar:
                send(V.at[cz], V.at[cz], VS.at[2], VR.at[2], dev)

    def spread(vals, at):
        n = at.size
        select = (lax.broadcasted_iota(jnp.int32, (LANES, n), 0) == tab[1:2, at]).astype(BF)
        return jnp.dot(vals, select, preferred_element_type=F32)

    def v_rows():
        take(V.at[ALL3], VR.at[2])
        nd = d // pair

        def body(t):
            at = pl.ds(pl.multiple_of(t * pair, pair), pair)
            m = spread(V[...].reshape(-1, LANES), at).reshape(LANES, LINE, pair)
            dev = lax.broadcasted_iota(jnp.int32, m.shape, 0)
            v = jnp.sum(jnp.where(dev == tab[0:1, at][None], m, 0.0), axis=0)
            for i, src in enumerate((0, 1, 3, 4)):
                lnv[i, :, at] = v[src:src + 1]
            for o in TWO:
                bout[2 * t + o] = v[2:3, o * lane:(o + 1) * lane]
            bdown[:, at] = v[5:6]
        loop(nd, body)
        dev = lax.broadcasted_iota(jnp.int32, (LANES, LINE * LANES), 0)
        slot = lax.broadcasted_iota(jnp.int32, (LANES, LINE * LANES), 1)
        for i in TWO:
            take_row = (slot == dev * LINE + 6 + i).astype(BF)
            vrow[i] = jnp.dot(take_row, V[...].reshape(-1, LANES), preferred_element_type=F32).astype(BF)

    def v_long(i, out, first, count):
        wide = 3 * pair

        def body(t):
            at = pl.ds(pl.multiple_of(first + t * wide, pair), wide)
            m = spread(vrow[i], at)
            dev = lax.broadcasted_iota(jnp.int32, m.shape, 0)
            v = jnp.sum(jnp.where(dev == tab[0:1, at], m, 0.0), axis=0, keepdims=True)
            for o in range(6):
                out[6 * t + o] = v[:, o * lane:(o + 1) * lane]
        loop(count, body)

    def issue(t):
        if t + 1 < CHUNKS:
            axis_first(t + 1, 1)
            axis_second(t + 1, 1)
        axis_first(t, 2)

    def visit1(t):
        last, ahead, far = t - 1, t + 1, t + 2
        if t:
            sides_in(last)
            across_in(last)
        if far < CHUNKS:
            p0_forward(far)
        if ahead < CHUNKS:
            axis_forward(ahead, 1)
        axis_second(t, 2)

    def visit2(t):
        last, ahead, far, farther = t - 1, t + 1, t + 2, t + 3
        axis_forward(t, 2)
        if far < CHUNKS:
            await_group(far, 0, ACROSS)
        if ahead < CHUNKS:
            for role in (SECOND, ACROSS):
                await_group(ahead, 1, role)
            if farther in LATE:
                p0_send(farther)
            issue(ahead)
        if ahead == LAST:
            axis_second(LAST, 2)
        if t:
            await_siblings(last, *QUARTERS)

    def load_cols(k, u, slot):
        x, c = thirds(u)
        for s in TWO:
            g = (k * 2 + s) * 3 + c
            dst = wbuf.at[slot, :, :, :, pl.ds(s * lane, lane)]

            @pl.when(c == 0)
            def _():
                pltpu.make_async_copy(G12.at[g, :, :, x], dst, LS.at[slot]).start()

            @pl.when(c == 1)
            def _():
                pltpu.make_async_copy(G12.at[g, x], dst, LS.at[slot]).start()

            @pl.when(c > 1)
            def _():
                for y in range(4):
                    pltpu.make_async_copy(
                        G12.at[g, y, x], wbuf.at[slot, :, y, :, pl.ds(s * lane, lane)], LS.at[slot]).start()

    def load_rows(k, c, z, slot):
        for s in TWO:
            g = ((k - 6) * 2 + s) * 3 + c
            pltpu.make_async_copy(
                G3.at[g, z], wbuf3.at[slot, :, :, :, pl.ds(s * 3 * lane, 3 * lane)], LS.at[slot]).start()

    def run_units(k, unit, lo=0, hi=UNITS, known=None, primed=False):
        load, known, body = load_cols, known or hi, unit(k)
        if not primed:
            load(k, lo, lo % SLOTS)
            load(k, lo + 1, (lo + 1) % SLOTS)

        def step(u):
            slot = lax.rem(u, SLOTS)
            take(wbuf.at[slot], LS.at[slot])

            @pl.when(u + 2 < known)
            def _():
                load(k, u + 2, lax.rem(u + 2, SLOTS))
            body(u, slot)
        loop(hi, step, lo)

    def weight(slot):
        return wbuf[slot].reshape(d, pair)

    def tiles(k, u):
        x, c = thirds(u)
        first = 18 * x + 3 * (k % 3) + c
        return first, first + QKV

    def span(t):
        return pl.ds(pl.multiple_of(t * lane, lane), lane)

    def both(r):
        return r[:, :lane], r[:, lane:]

    def qkv_unit(k):
        def body(u, slot):
            r = jnp.dot(h[...], weight(slot), preferred_element_type=F32)
            for t, v in zip(tiles(k, u), both(r)):
                v = (v + bqkv[t]).astype(BF).T

                @pl.when(t < 18)
                def _():
                    qt[span(t), :] = v

                @pl.when(t >= 18)
                def _():
                    kv_ref[span(t - 18), :] = v
        return body

    def out_unit(k):
        def body(u, slot):
            r = jnp.dot(ctx[...], weight(slot), preferred_element_type=F32)
            for t, v in zip(tiles(k, u - QKV), both(r)):
                x1[:, span(t)] = (x_ref[:, span(t)].astype(F32) + v + bout[t]).astype(BF)
        return body

    def up_unit(k):
        def body(u, slot):
            r = jnp.dot(h[...], weight(slot), preferred_element_type=F32)
            for t, v in zip(tiles(k, u), both(r)):
                a[:, span(t)] = jax.nn.gelu(v + bup[t], approximate=True).astype(BF)
        return body

    def quarter(u):
        o, c = thirds(u)
        return c, wrap(place(c)[2] + o + o // 2 - o // 3 * 2)

    def down_lhs(c, z):
        n = 16 * (rows // 3)
        return a[:, pl.ds(pl.multiple_of((c * 4 + z) * n, lane), n)]

    def add(u, cols, r):
        @pl.when(u == 0)
        def _():
            acc[:, cols] = r

        @pl.when(u > 0)
        def _():
            acc[:, cols] += r

    def finish(k):
        n = 3 * lane
        for s in TWO:
            cols = pl.ds(s * share + (k - 6) * n, n)
            y_ref[:, cols] = (x1[:, cols].astype(F32) + acc[:, s * n:(s + 1) * n] + bdown[:, cols]).astype(BF)

    def run_down(k, lo=0, hi=UNITS, known=UNITS, primed=False):
        def load(u):
            c, z = quarter(u)
            load_rows(k, c, z, lax.rem(u, SLOTS))
        if not primed:
            load(lo)
            load(lo + 1)

        def step(u):
            slot = lax.rem(u, SLOTS)
            take(wbuf3.at[slot], LS.at[slot])

            @pl.when(u + 2 < known)
            def _():
                load(u + 2)
            w = wbuf3[slot].reshape(-1, 6 * lane)
            add(u, slice(None), jnp.dot(down_lhs(*quarter(u)), w, preferred_element_type=F32))
        loop(hi, step, lo)
        if hi == UNITS:
            finish(k)

    def run_last(lo, hi, s, ahead=None):
        n = 3 * lane
        cols = pl.ds(pl.multiple_of(s * n, lane), n)

        def step(u):
            c, z = quarter(u)
            if ahead is not None:
                take(G8.at[c, ahead], R.at[LAST * 3 + c, SIBLING, ahead])
            add(u, cols, jnp.dot(down_lhs(c, z), G8[3 * s + c, z].reshape(-1, n), preferred_element_type=F32))
        loop(hi, step, lo)

    def norm(src, which):
        n = seq // 8

        def step(b):
            at = pl.ds(pl.multiple_of(b * n, n), n)
            v = src[at, :].astype(F32)
            v = v - jnp.mean(v, axis=-1, keepdims=True)
            var = jnp.mean(v * v, axis=-1, keepdims=True)
            h[at, :] = (v * lax.rsqrt(var + LN_EPS) * lnv[which] + lnv[which + 1]).astype(BF)
        loop(8, step)

    def attend(lo, hi):
        qb = seq // 2
        scale = hd ** -0.5

        def step(i):
            q_rows = pl.ds(pl.multiple_of(i * hd, hd), hd)
            k_rows = q_rows
            v_rows = pl.ds(pl.multiple_of(i * hd + d, hd), hd)
            for b in TWO:
                n = (b + 1) * qb
                q = qt[q_rows, b * qb:n]
                s = lax.dot_general(q, kv_ref[k_rows, :n], (((0,), (0,)), ((), ())),
                                    preferred_element_type=F32) * scale
                row = lax.broadcasted_iota(jnp.int32, (qb, n), 0) + b * qb
                col = lax.broadcasted_iota(jnp.int32, (qb, n), 1)
                s = jnp.where(col <= row, s, -jnp.inf)
                e = jnp.exp(s - jnp.max(s, axis=-1, keepdims=True))
                w = (e / jnp.sum(e, axis=-1, keepdims=True)).astype(BF)
                o = lax.dot_general(kv_ref[v_rows, :n], w, (((1,), (1,)), ((), ())),
                                    preferred_element_type=F32)
                ctxt[q_rows, b * qb:n] = o.astype(BF)
        loop(hi, step, lo)

    def flip():
        def step(i):
            at = pl.ds(pl.multiple_of(i * pair, pair), pair)
            ctx[:, at] = ctxt[at, :].T
        loop(d // pair, step)

    x_copy = pltpu.make_async_copy(x_hbm, x_ref, OS.at[CHUNKS])
    x_copy.start()
    v_pack()
    permute_up()
    pl.semaphore_wait(barrier, len(partners))
    early, rest, whole = (0, 3 * lane), (3 * lane, 6 * lane), (0, share)
    x_send(0, *early)
    x_send(0, *rest)
    x3_send()
    v_send(0)
    x_wait(0, *early)
    x_blocks(0)
    p0_send(0)
    x_wait(0, *rest)
    for k in (1, 2):
        x_blocks(k)
        p0_send(k)
    p0_forward(0)
    v_send(1)
    x3_blocks()
    await_group(0, 0, ACROSS)
    axis_first(0, 1)
    axis_second(0, 1)
    p0_forward(1)
    p0_send(6)
    axis_forward(0, 1)
    await_group(1, 0, ACROSS)
    axis_first(1, 1)
    axis_second(1, 1)
    x_send(1, *whole)
    v_send(2)
    p0_send(7)
    p0_send(8)
    await_group(0, 1, SECOND)
    await_group(0, 1, ACROSS)
    axis_first(0, 2)
    visit1(0)
    x_copy.wait()
    x_wait(1, *whole)
    for k in LATE:
        x_blocks(k)
    visit2(0)
    v_rows()
    norm(x_ref, 0)
    visit1(1)
    v_long(0, bqkv, d, 9)
    visit2(1)
    run_units(0, qkv_unit, hi=QKV)
    visit1(2)
    v_long(1, bup, 4 * d, 12)
    visit2(2)
    run_units(1, qkv_unit, hi=QKV)
    visit1(3)
    visit2(3)
    run_units(2, qkv_unit, hi=QKV)
    q1, q2, q3 = 3, 6, QKV
    a1, a2 = heads * 7 // 24, heads * 14 // 24
    attend(0, a1)
    visit1(4)
    attend(a1, a2)
    visit2(4)
    attend(a2, heads)
    flip()
    run_units(0, out_unit, QKV)
    visit1(5)
    run_units(1, out_unit, QKV)
    run_units(2, out_unit, QKV)
    visit2(5)
    norm(x1, 2)
    run_units(3, up_unit)
    visit1(6)
    run_units(4, up_unit, hi=q2, known=UNITS)
    visit2(6)
    run_units(4, up_unit, q2, primed=True)
    run_units(5, up_unit, hi=q2, known=UNITS)
    visit1(7)
    run_units(5, up_unit, q2, primed=True)
    visit2(7)
    run_down(6, hi=q2)
    sides_in(7)
    run_down(6, q2, primed=True)
    across_in(7)
    await_siblings(7, FIRST, *SIDES)
    run_down(7, hi=q2, known=q3)
    axis_forward(LAST, 2)
    run_down(7, q2, q3, q3, True)
    await_siblings(7, ACROSS)
    run_down(7, q3)
    other = 1 - core
    sides_in(LAST)
    run_last(FIRST, q1, core)
    run_last(FIRST, q1, other, FIRST)
    run_last(q1, q3, core)
    run_last(q1, q2, other, SIDES[0])
    across_in(LAST)
    run_last(q2, q3, other, SIDES[1])
    run_last(q3, UNITS, core)
    run_last(q3, UNITS, other, ACROSS)
    finish(LAST)

    for k in range(CHUNKS):
        ref = Block(k).ref
        for p in THREE:
            take(ref.at[(ALL3,) + ZEROS[:2 - p] + (ALL3,)], S.at[k, p])
        take(ref.at[ALL3], S.at[k, SIBLING])
    for m, lo, n in ((0,) + early, (0,) + rest, (1,) + whole):
        take(stage12.at[m, OTHERS, :, pl.ds(lo, n)], XS.at[2 * m + (lo > 0)])
    take(stage3.at[0], XS.at[4])
    take(V.at[0, 0, OTHERS], VS.at[0])
    take(V.at[0, ALL3], VS.at[1])
    take(V.at[ALL3], VS.at[2])


def solution(mesh):
    batch_axes = ('dp', 'fsdp')

    def local_layer(prompts, ln1_gain, ln1_bias, w_qkv, b_qkv, w_out, b_out, ln2_gain, ln2_bias, w_up, b_up, w_down, b_down):
        _, seq, d = prompts.shape
        heads, hd = w_qkv.shape[2], w_qkv.shape[3]
        lane = d // 18
        rows = d // 16
        pair = 2 * lane
        third = rows // 3
        r = w_up.shape[0]

        parts = [ln1_gain, ln1_bias, b_out, ln2_gain, ln2_bias, b_down, b_qkv, b_up]
        orders = ((0, 1, 2), (2, 0, 1), (1, 2, 0))

        hidden = np.arange(4 * d).reshape(4, 4, 4, 3, third)
        hidden = np.concatenate([hidden[:, :, :, c].transpose(orders[c] + (3,)).reshape(-1) for c in THREE])
        index = [(np.arange(d), d // 128), (np.arange(3 * d), 3 * d // 128), (hidden, 4 * d // 128)]
        tab = np.stack([np.concatenate([i // n for i, n in index]), np.concatenate([i % n for i, n in index])])

        dims = (seq, d, heads, hd, rows, lane)
        vm = pl.BlockSpec(memory_space=pltpu.VMEM)
        hbm = pl.BlockSpec(memory_space=pl.ANY)
        dma = pltpu.SemaphoreType.DMA
        act, act_t = pltpu.VMEM((seq, d), BF), pltpu.VMEM((d, seq), BF)
        y, kv, _, _ = pl.pallas_call(
            functools.partial(layer_kernel, dims),
            out_shape=(
                pltpu.VMEM((seq, d), BF),
                pltpu.VMEM((2 * d, seq), BF),
                jax.ShapeDtypeStruct((36, 4, 4, 4, rows, lane), BF),
                jax.ShapeDtypeStruct((12, 4, 4, 4, third, 3 * lane), BF),
            ),
            in_specs=[hbm] + [vm] * 13,
            out_specs=(vm, vm, hbm, hbm),
            scratch_shapes=[
                act, act, act_t, act_t, act, act,
                pltpu.VMEM((seq, 4 * d), BF),
                pltpu.VMEM((SLOTS, 4, 4, rows, pair), BF),
                pltpu.VMEM((SLOTS, 4, 4, third, 6 * lane), BF),
                pltpu.VMEM((seq, 6 * lane), F32),
                pltpu.VMEM((18, rows, lane), BF),
                pltpu.VMEM((9, third, 3 * lane), BF),
                pltpu.VMEM((6, 4, 4, 4, third, 3 * lane), BF),
                pltpu.VMEM((r, 4 * d), BF),
                pltpu.VMEM((2, LINE, r, QKV * lane), BF),
                pltpu.VMEM((2, w_down.shape[0], QKV * lane), BF),
                pltpu.VMEM((LINE, LANES), F32),
                pltpu.VMEM((LINE, LANES), BF),
                pltpu.VMEM((4, 4, LINE, LINE, LANES), BF),
                pltpu.VMEM((4, 1, d), F32),
                pltpu.VMEM((54, 1, lane), F32),
                pltpu.VMEM((18, 1, lane), F32),
                pltpu.VMEM((72, 1, lane), F32),
                pltpu.VMEM((1, d), F32),
                pltpu.VMEM((2, LANES, LANES), BF),
                dma((3 * CHUNKS, 4, 4)),
                dma((CHUNKS, 4)),
                dma((SLOTS,)),
                dma((CHUNKS + 1,)),
                dma((5,)),
                dma((5,)),
                dma((3,)),
                dma((3,)),
            ],
            compiler_params=pltpu.CompilerParams(
                has_side_effects=True, collective_id=0, vmem_limit_bytes=54 << 20),
            name="layer",
        )(prompts[0], w_qkv.reshape(r, -1), w_out, w_up, w_down, jnp.asarray(tab, jnp.int32), *(p[None] for p in parts))
        kc, vc = (m.reshape(heads, hd, seq).transpose(2, 0, 1)[None] for m in (kv[:d], kv[d:]))
        return y[None], kc, vc

    weight_spec = P('fsdp')
    return jax.shard_map(local_layer, mesh=mesh, in_specs=(P(batch_axes),) + (weight_spec,) * 12, out_specs=(P(batch_axes), P(batch_axes), P(batch_axes)), check_vma=False)
```
